128 devices in a mesh: seq: 32 (over z_lo, y, x), head: 4 (over z_hi, core).
Axes of the slice: x: 4, y: 4, z: 4 (z_hi: 2, z_lo: 2; z = z_hi * 2 + z_lo), core: 2. Of those that a mesh axis runs over, the one named last changes fastest.
Arguments:
- text_states: bfloat16 [8192, 4096], P('seq', 'head'), may hold values from -200 to 200
- query_weight: bfloat16 [4096, 4096], P(None, 'head'), may hold values from -0.09375 to 0.09375
- image_keys: bfloat16 [16384, 1024], P('seq', 'head'), may hold values from -12 to 12
- image_values: bfloat16 [16384, 1024], P('seq', 'head'), may hold values from -24 to 24
- output_weight: bfloat16 [4096, 4096], P('head'), may hold values from -0.09375 to 0.09375
- attn_gate: float32 [1], replicated, may hold values from 0.3 to 1.5
- frame_lengths: int32 [64], replicated, may hold values from 1 to 512, 16384 in all
- frame_limit: int32 [128], replicated, may hold values from 0 to 64
Outputs:
- gated_branch: bfloat16 [8192, 4096], P('seq', 'head')
The draws below stay inside these ranges and needn't reach their ends.
Inputs may be any that keep to these rules, and one draw needn't show every extreme that they name: `frame_lengths`: the lengths sum to 16384.
All inputs are finite; a program needn't handle non-finite values.
Results may differ from the reference program's by a relative error of at most 0.014.
The reference program's roundings to bfloat16 on the way count: a program that leaves them out, or rounds other values in their place, can miss the bound.
Values may be sent and summed in bfloat16 or wider, within the bound.
A program may use at most 128 MiB of HBM per device.

```python
import math
import jax
import jax.numpy as jnp
import numpy as np
from jax import lax

D = 4096
HEADS = 32
KV_HEADS = 8
HD = 128
VID_DEV = 512
TBLK = 64
GROUP = 4
TEXT = 8192
VIDEO = 16384
FRAMES = 64
TEXT_BLOCKS = 128


def draw_text_states(key, part):
    normal_draw = jax.random.normal(jax.random.fold_in(key, 11), (TEXT, D), jnp.float32)
    return jnp.clip(normal_draw, -200.0, 200.0).astype(jnp.bfloat16)


def touch_ends(drawn, stream_key, low, largest):
    spot = [jax.random.randint(jax.random.fold_in(stream_key, axis), (), 0, length) for axis, length in enumerate(drawn.shape)]
    widest = drawn.shape.index(max(drawn.shape))
    beside = spot[:widest] + [(spot[widest] + 1) % drawn.shape[widest]] + spot[widest + 1:]
    return drawn.at[tuple(spot)].set(low).at[tuple(beside)].set(largest)


def block_scale(stream_key, extent, split, smallest, largest):
    def one(position, blocks):
        heights = jax.random.uniform(jax.random.fold_in(jax.random.fold_in(stream_key, 6), position), (blocks,), jnp.float32, smallest / len(split), largest / len(split))
        return jnp.repeat(jnp.exp(heights), extent[position] // blocks).reshape((-1,) + (1,) * (len(extent) - position - 1))

    factor_of = one(*split[0])
    for cut in split[1:]:
        factor_of = factor_of * one(*cut)
    return factor_of


def length_profile(count, total, reach, lean):
    loads = [(1 << 20) // math.isqrt(standing ** lean) + 1 for standing in range(2, count + 1)]
    rest, given = total - reach - (count - 1), [1] * (count - 1)
    while rest > 0:
        free = [i for i in range(count - 1) if given[i] < reach]
        whole, remaining = sum([loads[i] for i in free]), rest
        for i in free:
            addition = min(reach - given[i], max(1, remaining * loads[i] // whole), rest)
            given[i] = given[i] + addition
            rest = rest - addition
    return np.array([reach] + given)


def uneven(rng, count, total, limit, slope):
    if count == 2:
        one = jax.random.randint(rng, (), max(1, total - limit), min(limit, total - 1) + 1)
        return jnp.stack([one, total - one])
    sizes = jnp.asarray(length_profile(count, total, limit, slope), jnp.int32)
    couples = (count - 1) // 2
    giver, sink = sizes[1:1 + 2 * couples:2], sizes[2:2 + 2 * couples:2]
    margin = jnp.minimum(giver - 1, limit - sink)
    moved = jax.random.randint(jax.random.fold_in(rng, 1), (couples,), 0, 1 << 20) % (margin + 1)
    sizes = sizes.at[1:1 + 2 * couples:2].set(giver - moved).at[2:2 + 2 * couples:2].set(sink + moved)
    return sizes[jax.random.permutation(jax.random.fold_in(rng, 2), count)]


def centred(stream_key, extent, scale, reach, cuts=(), held_as=jnp.bfloat16):
    factor_of = block_scale(stream_key, extent, cuts, -0.22, 0.18) if cuts else 1.0
    drawn = jax.random.normal(stream_key, extent, jnp.float32) * scale * factor_of
    return jnp.minimum(jnp.maximum(drawn, -reach), reach).astype(held_as)


def setup_inputs(seed: int = 0) -> dict:
    keys = jax.random.split(jax.random.key(seed), 9)
    return {
        "text_states": draw_text_states(jax.random.fold_in(keys[8], 71), 0),
        "query_weight": centred(keys[1], (D, HEADS * HD), D ** -0.5, 0.09375, ((1, 4),)),
        "image_keys": centred(keys[2], (VIDEO, KV_HEADS * HD), 2.0, 12.0, ((0, 32), (1, 4))),
        "image_values": centred(keys[3], (VIDEO, KV_HEADS * HD), 4.0, 24.0, ((0, 32), (1, 4))),
        "output_weight": centred(keys[4], (HEADS * HD, D), (HEADS * HD) ** -0.5, 0.09375, ((0, 4),)),
        "attn_gate": jnp.clip(jax.random.uniform(keys[5], (1,), jnp.float32, 0.3, 1.5), 0.3, 1.5),
        "frame_lengths": uneven(keys[6], FRAMES, VIDEO, VID_DEV, 2).astype(jnp.int32),
        "frame_limit": touch_ends(jax.random.randint(keys[7], (TEXT_BLOCKS,), 0, FRAMES + 1), jax.random.fold_in(keys[7], 1), 0, FRAMES).astype(jnp.int32),
    }


masked_fill = -1e+30

def reference(text_states, query_weight, image_keys, image_values, output_weight, attn_gate, frame_lengths, frame_limit):
    queries = jnp.dot(text_states, query_weight, preferred_element_type=jnp.float32).astype(jnp.bfloat16)
    frame_ends = jnp.cumsum(frame_lengths).astype(jnp.int32)
    token_positions = jnp.arange(VIDEO, dtype=jnp.int32)
    key_frames = lax.optimization_barrier(jnp.sum((frame_ends[None, :] <= token_positions[:, None]).astype(jnp.int32), axis=1))
    row_limits = jnp.repeat(frame_limit, TBLK)
    query_heads = queries.reshape(TEXT, HEADS, HD).transpose(1, 0, 2)
    key_head_count = image_keys.reshape(VIDEO, KV_HEADS, HD).transpose(1, 0, 2)
    value_heads = image_values.reshape(VIDEO, KV_HEADS, HD).transpose(1, 0, 2)
    score_scale = 1.0 / math.sqrt(HD)
    block_rows = TEXT // 4

    def one_block(head_no, block_no):
        head_rows = lax.dynamic_index_in_dim(query_heads, head_no, 0, keepdims=False)
        query_rows = lax.dynamic_slice_in_dim(head_rows, block_no * block_rows, block_rows, 0)
        key_rows = lax.dynamic_index_in_dim(key_head_count, head_no // GROUP, 0, keepdims=False)
        value_rows = lax.dynamic_index_in_dim(value_heads, head_no // GROUP, 0, keepdims=False)
        limits = lax.dynamic_slice_in_dim(row_limits, block_no * block_rows, block_rows, 0)
        scores = jnp.dot(query_rows, key_rows.T, preferred_element_type=jnp.float32) * score_scale
        visible = key_frames[None, :] < limits[:, None]
        best_score = lax.optimization_barrier(jnp.max(jnp.where(visible, scores, masked_fill), axis=1))
        weights = jnp.where(visible, jnp.exp(scores - best_score[:, None]), 0.0)
        weight_sum = lax.optimization_barrier(jnp.sum(weights, axis=1))
        mixed = jnp.dot(weights.astype(jnp.bfloat16), value_rows, preferred_element_type=jnp.float32)
        return (mixed / jnp.maximum(weight_sum, 1.0)[:, None]).astype(jnp.bfloat16)

    def one_head(head_no):
        blocks = lax.map(lambda block_no: one_block(head_no, block_no), jnp.arange(4, dtype=jnp.int32))
        return blocks.reshape(TEXT, HD)
    heads_out = lax.map(one_head, jnp.arange(HEADS, dtype=jnp.int32))
    attention_output = heads_out.transpose(1, 0, 2).reshape(TEXT, HEADS * HD)
    projected = jnp.dot(attention_output, output_weight, preferred_element_type=jnp.float32)
    return (jnp.tanh(attn_gate[0]) * projected).astype(jnp.bfloat16)
```

```python
import functools
import math

import jax
import jax.numpy as jnp
from jax import lax
from jax.experimental import pallas as pl
from jax.experimental.pallas import tpu as pltpu
from jax.sharding import Mesh, PartitionSpec as P

HD = 128
TBLK = 64
GROUP = 4
NEG = -1e30
C = math.log2(math.e) / math.sqrt(HD)
TK = 512
CH = 128
UN = 4
PB = 2


def attn_kernel(blocks, cnt_ref, blk_ref, tile_ref, first_ref, mask_ref, bnd_ref, q_ref, k_ref, vt_ref, o_ref, st_ref, *scr):
    S = [scr[2*u:2*u+2] for u in range(UN)]; PP = [scr[2*UN+2*u:2*UN+2*u+2] for u in range(UN)]
    m_st, l_st, al_st, acc, m_c, l_c, a_c, kx, qs = scr[4*UN:]
    n = cnt_ref[0]
    m_st[...] = jnp.full_like(m_st, NEG)
    l_st[...] = jnp.zeros_like(l_st)
    al_st[...] = jnp.zeros_like(al_st)
    acc[...] = jnp.zeros_like(acc)
    m_c[...] = jnp.full_like(m_c, NEG)
    l_c[...] = jnp.zeros_like(l_c)
    a_c[...] = jnp.zeros_like(a_c)
    for h in range(2):
        for u in range(UN): PP[u][h][...] = jnp.zeros_like(PP[u][h])
    kx[blocks] = jnp.zeros((TK, HD), jnp.bfloat16)
    io = lax.broadcasted_iota(jnp.int32, (TK, HD), 0)
    @pl.loop(0, blocks)
    def _(b):
        kx[b] = jnp.where(io < bnd_ref[b], 0.0, 1.0).astype(jnp.bfloat16)
        r = pl.multiple_of(b * TBLK, TBLK)
        for h in range(2):
            for g in range(GROUP):
                qs[b, h, g*TBLK:(g+1)*TBLK, :] = q_ref[pl.ds(r, TBLK), (h*GROUP+g)*HD:(h*GROUP+g+1)*HD]
    qx = jnp.where(lax.broadcasted_iota(jnp.int32, (256, HD), 1) == 0, NEG, 0.0).astype(jnp.bfloat16)
    kx[blocks + 1, 0:256, :] = qx
    kx[blocks + 2] = jnp.ones((TK, HD), jnp.bfloat16)

    def qk(par, i, h):
        b = blk_ref[i]; t = tile_ref[i]
        lhs = jnp.concatenate([k_ref[t, :, h*HD:(h+1)*HD], kx[mask_ref[i]]], axis=1)
        rhs = jnp.concatenate([qs[b, h], kx[blocks+1, 0:256, :]], axis=1)
        S[par][h][...] = lax.dot_general(lhs, rhs, (((1,), (1,)), ((), ())), preferred_element_type=jnp.float32)

    def pv(par, i, h, late):
        b = blk_ref[i]; t = tile_ref[i]
        r = lax.dot_general(vt_ref[t, h*HD:(h+1)*HD, :], PP[par][h][...], (((1,), (0,)), ((), ())), preferred_element_type=jnp.float32)
        new = a_c[h] * al_st[par, h] + r
        a_c[h] = new
        late.append((acc, b, h, new))

    def softmax(par, i, h, late):
        b = blk_ref[i]
        first = first_ref[i] == 1
        s_ref = S[par][h]; p_ref = PP[par][h]
        mx = None
        for c in range(TK//CH):
            s = s_ref[c*CH:(c+1)*CH, :]
            v = jnp.max(s.reshape(CH//8, 8, 256), axis=0)
            mx = v if mx is None else jnp.maximum(mx, v)
        m_prev = jnp.where(first, jnp.full((1,256),NEG,jnp.float32), m_c[h])
        m_new = jnp.maximum(m_prev, jnp.max(mx, axis=0, keepdims=True))
        m_c[h] = m_new
        alpha = jnp.exp2((m_prev - m_new) * C)
        al_st[par, h] = alpha
        ls = None
        for c in range(TK//CH):
            p = jnp.exp2((s_ref[c*CH:(c+1)*CH, :] - m_new) * C)
            v = jnp.sum(p.reshape(CH//8, 8, 256), axis=0)
            ls = v if ls is None else ls + v
            p_ref[c*CH:(c+1)*CH, :] = p.astype(jnp.bfloat16)
        l_new = l_c[h] * alpha + ls
        l_c[h] = l_new
        late.append((m_st, b, h, m_new)); late.append((l_st, b, h, l_new))

    def flush(late):
        for ref, b, h, v in late:
            ref[b, h] = v

    for u in range(PB):
        for h in range(2): qk(u, PB+u, h)
    def block(base, i):
        late = []
        us = [(u, h) for u in range(PB) for h in range(2)]
        for u, h in us: qk((base+u+PB)%UN, i+u+PB, h)
        for u, h in us: pv((base+u-PB)%UN, i+u-PB, h, late)
        for u, h in us: softmax((base+u)%UN, i+u, h, late)
        flush(late)
    R = UN // PB
    def tail(base, i):
        late = []
        for u in range(PB):
            for h in range(2): pv((base+u)%UN, i+u, h, late)
        flush(late)
    @pl.loop(0, lax.div(n + R, R))
    def _(j):
        for r in range(R):
            step = j * R + r
            @pl.when(step < n)
            def _():
                block(r*PB, (step+1) * PB)
            @pl.when(step == n)
            def _():
                tail(((r-1)*PB)%UN, step * PB)
    @pl.loop(0, blocks)
    def _(b):
        for h in range(2):
            l = jnp.sum(l_st[b, h], axis=0, keepdims=True)
            o_ref[b, h] = (acc[b, h] / jnp.maximum(l, 1.0)).astype(jnp.bfloat16)
            st_ref[b, h, 0:1, :] = m_st[b, h]
            st_ref[b, h, 1:2, :] = l

def tables(nvis, NT):
    blocks = nvis.shape[0]
    tiles = (nvis + TK - 1)//TK
    ends = jnp.cumsum(tiles)
    starts = ends - tiles
    N = blocks*NT
    total = ends[-1]
    idx = jnp.arange(-PB, N+3*PB, dtype=jnp.int32)
    ii = jnp.clip(idx, 0, jnp.maximum(total-1, 0))
    blk = jnp.minimum(jnp.sum((ends[None,:] <= ii[:,None]).astype(jnp.int32), axis=1), blocks-1)
    sel = (jnp.arange(blocks)[None,:]==blk[:,None]).astype(jnp.int32)
    tile = jnp.clip(ii - jnp.sum(sel*starts[None,:],axis=1), 0, NT-1)
    real = idx < total
    rem = jnp.sum(sel*nvis[None,:],axis=1) - tile*TK
    mask = jnp.where(real, jnp.where(rem < TK, blk, blocks), blocks + 2)
    first = jnp.where(real & (tile == 0) & (idx >= 0), 1, 0)
    bnd = nvis - jnp.maximum(tiles - 1, 0)*TK
    return ((total + PB-1)//PB).reshape(1).astype(jnp.int32), blk, tile, first, mask, bnd

def attention(nvis, q, k, vt):
    blocks = nvis.shape[0]
    NT = k.shape[0]
    sm = pl.BlockSpec(memory_space=pltpu.SMEM); vm = pl.BlockSpec(memory_space=pltpu.VMEM)
    return pl.pallas_call(
        functools.partial(attn_kernel, blocks),
        out_shape=(jax.ShapeDtypeStruct((blocks,2,HD,256), jnp.bfloat16), jax.ShapeDtypeStruct((blocks,2,2,256), jnp.float32)),
        in_specs=[sm]*6+[vm]*3, out_specs=(vm,vm),
        scratch_shapes=[pltpu.VMEM((TK,256),jnp.float32)]*(2*UN) + [pltpu.VMEM((TK,256),jnp.bfloat16)]*(2*UN) + [
            pltpu.VMEM((blocks,2,1,256),jnp.float32), pltpu.VMEM((blocks,2,8,256),jnp.float32), pltpu.VMEM((UN,2,1,256),jnp.float32), pltpu.VMEM((blocks,2,HD,256),jnp.float32), pltpu.VMEM((2,1,256),jnp.float32), pltpu.VMEM((2,8,256),jnp.float32), pltpu.VMEM((2,HD,256),jnp.float32),
            pltpu.VMEM((blocks+3,TK,HD),jnp.bfloat16), pltpu.VMEM((blocks,2,256,HD),jnp.bfloat16)],
        compiler_params=pltpu.CompilerParams(vmem_limit_bytes=60*1024*1024),
        cost_estimate=pl.CostEstimate(flops=10**10, bytes_accessed=10**7, transcendentals=10**7),
    )(*tables(nvis, NT), q, k, vt)


def shards(text, wq, keys, values, wo, gate, lengths, limits):
    xi = lax.axis_index("x")
    group = lax.axis_index("zl") * 4 + lax.axis_index("y")
    rows = text.shape[0]
    heads = ("zh", "core")
    k_all = lax.all_gather(keys, ("zl", "y"))
    vt_all = lax.all_gather(values.T, ("zl", "y"))
    text_all = lax.all_gather(text, heads, axis=1, tiled=True)
    q = jnp.dot(text_all, wq, preferred_element_type=jnp.float32).astype(jnp.bfloat16)
    q_all = lax.all_gather(q, "x", axis=0, tiled=True)
    blocks = 4 * rows // TBLK
    ends = jnp.cumsum(lengths)
    lim = lax.dynamic_slice_in_dim(limits, group * blocks, blocks, 0)
    seen = jnp.sum(jnp.where(jnp.arange(lengths.shape[0])[None, :] < lim[:, None], lengths[None, :], 0), axis=1)
    first_token = (jnp.arange(8) * 4 + xi) * keys.shape[0]
    nvis = jnp.sum(jnp.clip(seen[:, None] - first_token[None, :], 0, keys.shape[0]), axis=1).astype(jnp.int32)
    o, st = attention(nvis, q_all, k_all, vt_all)
    o = lax.all_to_all(o, "x", 0, 0, tiled=True)
    st = lax.all_to_all(st, "x", 0, 0, tiled=True)
    b = rows // TBLK
    o = o.reshape(4, b, 2, HD, 4 * TBLK).astype(jnp.float32)
    st = st.reshape(4, b, 2, 2, 4 * TBLK)
    m, l = st[:, :, :, 0], st[:, :, :, 1]
    share = l * jnp.exp2((m - jnp.max(m, axis=0)) * C)
    total = jnp.maximum(jnp.sum(share, axis=0), 1.0)
    mixed = jnp.sum(o * (share / total)[:, :, :, None, :], axis=0).astype(jnp.bfloat16)
    attn = mixed.reshape(b, 2, HD, GROUP, TBLK).transpose(0, 4, 1, 3, 2).reshape(rows, -1)
    part = jnp.dot(attn, wo, preferred_element_type=jnp.float32).astype(jnp.bfloat16)
    part = part.reshape(rows, 4, -1).transpose(1, 0, 2)
    got = lax.all_to_all(part, heads, 0, 0, tiled=True)
    return (jnp.tanh(gate[0]) * got.astype(jnp.float32).sum(axis=0)).astype(jnp.bfloat16)


def solution(mesh):
    mesh = Mesh(mesh.devices.reshape(2, 4, 4, 2, 2), ("zl", "y", "x", "zh", "core"))
    seq, head = ("zl", "y", "x"), ("zh", "core")
    in_specs = (P(seq, head), P(None, head), P(seq, head), P(seq, head), P(head, None), P(), P(), P())
    return jax.shard_map(shards, mesh=mesh, in_specs=in_specs, out_specs=P(seq, head), check_vma=False)
```

```python
import functools
import math

import jax
import jax.numpy as jnp
from jax import lax
from jax.experimental import pallas as pl
from jax.experimental.pallas import tpu as pltpu
from jax.sharding import Mesh, PartitionSpec as P

HD = 128
TBLK = 64
GROUP = 4
NEG = -1e30
C = math.log2(math.e) / math.sqrt(HD)
TK = 512
CH = 128
UN = 4
PB = 2


def attn_kernel(blocks, cnt_ref, blk_ref, tile_ref, first_ref, mask_ref, bnd_ref, q_ref, k_ref, vt_ref, o_ref, st_ref, *scr):
    S = [scr[2*u:2*u+2] for u in range(UN)]; PP = [scr[2*UN+2*u:2*UN+2*u+2] for u in range(UN)]
    m_st, l_st, al_st, acc, m_c, l_c, a_c, kx, qs = scr[4*UN:]
    n = cnt_ref[0]
    m_st[...] = jnp.full_like(m_st, NEG)
    l_st[...] = jnp.zeros_like(l_st)
    al_st[...] = jnp.zeros_like(al_st)
    acc[...] = jnp.zeros_like(acc)
    m_c[...] = jnp.full_like(m_c, NEG)
    l_c[...] = jnp.zeros_like(l_c)
    a_c[...] = jnp.zeros_like(a_c)
    for h in range(2):
        for u in range(UN): PP[u][h][...] = jnp.zeros_like(PP[u][h])
    kx[blocks] = jnp.zeros((TK, HD), jnp.bfloat16)
    io = lax.broadcasted_iota(jnp.int32, (TK, HD), 0)
    @pl.loop(0, blocks)
    def _(b):
        kx[b] = jnp.where(io < bnd_ref[b], 0.0, 1.0).astype(jnp.bfloat16)
        r = pl.multiple_of(b * TBLK, TBLK)
        for h in range(2):
            for g in range(GROUP):
                qs[b, h, g*TBLK:(g+1)*TBLK, :] = q_ref[pl.ds(r, TBLK), (h*GROUP+g)*HD:(h*GROUP+g+1)*HD]
    qx = jnp.where(lax.broadcasted_iota(jnp.int32, (256, HD), 1) == 0, NEG, 0.0).astype(jnp.bfloat16)
    kx[blocks + 1, 0:256, :] = qx
    kx[blocks + 2] = jnp.ones((TK, HD), jnp.bfloat16)

    def qk(par, i, h):
        b = blk_ref[i]; t = tile_ref[i]
        lhs = jnp.concatenate([k_ref[t, :, h*HD:(h+1)*HD], kx[mask_ref[i]]], axis=1)
        rhs = jnp.concatenate([qs[b, h], kx[blocks+1, 0:256, :]], axis=1)
        S[par][h][...] = lax.dot_general(lhs, rhs, (((1,), (1,)), ((), ())), preferred_element_type=jnp.float32)

    def pv(par, i, h, late):
        b = blk_ref[i]; t = tile_ref[i]
        r = lax.dot_general(vt_ref[t, h*HD:(h+1)*HD, :], PP[par][h][...], (((1,), (0,)), ((), ())), preferred_element_type=jnp.float32)
        new = a_c[h] * al_st[par, h] + r
        a_c[h] = new
        late.append((acc, b, h, new))

    def softmax(par, i, h, late):
        b = blk_ref[i]
        first = first_ref[i] == 1
        s_ref = S[par][h]; p_ref = PP[par][h]
        mx = None
        for c in range(TK//CH):
            s = s_ref[c*CH:(c+1)*CH, :]
            v = jnp.max(s.reshape(CH//8, 8, 256), axis=0)
            mx = v if mx is None else jnp.maximum(mx, v)
        m_prev = jnp.where(first, jnp.full((1,256),NEG,jnp.float32), m_c[h])
        m_new = jnp.maximum(m_prev, jnp.max(mx, axis=0, keepdims=True))
        m_c[h] = m_new
        alpha = jnp.exp2((m_prev - m_new) * C)
        al_st[par, h] = alpha
        ls = None
        for c in range(TK//CH):
            p = jnp.exp2((s_ref[c*CH:(c+1)*CH, :] - m_new) * C)
            v = jnp.sum(p.reshape(CH//8, 8, 256), axis=0)
            ls = v if ls is None else ls + v
            p_ref[c*CH:(c+1)*CH, :] = p.astype(jnp.bfloat16)
        l_new = l_c[h] * alpha + ls
        l_c[h] = l_new
        late.append((m_st, b, h, m_new)); late.append((l_st, b, h, l_new))

    def flush(late):
        for ref, b, h, v in late:
            ref[b, h] = v

    for u in range(PB):
        for h in range(2): qk(u, PB+u, h)
    def block(base, i):
        late = []
        us = [(u, h) for u in range(PB) for h in range(2)]
        for u, h in us: qk((base+u+PB)%UN, i+u+PB, h)
        for u, h in us: pv((base+u-PB)%UN, i+u-PB, h, late)
        for u, h in us: softmax((base+u)%UN, i+u, h, late)
        flush(late)
    R = UN // PB
    def tail(base, i):
        late = []
        for u in range(PB):
            for h in range(2): pv((base+u)%UN, i+u, h, late)
        flush(late)
    @pl.loop(0, lax.div(n + R, R))
    def _(j):
        for r in range(R):
            step = j * R + r
            @pl.when(step < n)
            def _():
                block(r*PB, (step+1) * PB)
            @pl.when(step == n)
            def _():
                tail(((r-1)*PB)%UN, step * PB)
    @pl.loop(0, blocks)
    def _(b):
        for h in range(2):
            l = jnp.sum(l_st[b, h], axis=0, keepdims=True)
            o_ref[b, h] = (acc[b, h] / jnp.maximum(l, 1.0)).astype(jnp.bfloat16)
            st_ref[b, h, 0:1, :] = m_st[b, h]
            st_ref[b, h, 1:2, :] = l

def tables(nvis, NT):
    blocks = nvis.shape[0]
    tiles = (nvis + TK - 1)//TK
    ends = jnp.cumsum(tiles)
    starts = ends - tiles
    N = blocks*NT
    total = ends[-1]
    idx = jnp.arange(-PB, N+3*PB, dtype=jnp.int32)
    ii = jnp.clip(idx, 0, jnp.maximum(total-1, 0))
    blk = jnp.minimum(jnp.sum((ends[None,:] <= ii[:,None]).astype(jnp.int32), axis=1), blocks-1)
    sel = (jnp.arange(blocks)[None,:]==blk[:,None]).astype(jnp.int32)
    tile = jnp.clip(ii - jnp.sum(sel*starts[None,:],axis=1), 0, NT-1)
    real = idx < total
    rem = jnp.sum(sel*nvis[None,:],axis=1) - tile*TK
    mask = jnp.where(real, jnp.where(rem < TK, blk, blocks), blocks + 2)
    first = jnp.where(real & (tile == 0) & (idx >= 0), 1, 0)
    bnd = nvis - jnp.maximum(tiles - 1, 0)*TK
    return ((total + PB-1)//PB).reshape(1).astype(jnp.int32), blk, tile, first, mask, bnd

def attention(nvis, q, k, vt):
    blocks = nvis.shape[0]
    NT = k.shape[0]
    sm = pl.BlockSpec(memory_space=pltpu.SMEM); vm = pl.BlockSpec(memory_space=pltpu.VMEM)
    return pl.pallas_call(
        functools.partial(attn_kernel, blocks),
        out_shape=(jax.ShapeDtypeStruct((blocks,2,HD,256), jnp.bfloat16), jax.ShapeDtypeStruct((blocks,2,2,256), jnp.float32)),
        in_specs=[sm]*6+[vm]*3, out_specs=(vm,vm),
        scratch_shapes=[pltpu.VMEM((TK,256),jnp.float32)]*(2*UN) + [pltpu.VMEM((TK,256),jnp.bfloat16)]*(2*UN) + [
            pltpu.VMEM((blocks,2,1,256),jnp.float32), pltpu.VMEM((blocks,2,8,256),jnp.float32), pltpu.VMEM((UN,2,1,256),jnp.float32), pltpu.VMEM((blocks,2,HD,256),jnp.float32), pltpu.VMEM((2,1,256),jnp.float32), pltpu.VMEM((2,8,256),jnp.float32), pltpu.VMEM((2,HD,256),jnp.float32),
            pltpu.VMEM((blocks+3,TK,HD),jnp.bfloat16), pltpu.VMEM((blocks,2,256,HD),jnp.bfloat16)],
        compiler_params=pltpu.CompilerParams(vmem_limit_bytes=60*1024*1024),
        cost_estimate=pl.CostEstimate(flops=10**10, bytes_accessed=10**7, transcendentals=10**7),
    )(*tables(nvis, NT), q, k, vt)


MESH_ID = pl.DeviceIdType.MESH


def gather_kernel(text_ref, k_ref, vt_ref, wq_hbm, q_all, k_all, vt_all, tx, relay, wq, part, wq_sem,
                  t1s, t1r, t2s, t2r, t3s, t3r, t4s, t4r, ks, kr, qs_, qr):
    zl, y, x = lax.axis_index("zl"), lax.axis_index("y"), lax.axis_index("x")
    zh, core = lax.axis_index("zh"), lax.axis_index("core")
    inner = {"zl": 1 - zl}
    outer = {"zh": 1 - zh, "zl": 1 - zl}
    other = {"core": 1 - core}
    yp, ym = {"y": lax.rem(y + 1, 4)}, {"y": lax.rem(y + 3, 4)}
    xp, xm = {"x": lax.rem(x + 1, 4)}, {"x": lax.rem(x + 3, 4)}

    load = pltpu.make_async_copy(wq_hbm, wq, wq_sem)
    load.start()
    barrier = pltpu.get_barrier_semaphore()
    for peer in (inner, outer, other, yp, ym, xp, xm):
        pl.semaphore_signal(barrier, inc=1, device_id=peer, device_id_type=MESH_ID)
    pl.semaphore_wait(barrier, 7)

    def copy(src, dst, ssem, rsem, dev):
        return pltpu.make_async_remote_copy(src_ref=src, dst_ref=dst, send_sem=ssem, recv_sem=rsem,
                                            device_id=dev, device_id_type=MESH_ID)

    rows = text_ref.shape[0]
    step = rows // 4
    piece = [pl.ds(p * step, step) for p in range(4)]
    started = []

    def go(c):
        c.start()
        started.append(c)
        return c

    t1 = [go(copy(text_ref.at[piece[p]], relay.at[p], t1s.at[p], t1r.at[p], outer if p % 2 else inner)) for p in (1, 0, 3, 2)]
    t1 = {p: c for p, c in zip((1, 0, 3, 2), t1)}
    t3 = go(copy(text_ref, tx.at[1], t3s, t3r, other))
    c_me = zl * 4 + y
    c_in = (1 - zl) * 4 + y
    c_m, c_p = zl * 4 + lax.rem(y + 3, 4), zl * 4 + lax.rem(y + 1, 4)
    cz_m, cz_p = (1 - zl) * 4 + lax.rem(y + 3, 4), (1 - zl) * 4 + lax.rem(y + 1, 4)
    K = lambda c: k_all.at[c]
    V = lambda c: vt_all.at[c]
    sem = iter(range(14))

    def kv(src, dst, dev):
        i = next(sem)
        return go(copy(src, dst, ks.at[i], kr.at[i], dev))

    a_kp = kv(k_ref, K(c_me), yp)
    a_vm = kv(vt_ref, V(c_me), ym)
    a_vp = kv(vt_ref, V(c_me), yp)
    a_km = kv(k_ref, K(c_me), ym)
    k_all[c_me] = k_ref[...]
    vt_all[c_me] = vt_ref[...]
    t2 = {}
    for p in (1, 0, 3, 2):
        t1[p].wait_recv()
        t2[p] = go(copy(relay.at[p], tx.at[2, piece[p]], t2s.at[p], t2r.at[p], inner if p % 2 else outer))
    z_k = kv(k_ref, K(c_me), inner)
    z_v = kv(vt_ref, V(c_me), inner)
    a_kp.wait_recv()
    f_k = kv(K(c_m), K(c_m), yp)
    a_vm.wait_recv()
    f_v = kv(V(c_p), V(c_p), ym)

    NT = 256
    half = rows // 2

    def project(src, slot, h, first, last):
        r = pl.ds(h * half, half)

        @pl.loop(0, wq.shape[2] // NT)
        def _(n):
            cols = pl.ds(pl.multiple_of(n * NT, NT), NT)
            d = jnp.dot(src[0][r, :], wq[slot[0], :, cols], preferred_element_type=jnp.float32)
            d = d + jnp.dot(src[1][r, :], wq[slot[1], :, cols], preferred_element_type=jnp.float32)
            if not first:
                d = d + part[r, cols]
            if last:
                q_all[x, r, cols] = d.astype(jnp.bfloat16)
            else:
                part[r, cols] = d

    load.wait()
    t3.wait_recv()
    mine = zh * 2 + core
    beside = zh * 2 + 1 - core
    far = (1 - zh) * 2 + core
    far_beside = (1 - zh) * 2 + 1 - core
    for h in range(2):
        project((text_ref, tx.at[1]), (mine, beside), h, True, False)
    t4 = {}
    for p in (1, 0, 3, 2):
        t2[p].wait_recv()
        t4[p] = go(copy(tx.at[2, piece[p]], tx.at[3, piece[p]], t4s.at[p], t4r.at[p], other))
    halves = [pl.ds(h * half, half) for h in range(2)]
    q = {}

    def qcopy(i, src_x, h, dev):
        ref = q_all.at[src_x, halves[h]]
        return go(copy(ref, ref, qs_.at[i], qr.at[i], dev))

    for h in range(2):
        for p in (2 * h, 2 * h + 1):
            t4[p].wait_recv()
        project((tx.at[2], tx.at[3]), (far, far_beside), h, False, True)
        q[h, 1] = qcopy(2 * h, x, h, xp)
        q[h, -1] = qcopy(2 * h + 1, x, h, xm)
    z_k.wait_recv()
    b_kp = kv(K(c_in), K(c_in), yp)
    b_km = kv(K(c_in), K(c_in), ym)
    q[0, 1].wait_recv()
    q_f = qcopy(4, lax.rem(x + 3, 4), 0, xp)
    z_v.wait_recv()
    b_vm = kv(V(c_in), V(c_in), ym)
    b_vp = kv(V(c_in), V(c_in), yp)
    q[1, -1].wait_recv()
    q_b = qcopy(5, lax.rem(x + 1, 4), 1, xm)
    b_kp.wait_recv()
    g_k = kv(K(cz_m), K(cz_m), yp)
    b_vm.wait_recv()
    g_v = kv(V(cz_p), V(cz_p), ym)
    for c in (a_vp, a_km, f_k, f_v, q[0, -1], q[1, 1], q_f, q_b, b_km, b_vp, g_k, g_v):
        c.wait_recv()
    for c in started:
        c.wait_send()


def gather_all(text, keys, values_t, wq):
    rows, width = text.shape
    bf = jnp.bfloat16
    vm = pl.BlockSpec(memory_space=pltpu.VMEM)
    dma = pltpu.SemaphoreType.DMA
    return pl.pallas_call(
        gather_kernel,
        out_shape=(
            jax.ShapeDtypeStruct((4, rows, wq.shape[1]), bf),
            jax.ShapeDtypeStruct((8, *keys.shape), bf),
            jax.ShapeDtypeStruct((8, *values_t.shape), bf),
        ),
        in_specs=[vm, vm, vm, pl.BlockSpec(memory_space=pl.ANY)],
        out_specs=(vm, vm, vm),
        scratch_shapes=[
            pltpu.VMEM((4, rows, width), bf),
            pltpu.VMEM((4, rows // 4, width), bf),
            pltpu.VMEM((4, width, wq.shape[1]), bf),
            pltpu.VMEM((rows, wq.shape[1]), jnp.float32),
            dma, dma((4,)), dma((4,)), dma((4,)), dma((4,)), dma, dma, dma((4,)), dma((4,)), dma((14,)), dma((14,)), dma((6,)), dma((6,)),
        ],
        compiler_params=pltpu.CompilerParams(collective_id=0, has_side_effects=True, vmem_limit_bytes=48 * 1024 * 1024),
        cost_estimate=pl.CostEstimate(flops=2 * rows * 4 * width * wq.shape[1], bytes_accessed=20 * 2**20, transcendentals=0),
        name="gather",
    )(text, keys, values_t, wq.reshape(4, width, wq.shape[1]))


def shards(text, wq, keys, values, wo, gate, lengths, limits):
    xi = lax.axis_index("x")
    group = lax.axis_index("zl") * 4 + lax.axis_index("y")
    rows = text.shape[0]
    q_all, k_all, vt_all = gather_all(text, keys, values.T, wq)
    q_all = q_all.reshape(4 * rows, -1)
    blocks = 4 * rows // TBLK
    ends = jnp.cumsum(lengths)
    lim = lax.dynamic_slice_in_dim(limits, group * blocks, blocks, 0)
    seen = jnp.sum(jnp.where(jnp.arange(lengths.shape[0])[None, :] < lim[:, None], lengths[None, :], 0), axis=1)
    first_token = (jnp.arange(8) * 4 + xi) * keys.shape[0]
    nvis = jnp.sum(jnp.clip(seen[:, None] - first_token[None, :], 0, keys.shape[0]), axis=1).astype(jnp.int32)
    o, st = attention(nvis, q_all, k_all, vt_all)
    o = lax.all_to_all(o, "x", 0, 0, tiled=True)
    st = lax.all_to_all(st, "x", 0, 0, tiled=True)
    b = rows // TBLK
    o = o.reshape(4, b, 2, HD, 4 * TBLK).astype(jnp.float32)
    st = st.reshape(4, b, 2, 2, 4 * TBLK)
    m, l = st[:, :, :, 0], st[:, :, :, 1]
    share = l * jnp.exp2((m - jnp.max(m, axis=0)) * C)
    total = jnp.maximum(jnp.sum(share, axis=0), 1.0)
    mixed = jnp.sum(o * (share / total)[:, :, :, None, :], axis=0).astype(jnp.bfloat16)
    attn = mixed.reshape(b, 2, HD, GROUP, TBLK).transpose(0, 4, 1, 3, 2).reshape(rows, -1)
    part = jnp.dot(attn, wo, preferred_element_type=jnp.float32).astype(jnp.bfloat16)
    part = part.reshape(rows, 4, -1).transpose(1, 0, 2)
    got = lax.all_to_all(part, ("zh", "core"), 0, 0, tiled=True)
    return (jnp.tanh(gate[0]) * got.astype(jnp.float32).sum(axis=0)).astype(jnp.bfloat16)


def solution(mesh):
    mesh = Mesh(mesh.devices.reshape(2, 4, 4, 2, 2), ("zl", "y", "x", "zh", "core"))
    seq, head = ("zl", "y", "x"), ("zh", "core")
    in_specs = (P(seq, head), P(None, head), P(seq, head), P(seq, head), P(head, None), P(), P(), P())
    return jax.shard_map(shards, mesh=mesh, in_specs=in_specs, out_specs=P(seq, head), check_vma=False)
```

```python
import functools
import math

import jax
import jax.numpy as jnp
from jax import lax
from jax.experimental import pallas as pl
from jax.experimental.pallas import tpu as pltpu
from jax.sharding import Mesh, PartitionSpec as P

HD = 128
TBLK = 64
GROUP = 4
NEG = -1e30
C = math.log2(math.e) / math.sqrt(HD)
TK = 512
CH = 128
UN = 4
PB = 2


def attn_kernel(blocks, cnt_ref, blk_ref, tile_ref, first_ref, mask_ref, bnd_ref, q_ref, k_ref, vt_ref, o_ref, st_ref, *scr):
    S = [scr[2*u:2*u+2] for u in range(UN)]; PP = [scr[2*UN+2*u:2*UN+2*u+2] for u in range(UN)]
    m_st, l_st, al_st, acc, m_c, l_c, a_c, kx, qs = scr[4*UN:]
    n = cnt_ref[0]
    m_st[...] = jnp.full_like(m_st, NEG)
    l_st[...] = jnp.zeros_like(l_st)
    al_st[...] = jnp.zeros_like(al_st)
    acc[...] = jnp.zeros_like(acc)
    m_c[...] = jnp.full_like(m_c, NEG)
    l_c[...] = jnp.zeros_like(l_c)
    a_c[...] = jnp.zeros_like(a_c)
    for h in range(2):
        for u in range(UN): PP[u][h][...] = jnp.zeros_like(PP[u][h])
    kx[blocks] = jnp.zeros((TK, HD), jnp.bfloat16)
    io = lax.broadcasted_iota(jnp.int32, (TK, HD), 0)
    @pl.loop(0, blocks)
    def _(b):
        kx[b] = jnp.where(io < bnd_ref[b], 0.0, 1.0).astype(jnp.bfloat16)
        r = pl.multiple_of(b * TBLK, TBLK)
        for h in range(2):
            for g in range(GROUP):
                qs[b, h, g*TBLK:(g+1)*TBLK, :] = q_ref[pl.ds(r, TBLK), (h*GROUP+g)*HD:(h*GROUP+g+1)*HD]
    qx = jnp.where(lax.broadcasted_iota(jnp.int32, (256, HD), 1) == 0, NEG, 0.0).astype(jnp.bfloat16)
    kx[blocks + 1, 0:256, :] = qx
    kx[blocks + 2] = jnp.ones((TK, HD), jnp.bfloat16)

    def qk(par, i, h):
        b = blk_ref[i]; t = tile_ref[i]
        lhs = jnp.concatenate([k_ref[t, :, h*HD:(h+1)*HD], kx[mask_ref[i]]], axis=1)
        rhs = jnp.concatenate([qs[b, h], kx[blocks+1, 0:256, :]], axis=1)
        S[par][h][...] = lax.dot_general(lhs, rhs, (((1,), (1,)), ((), ())), preferred_element_type=jnp.float32)

    def pv(par, i, h, late):
        b = blk_ref[i]; t = tile_ref[i]
        r = lax.dot_general(vt_ref[t, h*HD:(h+1)*HD, :], PP[par][h][...], (((1,), (0,)), ((), ())), preferred_element_type=jnp.float32)
        new = a_c[h] * al_st[par, h] + r
        a_c[h] = new
        late.append((acc, b, h, new))

    def softmax(par, i, h, late):
        b = blk_ref[i]
        first = first_ref[i] == 1
        s_ref = S[par][h]; p_ref = PP[par][h]
        mx = None
        for c in range(TK//CH):
            s = s_ref[c*CH:(c+1)*CH, :]
            v = jnp.max(s.reshape(CH//8, 8, 256), axis=0)
            mx = v if mx is None else jnp.maximum(mx, v)
        m_prev = jnp.where(first, jnp.full((1,256),NEG,jnp.float32), m_c[h])
        m_new = jnp.maximum(m_prev, jnp.max(mx, axis=0, keepdims=True))
        m_c[h] = m_new
        alpha = jnp.exp2((m_prev - m_new) * C)
        al_st[par, h] = alpha
        ls = None
        for c in range(TK//CH):
            p = jnp.exp2((s_ref[c*CH:(c+1)*CH, :] - m_new) * C)
            v = jnp.sum(p.reshape(CH//8, 8, 256), axis=0)
            ls = v if ls is None else ls + v
            p_ref[c*CH:(c+1)*CH, :] = p.astype(jnp.bfloat16)
        l_new = l_c[h] * alpha + ls
        l_c[h] = l_new
        late.append((m_st, b, h, m_new)); late.append((l_st, b, h, l_new))

    def flush(late):
        for ref, b, h, v in late:
            ref[b, h] = v

    for u in range(PB):
        for h in range(2): qk(u, PB+u, h)
    def block(base, i):
        late = []
        us = [(u, h) for u in range(PB) for h in range(2)]
        for u, h in us: qk((base+u+PB)%UN, i+u+PB, h)
        for u, h in us: pv((base+u-PB)%UN, i+u-PB, h, late)
        for u, h in us: softmax((base+u)%UN, i+u, h, late)
        flush(late)
    R = UN // PB
    def tail(base, i):
        late = []
        for u in range(PB):
            for h in range(2): pv((base+u)%UN, i+u, h, late)
        flush(late)
    @pl.loop(0, lax.div(n + R, R))
    def _(j):
        for r in range(R):
            step = j * R + r
            @pl.when(step < n)
            def _():
                block(r*PB, (step+1) * PB)
            @pl.when(step == n)
            def _():
                tail(((r-1)*PB)%UN, step * PB)
    @pl.loop(0, blocks)
    def _(b):
        for h in range(2):
            l = jnp.sum(l_st[b, h], axis=0, keepdims=True)
            o_ref[b, h] = (acc[b, h] / jnp.maximum(l, 1.0)).astype(jnp.bfloat16)
            st_ref[b, h, 0:1, :] = m_st[b, h]
            st_ref[b, h, 1:2, :] = l

def tables(nvis, NT):
    blocks = nvis.shape[0]
    tiles = (nvis + TK - 1)//TK
    ends = jnp.cumsum(tiles)
    starts = ends - tiles
    N = blocks*NT
    total = ends[-1]
    idx = jnp.arange(-PB, N+3*PB, dtype=jnp.int32)
    ii = jnp.clip(idx, 0, jnp.maximum(total-1, 0))
    blk = jnp.minimum(jnp.sum((ends[None,:] <= ii[:,None]).astype(jnp.int32), axis=1), blocks-1)
    sel = (jnp.arange(blocks)[None,:]==blk[:,None]).astype(jnp.int32)
    tile = jnp.clip(ii - jnp.sum(sel*starts[None,:],axis=1), 0, NT-1)
    real = idx < total
    rem = jnp.sum(sel*nvis[None,:],axis=1) - tile*TK
    mask = jnp.where(real, jnp.where(rem < TK, blk, blocks), blocks + 2)
    first = jnp.where(real & (tile == 0) & (idx >= 0), 1, 0)
    bnd = nvis - jnp.maximum(tiles - 1, 0)*TK
    return ((total + PB-1)//PB).reshape(1).astype(jnp.int32), blk, tile, first, mask, bnd

def attention(nvis, q, k, vt):
    blocks = nvis.shape[0]
    NT = k.shape[0]
    sm = pl.BlockSpec(memory_space=pltpu.SMEM); vm = pl.BlockSpec(memory_space=pltpu.VMEM)
    return pl.pallas_call(
        functools.partial(attn_kernel, blocks),
        out_shape=(jax.ShapeDtypeStruct((blocks,2,HD,256), jnp.bfloat16), jax.ShapeDtypeStruct((blocks,2,2,256), jnp.float32)),
        in_specs=[sm]*6+[vm]*3, out_specs=(vm,vm),
        scratch_shapes=[pltpu.VMEM((TK,256),jnp.float32)]*(2*UN) + [pltpu.VMEM((TK,256),jnp.bfloat16)]*(2*UN) + [
            pltpu.VMEM((blocks,2,1,256),jnp.float32), pltpu.VMEM((blocks,2,8,256),jnp.float32), pltpu.VMEM((UN,2,1,256),jnp.float32), pltpu.VMEM((blocks,2,HD,256),jnp.float32), pltpu.VMEM((2,1,256),jnp.float32), pltpu.VMEM((2,8,256),jnp.float32), pltpu.VMEM((2,HD,256),jnp.float32),
            pltpu.VMEM((blocks+3,TK,HD),jnp.bfloat16), pltpu.VMEM((blocks,2,256,HD),jnp.bfloat16)],
        compiler_params=pltpu.CompilerParams(vmem_limit_bytes=60*1024*1024),
        cost_estimate=pl.CostEstimate(flops=10**10, bytes_accessed=10**7, transcendentals=10**7),
    )(*tables(nvis, NT), q, k, vt)


MESH_ID = pl.DeviceIdType.MESH


def gather_kernel(text_ref, k_ref, vt_ref, wq_hbm, q_all, k_all, vt_all, tx, relay, wq, part, wq_sem,
                  t1s, t1r, t2s, t2r, t3s, t3r, t4s, t4r, ks, kr, qs_, qr):
    zl, y, x = lax.axis_index("zl"), lax.axis_index("y"), lax.axis_index("x")
    zh, core = lax.axis_index("zh"), lax.axis_index("core")
    inner = {"zl": 1 - zl}
    outer = {"zh": 1 - zh, "zl": 1 - zl}
    other = {"core": 1 - core}
    yp, ym = {"y": lax.rem(y + 1, 4)}, {"y": lax.rem(y + 3, 4)}
    xp, xm = {"x": lax.rem(x + 1, 4)}, {"x": lax.rem(x + 3, 4)}

    load = pltpu.make_async_copy(wq_hbm, wq, wq_sem)
    load.start()
    barrier = pltpu.get_barrier_semaphore()
    for peer in (inner, outer, other, yp, ym, xp, xm):
        pl.semaphore_signal(barrier, inc=1, device_id=peer, device_id_type=MESH_ID)
    pl.semaphore_wait(barrier, 7)

    def copy(src, dst, ssem, rsem, dev):
        return pltpu.make_async_remote_copy(src_ref=src, dst_ref=dst, send_sem=ssem, recv_sem=rsem,
                                            device_id=dev, device_id_type=MESH_ID)

    rows = text_ref.shape[0]
    step = rows // 4
    piece = [pl.ds(p * step, step) for p in range(4)]
    started = []

    def go(c):
        c.start()
        started.append(c)
        return c

    t1 = [go(copy(text_ref.at[piece[p]], relay.at[p], t1s.at[p], t1r.at[p], outer if p % 2 else inner)) for p in (1, 0, 3, 2)]
    t1 = {p: c for p, c in zip((1, 0, 3, 2), t1)}
    t3 = go(copy(text_ref, tx.at[1], t3s, t3r, other))
    c_me = zl * 4 + y
    c_in = (1 - zl) * 4 + y
    c_m, c_p = zl * 4 + lax.rem(y + 3, 4), zl * 4 + lax.rem(y + 1, 4)
    cz_m, cz_p = (1 - zl) * 4 + lax.rem(y + 3, 4), (1 - zl) * 4 + lax.rem(y + 1, 4)
    K = lambda c: k_all.at[c]
    V = lambda c: vt_all.at[c]
    sem = iter(range(14))

    def kv(src, dst, dev):
        i = next(sem)
        return go(copy(src, dst, ks.at[i], kr.at[i], dev))

    a_kp = kv(k_ref, K(c_me), yp)
    a_vm = kv(vt_ref, V(c_me), ym)
    a_vp = kv(vt_ref, V(c_me), yp)
    a_km = kv(k_ref, K(c_me), ym)
    k_all[c_me] = k_ref[...]
    vt_all[c_me] = vt_ref[...]
    t2 = {}
    for p in (1, 0, 3, 2):
        t1[p].wait_recv()
        t2[p] = go(copy(relay.at[p], tx.at[2, piece[p]], t2s.at[p], t2r.at[p], inner if p % 2 else outer))
    z_k = kv(k_ref, K(c_me), inner)
    z_v = kv(vt_ref, V(c_me), inner)
    a_kp.wait_recv()
    f_k = kv(K(c_m), K(c_m), yp)
    a_vm.wait_recv()
    f_v = kv(V(c_p), V(c_p), ym)

    NT = 256
    half = rows // 2

    def project(src, slot, h, first, last):
        r = pl.ds(h * half, half)

        @pl.loop(0, wq.shape[2] // NT)
        def _(n):
            cols = pl.ds(pl.multiple_of(n * NT, NT), NT)
            d = jnp.dot(src[0][r, :], wq[slot[0], :, cols], preferred_element_type=jnp.float32)
            d = d + jnp.dot(src[1][r, :], wq[slot[1], :, cols], preferred_element_type=jnp.float32)
            if not first:
                d = d + part[r, cols]
            if last:
                q_all[x, r, cols] = d.astype(jnp.bfloat16)
            else:
                part[r, cols] = d

    load.wait()
    t3.wait_recv()
    mine = zh * 2 + core
    beside = zh * 2 + 1 - core
    far = (1 - zh) * 2 + core
    far_beside = (1 - zh) * 2 + 1 - core
    for h in range(2):
        project((text_ref, tx.at[1]), (mine, beside), h, True, False)
    t4 = {}
    for p in (1, 0, 3, 2):
        t2[p].wait_recv()
        t4[p] = go(copy(tx.at[2, piece[p]], tx.at[3, piece[p]], t4s.at[p], t4r.at[p], other))
    halves = [pl.ds(h * half, half) for h in range(2)]
    q = {}

    def qcopy(i, src_x, h, dev):
        ref = q_all.at[src_x, halves[h]]
        return go(copy(ref, ref, qs_.at[i], qr.at[i], dev))

    for h in range(2):
        for p in (2 * h, 2 * h + 1):
            t4[p].wait_recv()
        project((tx.at[2], tx.at[3]), (far, far_beside), h, False, True)
        q[h, 1] = qcopy(2 * h, x, h, xp)
        q[h, -1] = qcopy(2 * h + 1, x, h, xm)
    z_k.wait_recv()
    b_kp = kv(K(c_in), K(c_in), yp)
    b_km = kv(K(c_in), K(c_in), ym)
    q[0, 1].wait_recv()
    q_f = qcopy(4, lax.rem(x + 3, 4), 0, xp)
    z_v.wait_recv()
    b_vm = kv(V(c_in), V(c_in), ym)
    b_vp = kv(V(c_in), V(c_in), yp)
    q[1, -1].wait_recv()
    q_b = qcopy(5, lax.rem(x + 1, 4), 1, xm)
    b_kp.wait_recv()
    g_k = kv(K(cz_m), K(cz_m), yp)
    b_vm.wait_recv()
    g_v = kv(V(cz_p), V(cz_p), ym)
    for c in (a_vp, a_km, f_k, f_v, q[0, -1], q[1, 1], q_f, q_b, b_km, b_vp, g_k, g_v):
        c.wait_recv()
    for c in started:
        c.wait_send()


def gather_all(text, keys, values_t, wq):
    rows, width = text.shape
    bf = jnp.bfloat16
    vm = pl.BlockSpec(memory_space=pltpu.VMEM)
    dma = pltpu.SemaphoreType.DMA
    return pl.pallas_call(
        gather_kernel,
        out_shape=(
            jax.ShapeDtypeStruct((4, rows, wq.shape[1]), bf),
            jax.ShapeDtypeStruct((8, *keys.shape), bf),
            jax.ShapeDtypeStruct((8, *values_t.shape), bf),
        ),
        in_specs=[vm, vm, vm, pl.BlockSpec(memory_space=pl.ANY)],
        out_specs=(vm, vm, vm),
        scratch_shapes=[
            pltpu.VMEM((4, rows, width), bf),
            pltpu.VMEM((4, rows // 4, width), bf),
            pltpu.VMEM((4, width, wq.shape[1]), bf),
            pltpu.VMEM((rows, wq.shape[1]), jnp.float32),
            dma, dma((4,)), dma((4,)), dma((4,)), dma((4,)), dma, dma, dma((4,)), dma((4,)), dma((14,)), dma((14,)), dma((6,)), dma((6,)),
        ],
        compiler_params=pltpu.CompilerParams(collective_id=0, has_side_effects=True, vmem_limit_bytes=48 * 1024 * 1024),
        cost_estimate=pl.CostEstimate(flops=2 * rows * 4 * width * wq.shape[1], bytes_accessed=20 * 2**20, transcendentals=0),
        name="gather",
    )(text, keys, values_t, wq.reshape(4, width, wq.shape[1]))


def combine_kernel(gate_ref, o_ref, st_ref, wo_hbm, out_ref, og, orel, stg, wo, attn, pair_out, pair_in, keep, zs, zrel, zin,
                   wo_sem, sts, str_, rs, rr, ds_, dr, fs, fr, cs, cr, as_, ar, bs, br):
    zl, y, x = lax.axis_index("zl"), lax.axis_index("y"), lax.axis_index("x")
    zh, core = lax.axis_index("zh"), lax.axis_index("core")
    inner = {"zl": 1 - zl}
    outer = {"zh": 1 - zh, "zl": 1 - zl}
    other = {"core": 1 - core}
    ip, im, i2 = lax.rem(x + 1, 4), lax.rem(x + 3, 4), lax.rem(x + 2, 4)
    xp, xm, x2 = {"x": ip}, {"x": im}, {"x": i2}

    load = pltpu.make_async_copy(wo_hbm, wo, wo_sem)
    load.start()
    barrier = pltpu.get_barrier_semaphore()
    for peer in (inner, outer, other, xp, xm, x2):
        pl.semaphore_signal(barrier, inc=1, device_id=peer, device_id_type=MESH_ID)
    pl.semaphore_wait(barrier, 6)
    started = []

    def go(src, dst, ssem, rsem, dev):
        c = pltpu.make_async_remote_copy(src_ref=src, dst_ref=dst, send_sem=ssem, recv_sem=rsem,
                                         device_id=dev, device_id_type=MESH_ID)
        c.start()
        started.append(c)
        return c

    nb = out_ref.shape[0] // TBLK
    stc = [go(st_ref.at[pl.ds(i * nb, nb)], stg.at[s], sts.at[s], str_.at[s], dev)
           for s, i, dev in ((0, ip, xp), (1, im, xm), (2, i2, x2))]
    to_relay = lambda j: go(o_ref.at[i2 * nb + j], orel.at[j], rs.at[j], rr.at[j], xp if j < 2 else xm)
    direct = lambda j, s: go(o_ref.at[(im if s else ip) * nb + j], og.at[s, j], ds_.at[s, j], dr.at[s, j], xm if s else xp)
    onward = lambda j: go(orel.at[j], og.at[2, j], fs.at[j], fr.at[j], xp if j < 2 else xm)
    r, d, f = {}, {}, {}
    r[0] = to_relay(0)
    r[2] = to_relay(2)
    r[1] = to_relay(1)
    r[3] = to_relay(3)
    d[0, 0] = direct(0, 0)
    d[0, 1] = direct(0, 1)
    d[1, 1] = direct(1, 1)
    r[0].wait_recv()
    f[0] = onward(0)
    d[1, 0] = direct(1, 0)
    r[2].wait_recv()
    f[2] = onward(2)
    d[2, 1] = direct(2, 1)
    r[1].wait_recv()
    f[1] = onward(1)
    d[2, 0] = direct(2, 0)
    d[3, 0] = direct(3, 0)
    r[3].wait_recv()
    f[3] = onward(3)
    d[3, 1] = direct(3, 1)
    load.wait()
    for c in stc:
        c.wait_recv()
    gate = gate_ref[0]
    width = out_ref.shape[1]
    pairs, z1, z2 = {}, {}, {}

    def mix_and_project(j):
        for c in (d[j, 0], d[j, 1], f[j]):
            c.wait_recv()
        for h in range(2):
            m = [st_ref[x * nb + j, h, 0:1, :]] + [stg[s, j, h, 0:1, :] for s in range(3)]
            l = [st_ref[x * nb + j, h, 1:2, :]] + [stg[s, j, h, 1:2, :] for s in range(3)]
            best = jnp.maximum(jnp.maximum(m[0], m[1]), jnp.maximum(m[2], m[3]))
            share = [l[s] * jnp.exp2((m[s] - best) * C) for s in range(4)]
            total = jnp.maximum((share[0] + share[1]) + (share[2] + share[3]), 1.0)
            mixed = o_ref[x * nb + j, h].astype(jnp.float32) * (share[0] / total)
            for s in range(3):
                mixed = mixed + og[s, j, h].astype(jnp.float32) * (share[s + 1] / total)
            mixed = mixed.T.astype(jnp.bfloat16)
            for g in range(GROUP):
                col = (h * GROUP + g) * HD
                attn[:, col:col + HD] = mixed[g * TBLK:(g + 1) * TBLK, :]
        def proj(zo, co):
            cols = pl.ds(pl.multiple_of((zo * 2 + co) * width, width), width)
            return jnp.dot(attn[...], wo[:, cols], preferred_element_type=jnp.float32)
        for zo in range(2):
            pair_out[j, zo] = proj(zo, 1 - core).astype(jnp.bfloat16)
        pairs[j] = go(pair_out.at[j], pair_in.at[j], cs.at[j], cr.at[j], other)
        keep[j, 1] = proj(1 - zh, core)
        keep[j, 0] = proj(zh, core)

    hh = TBLK // 2

    def sum_pair(j):
        pairs[j].wait_recv()
        zs[j] = (keep[j, 1] + pair_in[j, 1 - zh].astype(jnp.float32)).astype(jnp.bfloat16)
        for v, dev in ((0, inner), (1, outer)):
            part = pl.ds(v * hh, hh)
            z1[j, v] = go(zs.at[j, part], zrel.at[j, v], as_.at[j, v], ar.at[j, v], dev)
        keep[j, 0] = keep[j, 0] + pair_in[j, zh].astype(jnp.float32)

    def relay_z(j):
        for v, dev in ((0, outer), (1, inner)):
            z1[j, v].wait_recv()
            z2[j, v] = go(zrel.at[j, v], zin.at[j, pl.ds(v * hh, hh)], bs.at[j, v], br.at[j, v], dev)

    def finish(j):
        for v in range(2):
            z2[j, v].wait_recv()
        out_ref[j * TBLK:(j + 1) * TBLK, :] = (gate * (keep[j, 0] + zin[j].astype(jnp.float32))).astype(jnp.bfloat16)

    for j in range(nb + 3):
        if j < nb:
            mix_and_project(j)
            sum_pair(j)
        if 1 <= j <= nb:
            relay_z(j - 1)
        if 2 <= j <= nb + 1:
            finish(j - 2)
    for c in started:
        c.wait_send()


def combine_all(gate, o, st, wo, rows):
    bf = jnp.bfloat16
    nb = rows // TBLK
    width = wo.shape[1] // 4
    vm = pl.BlockSpec(memory_space=pltpu.VMEM)
    dma = pltpu.SemaphoreType.DMA
    tile = o.shape[1:]
    return pl.pallas_call(
        combine_kernel,
        out_shape=jax.ShapeDtypeStruct((rows, width), bf),
        in_specs=[pl.BlockSpec(memory_space=pltpu.SMEM), vm, vm, pl.BlockSpec(memory_space=pl.ANY)],
        out_specs=vm,
        scratch_shapes=[
            pltpu.VMEM((3, nb, *tile), bf),
            pltpu.VMEM((nb, *tile), bf),
            pltpu.VMEM((3, nb, *st.shape[1:]), jnp.float32),
            pltpu.VMEM(wo.shape, bf),
            pltpu.VMEM((TBLK, wo.shape[0]), bf),
            pltpu.VMEM((nb, 2, TBLK, width), bf),
            pltpu.VMEM((nb, 2, TBLK, width), bf),
            pltpu.VMEM((nb, 2, TBLK, width), jnp.float32),
            pltpu.VMEM((nb, TBLK, width), bf),
            pltpu.VMEM((nb, 2, TBLK // 2, width), bf),
            pltpu.VMEM((nb, TBLK, width), bf),
            dma, dma((3,)), dma((3,)), dma((4,)), dma((4,)), dma((2, 4)), dma((2, 4)), dma((4,)), dma((4,)), dma((4,)), dma((4,)),
            dma((4, 2)), dma((4, 2)), dma((4, 2)), dma((4, 2)),
        ],
        compiler_params=pltpu.CompilerParams(collective_id=1, has_side_effects=True, vmem_limit_bytes=48 * 1024 * 1024),
        cost_estimate=pl.CostEstimate(flops=2 * rows * wo.shape[0] * wo.shape[1], bytes_accessed=20 * 2**20, transcendentals=0),
        name="combine",
    )(gate, o, st, wo)


def shards(text, wq, keys, values, wo, gate, lengths, limits):
    xi = lax.axis_index("x")
    group = lax.axis_index("zl") * 4 + lax.axis_index("y")
    rows = text.shape[0]
    q_all, k_all, vt_all = gather_all(text, keys, values.T, wq)
    q_all = q_all.reshape(4 * rows, -1)
    blocks = 4 * rows // TBLK
    ends = jnp.cumsum(lengths)
    lim = lax.dynamic_slice_in_dim(limits, group * blocks, blocks, 0)
    seen = jnp.sum(jnp.where(jnp.arange(lengths.shape[0])[None, :] < lim[:, None], lengths[None, :], 0), axis=1)
    first_token = (jnp.arange(8) * 4 + xi) * keys.shape[0]
    nvis = jnp.sum(jnp.clip(seen[:, None] - first_token[None, :], 0, keys.shape[0]), axis=1).astype(jnp.int32)
    o, st = attention(nvis, q_all, k_all, vt_all)
    return combine_all(jnp.tanh(gate), o, st, wo, rows)


def solution(mesh):
    mesh = Mesh(mesh.devices.reshape(2, 4, 4, 2, 2), ("zl", "y", "x", "zh", "core"))
    seq, head = ("zl", "y", "x"), ("zh", "core")
    in_specs = (P(seq, head), P(None, head), P(seq, head), P(seq, head), P(head, None), P(), P(), P())
    return jax.shard_map(shards, mesh=mesh, in_specs=in_specs, out_specs=P(seq, head), check_vma=False)
```

```python
import math

import jax
import jax.numpy as jnp
from jax import lax
from jax.experimental import pallas as pl
from jax.experimental.pallas import tpu as pltpu
from jax.sharding import Mesh, PartitionSpec as P

HD = 128
TBLK = 64
GROUP = 4
NEG = -1e30
C = math.log2(math.e) / math.sqrt(HD)
TK = 512
CH = 128
UN = 4
PB = 2


def attn_kernel(nv_ref, q_ref, k_ref, vt_ref, kx_ref, o_ref, st_ref, *scr):
    S = [scr[2 * u:2 * u + 2] for u in range(UN)]
    PP = [scr[2 * UN + 2 * u:2 * UN + 2 * u + 2] for u in range(UN)]
    mx_st, al_st, m_c, l_c, a_c, qx, tiles, after, blk, tile, first, flag = scr[4 * UN:]
    blocks = o_ref.shape[0]

    total = jnp.int32(0)
    for b in range(blocks):
        tiles[b] = lax.shift_right_logical(nv_ref[b] + (TK - 1), TK.bit_length() - 1)
        total = total + tiles[b]
    nxt = jnp.int32(0)
    for b in reversed(range(blocks)):
        after[b] = nxt
        nxt = jnp.where(tiles[b] > 0, b, nxt)
    n = lax.shift_right_logical(total + (PB - 1), PB.bit_length() - 1)

    def describe(i, b, t, real):
        blk[i] = b
        tile[i] = t
        first[i] = jnp.where(real & (t == 0), 1, 0)
        flag[i] = jnp.where(real, jnp.where(t + 1 == tiles[b], b, blocks), blocks + 1)

    def advance(i):
        b, t = blk[i - 1], tile[i - 1]
        ends = t + 1 >= tiles[b]
        real = i < total + PB
        nb = jnp.where(real & ends, after[b], b)
        nt = jnp.where(real, jnp.where(ends, 0, t + 1), t)
        describe(i, nb, nt, real)

    for i in range(PB):
        describe(i, nxt, 0, total < 0)
    describe(PB, nxt, 0, total > 0)
    for i in range(PB + 1, 3 * PB):
        advance(i)

    o_ref[...] = jnp.zeros_like(o_ref)
    for b in range(blocks):
        for h in range(2):
            st_ref[b, h, 0:1, :] = jnp.full((1, 4 * TBLK), NEG, jnp.float32)
            st_ref[b, h, 1:2, :] = jnp.zeros((1, 4 * TBLK), jnp.float32)
    al_st[...] = jnp.zeros_like(al_st)
    m_c[...] = jnp.full_like(m_c, NEG)
    l_c[...] = jnp.zeros_like(l_c)
    a_c[...] = jnp.zeros_like(a_c)
    for h in range(2):
        for u in range(UN):
            PP[u][h][...] = jnp.zeros_like(PP[u][h])
    qx[...] = jnp.where(lax.broadcasted_iota(jnp.int32, qx.shape, 0) == 0, NEG, 0.0).astype(jnp.bfloat16)

    def qk(par, i, h):
        b, t = blk[i], tile[i]
        lhs = jnp.concatenate([k_ref[t, :, h * HD:(h + 1) * HD], kx_ref[flag[i]]], axis=1)
        rhs = jnp.concatenate([q_ref[b, h], qx[...]], axis=0)
        s = jnp.dot(lhs, rhs, preferred_element_type=jnp.float32)
        S[par][h][...] = s
        mx_st[par, h] = jnp.max(s.reshape(TK // 8, 8, 4 * TBLK), axis=0)

    def pv(par, i, h, late):
        r = jnp.dot(vt_ref[tile[i], h * HD:(h + 1) * HD, :], PP[par][h][...], preferred_element_type=jnp.float32)
        new = a_c[h] * al_st[par, h] + r
        a_c[h] = new
        late.append((i, h, new))

    def softmax(par, i, h, late):
        s_ref, p_ref = S[par][h], PP[par][h]
        m_prev = jnp.where(first[i] == 1, jnp.full((1, 4 * TBLK), NEG, jnp.float32), m_c[h])
        m_new = jnp.maximum(m_prev, jnp.max(mx_st[par, h], axis=0, keepdims=True))
        m_c[h] = m_new
        alpha = jnp.exp2((m_prev - m_new) * C)
        al_st[par, h] = alpha
        ls = None
        for c in range(TK // CH):
            p = jnp.exp2((s_ref[c * CH:(c + 1) * CH, :] - m_new) * C)
            v = jnp.sum(p.reshape(CH // 8, 8, 4 * TBLK), axis=0)
            ls = v if ls is None else ls + v
            p_ref[c * CH:(c + 1) * CH, :] = p.astype(jnp.bfloat16)
        l_new = l_c[h] * alpha + ls
        l_c[h] = l_new
        late.append((i, h, m_new, jnp.sum(l_new, axis=0, keepdims=True)))

    def flush(late):
        for i, h, *v in late:
            if len(v) == 1:
                o_ref[blk[i], h] = v[0].astype(jnp.bfloat16)
            else:
                st_ref[blk[i], h, 0:1, :] = v[0]
                st_ref[blk[i], h, 1:2, :] = v[1]

    for u in range(PB):
        for h in range(2):
            qk(u, PB + u, h)

    us = [(u, h) for u in range(PB) for h in range(2)]

    def block(base, i):
        late = []
        for u, h in us:
            qk((base + u + PB) % UN, i + u + PB, h)
        for u, h in us:
            pv((base + u - PB) % UN, i + u - PB, h, late)
        for u, h in us:
            softmax((base + u) % UN, i + u, h, late)
        for u in range(PB):
            advance(i + u + 2 * PB)
        flush(late)

    def tail(base, i):
        late = []
        for u, h in us:
            pv((base + u) % UN, i + u, h, late)
        flush(late)

    R = UN // PB

    @pl.loop(0, lax.div(n + R, R))
    def _(j):
        for r in range(R):
            step = j * R + r

            @pl.when(step < n)
            def _():
                block(r * PB, (step + 1) * PB)

            @pl.when((step == n) & (n > 0))
            def _():
                tail(((r - 1) * PB) % UN, step * PB)


def attention(nv, q, k, vt, kx):
    blocks = nv.shape[0]
    sm = pl.BlockSpec(memory_space=pltpu.SMEM)
    vm = pl.BlockSpec(memory_space=pltpu.VMEM)
    f32, bf = jnp.float32, jnp.bfloat16
    w = 4 * TBLK
    table = pltpu.SMEM((blocks * k.shape[0] + 4 * PB,), jnp.int32)
    return pl.pallas_call(
        attn_kernel,
        out_shape=(jax.ShapeDtypeStruct((blocks, 2, HD, w), bf), jax.ShapeDtypeStruct((blocks, 2, 2, w), f32)),
        in_specs=[sm] + [vm] * 4,
        out_specs=(vm, vm),
        scratch_shapes=[pltpu.VMEM((TK, w), f32)] * (2 * UN) + [pltpu.VMEM((TK, w), bf)] * (2 * UN) + [
            pltpu.VMEM((UN, 2, 8, w), f32), pltpu.VMEM((UN, 2, 1, w), f32), pltpu.VMEM((2, 1, w), f32),
            pltpu.VMEM((2, 8, w), f32), pltpu.VMEM((2, HD, w), f32), pltpu.VMEM((HD, w), bf),
            pltpu.SMEM((blocks,), jnp.int32), pltpu.SMEM((blocks,), jnp.int32), table, table, table, table],
        compiler_params=pltpu.CompilerParams(vmem_limit_bytes=24 * 1024 * 1024),
        cost_estimate=pl.CostEstimate(flops=10**10, bytes_accessed=10**7, transcendentals=10**7),
        name="attend",
    )(nv, q, k, vt, kx)


MESH_ID = pl.DeviceIdType.MESH


def gather_kernel(text_hbm, k_hbm, v_hbm, wq_hbm, len_ref, lim_ref, nv_ref, q_all, k_all, vt_all, kx_all,
                  text_ref, v_ref, tx, relay, wq, part, ends, in_sem, t1s, t1r, t2s, t2r, t3s, t3r, t4s, t4r, ks, kr, qs_, qr):
    zl, y, x = lax.axis_index("zl"), lax.axis_index("y"), lax.axis_index("x")
    zh, core = lax.axis_index("zh"), lax.axis_index("core")
    inner = {"zl": 1 - zl}
    outer = {"zh": 1 - zh, "zl": 1 - zl}
    other = {"core": 1 - core}
    yp, ym = {"y": lax.rem(y + 1, 4)}, {"y": lax.rem(y + 3, 4)}
    xp, xm = {"x": lax.rem(x + 1, 4)}, {"x": lax.rem(x + 3, 4)}

    c_me = zl * 4 + y
    loads = [pltpu.make_async_copy(src, dst, in_sem.at[i]) for i, (src, dst) in enumerate(
        ((v_hbm, v_ref), (text_hbm, text_ref), (k_hbm, k_all.at[c_me]), (wq_hbm, wq)))]
    for c in loads:
        c.start()
    barrier = pltpu.get_barrier_semaphore()
    for peer in (inner, outer, other, yp, ym, xp, xm):
        pl.semaphore_signal(barrier, inc=1, device_id=peer, device_id_type=MESH_ID)
    loads[0].wait()
    vt_all[c_me] = v_ref[...].astype(jnp.float32).T.astype(jnp.bfloat16)
    loads[1].wait()
    loads[2].wait()
    pl.semaphore_wait(barrier, 7)

    def copy(src, dst, ssem, rsem, dev):
        return pltpu.make_async_remote_copy(src_ref=src, dst_ref=dst, send_sem=ssem, recv_sem=rsem,
                                            device_id=dev, device_id_type=MESH_ID)

    rows = text_ref.shape[0]
    step = rows // 4
    piece = [pl.ds(p * step, step) for p in range(4)]
    started = []

    def go(c):
        c.start()
        started.append(c)
        return c

    t1 = [go(copy(text_ref.at[piece[p]], relay.at[p], t1s.at[p], t1r.at[p], outer if p % 2 else inner)) for p in (1, 0, 3, 2)]
    t1 = {p: c for p, c in zip((1, 0, 3, 2), t1)}
    t3 = go(copy(text_ref, tx.at[0], t3s, t3r, other))
    c_in = (1 - zl) * 4 + y
    c_m, c_p = zl * 4 + lax.rem(y + 3, 4), zl * 4 + lax.rem(y + 1, 4)
    cz_m, cz_p = (1 - zl) * 4 + lax.rem(y + 3, 4), (1 - zl) * 4 + lax.rem(y + 1, 4)
    K = lambda c: k_all.at[c]
    V = lambda c: vt_all.at[c]
    sem = iter(range(14))

    def kv(src, dst, dev):
        i = next(sem)
        return go(copy(src, dst, ks.at[i], kr.at[i], dev))

    a_kp = kv(K(c_me), K(c_me), yp)
    a_vm = kv(V(c_me), V(c_me), ym)
    a_vp = kv(V(c_me), V(c_me), yp)
    a_km = kv(K(c_me), K(c_me), ym)
    t2 = {}
    for p in (1, 0, 3, 2):
        t1[p].wait_recv()
        t2[p] = go(copy(relay.at[p], tx.at[1, piece[p]], t2s.at[p], t2r.at[p], inner if p % 2 else outer))
    z_k = kv(K(c_me), K(c_me), inner)
    z_v = kv(V(c_me), V(c_me), inner)
    a_kp.wait_recv()
    f_k = kv(K(c_m), K(c_m), yp)
    a_vm.wait_recv()
    f_v = kv(V(c_p), V(c_p), ym)

    NT = GROUP * HD
    half = rows // 2

    def project(src, slot, h, first, last):
        r = pl.ds(h * half, half)

        @pl.loop(0, wq.shape[2] // NT)
        def _(n):
            cols = pl.ds(pl.multiple_of(n * NT, NT), NT)
            d = jnp.dot(src[0][r, :], wq[slot[0], :, cols], preferred_element_type=jnp.float32)
            d = d + jnp.dot(src[1][r, :], wq[slot[1], :, cols], preferred_element_type=jnp.float32)
            if not first:
                d = d + part[r, cols]
            if last:
                for b in range(half // TBLK):
                    heads = [d[b * TBLK:(b + 1) * TBLK, g * HD:(g + 1) * HD] for g in range(GROUP)]
                    q_all[x, h * (half // TBLK) + b, n] = jnp.concatenate(heads, axis=0).T.astype(jnp.bfloat16)
            else:
                part[r, cols] = d

    ends[0] = jnp.int32(0)
    for f in range(len_ref.shape[0]):
        ends[f + 1] = ends[f] + len_ref[f]
    blocks = nv_ref.shape[0]
    chunk = k_all.shape[1]
    spot = lax.broadcasted_iota(jnp.int32, kx_all.shape[1:], 0)
    for b in range(blocks):
        seen = ends[lim_ref[c_me * blocks + b]]
        tail = jnp.clip((seen & (4 * chunk - 1)) - x * chunk, 0, chunk)
        mine = lax.shift_right_logical(seen, (4 * chunk).bit_length() - 1) * chunk + tail
        nv_ref[b] = mine
        edge = mine & (TK - 1)
        kx_all[b] = jnp.where(spot < jnp.where(edge == 0, TK, edge), 0.0, 1.0).astype(jnp.bfloat16)
    kx_all[blocks] = jnp.zeros(kx_all.shape[1:], jnp.bfloat16)
    kx_all[blocks + 1] = jnp.ones(kx_all.shape[1:], jnp.bfloat16)
    loads[3].wait()
    t3.wait_recv()
    mine = zh * 2 + core
    beside = zh * 2 + 1 - core
    far = (1 - zh) * 2 + core
    far_beside = (1 - zh) * 2 + 1 - core
    for h in range(2):
        project((text_ref, tx.at[0]), (mine, beside), h, True, False)
    t4 = {}
    for p in (1, 0, 3, 2):
        t2[p].wait_recv()
        t4[p] = go(copy(tx.at[1, piece[p]], tx.at[2, piece[p]], t4s.at[p], t4r.at[p], other))
    halves = [pl.ds(h * (half // TBLK), half // TBLK) for h in range(2)]
    q = {}

    def qcopy(i, src_x, h, dev):
        ref = q_all.at[src_x, halves[h]]
        return go(copy(ref, ref, qs_.at[i], qr.at[i], dev))

    for h in range(2):
        for p in (2 * h, 2 * h + 1):
            t4[p].wait_recv()
        project((tx.at[1], tx.at[2]), (far, far_beside), h, False, True)
        q[h, 1] = qcopy(2 * h, x, h, xp)
        q[h, -1] = qcopy(2 * h + 1, x, h, xm)
    z_k.wait_recv()
    b_kp = kv(K(c_in), K(c_in), yp)
    b_km = kv(K(c_in), K(c_in), ym)
    q[0, 1].wait_recv()
    q_f = qcopy(4, lax.rem(x + 3, 4), 0, xp)
    z_v.wait_recv()
    b_vm = kv(V(c_in), V(c_in), ym)
    b_vp = kv(V(c_in), V(c_in), yp)
    q[1, -1].wait_recv()
    q_b = qcopy(5, lax.rem(x + 1, 4), 1, xm)
    b_kp.wait_recv()
    g_k = kv(K(cz_m), K(cz_m), yp)
    b_vm.wait_recv()
    g_v = kv(V(cz_p), V(cz_p), ym)
    for c in (a_vp, a_km, f_k, f_v, q[0, -1], q[1, 1], q_f, q_b, b_km, b_vp, g_k, g_v):
        c.wait_recv()
    for c in started:
        c.wait_send()


def gather_all(text, keys, values, wq, lengths, limits):
    rows, width = text.shape
    bf = jnp.bfloat16
    blocks = 4 * rows // TBLK
    vm = pl.BlockSpec(memory_space=pltpu.VMEM)
    sm = pl.BlockSpec(memory_space=pltpu.SMEM)
    hbm = pl.BlockSpec(memory_space=pltpu.HBM)
    dma = pltpu.SemaphoreType.DMA
    return pl.pallas_call(
        gather_kernel,
        out_shape=(
            jax.ShapeDtypeStruct((blocks,), jnp.int32),
            jax.ShapeDtypeStruct((4, rows // TBLK, 2, HD, GROUP * TBLK), bf),
            jax.ShapeDtypeStruct((8, *keys.shape), bf),
            jax.ShapeDtypeStruct((8, *values.shape[::-1]), bf),
            jax.ShapeDtypeStruct((blocks + 2, TK, HD), bf),
        ),
        in_specs=[hbm] * 4 + [sm] * 2,
        out_specs=(sm, vm, vm, vm, vm),
        scratch_shapes=[
            pltpu.VMEM((rows, width), bf),
            pltpu.VMEM(values.shape, bf),
            pltpu.VMEM((3, rows, width), bf),
            pltpu.VMEM((4, rows // 4, width), bf),
            pltpu.VMEM((4, width, wq.shape[1]), bf),
            pltpu.VMEM((rows, wq.shape[1]), jnp.float32),
            pltpu.SMEM((lengths.shape[0] + 1,), jnp.int32),
            dma((4,)), dma((4,)), dma((4,)), dma((4,)), dma((4,)), dma, dma, dma((4,)), dma((4,)), dma((14,)), dma((14,)), dma((6,)), dma((6,)),
        ],
        compiler_params=pltpu.CompilerParams(collective_id=0, has_side_effects=True, vmem_limit_bytes=40 * 1024 * 1024),
        cost_estimate=pl.CostEstimate(flops=2 * rows * 4 * width * wq.shape[1], bytes_accessed=20 * 2**20, transcendentals=0),
        name="gather",
    )(text, keys, values, wq.reshape(4, width, wq.shape[1]), lengths, limits)


def combine_kernel(gate_ref, o_ref, st_ref, wo, out_ref, og, orel, stg, attn, pair_out, pair_in, keep, zs, zrel, zin,
                   sts, str_, rs, rr, ds_, dr, fs, fr, cs, cr, as_, ar, bs, br):
    zl, y, x = lax.axis_index("zl"), lax.axis_index("y"), lax.axis_index("x")
    zh, core = lax.axis_index("zh"), lax.axis_index("core")
    inner = {"zl": 1 - zl}
    outer = {"zh": 1 - zh, "zl": 1 - zl}
    other = {"core": 1 - core}
    ip, im, i2 = lax.rem(x + 1, 4), lax.rem(x + 3, 4), lax.rem(x + 2, 4)
    xp, xm, x2 = {"x": ip}, {"x": im}, {"x": i2}

    barrier = pltpu.get_barrier_semaphore()
    for peer in (inner, outer, other, xp, xm, x2):
        pl.semaphore_signal(barrier, inc=1, device_id=peer, device_id_type=MESH_ID)
    pl.semaphore_wait(barrier, 6)
    started = []

    def go(src, dst, ssem, rsem, dev):
        c = pltpu.make_async_remote_copy(src_ref=src, dst_ref=dst, send_sem=ssem, recv_sem=rsem,
                                         device_id=dev, device_id_type=MESH_ID)
        c.start()
        started.append(c)
        return c

    nb = out_ref.shape[0] // TBLK
    stc = [go(st_ref.at[pl.ds(i * nb, nb)], stg.at[s], sts.at[s], str_.at[s], dev)
           for s, i, dev in ((0, ip, xp), (1, im, xm), (2, i2, x2))]
    to_relay = lambda j: go(o_ref.at[i2 * nb + j], orel.at[j], rs.at[j], rr.at[j], xp if j < 2 else xm)
    direct = lambda j, s: go(o_ref.at[(im if s else ip) * nb + j], og.at[s, j], ds_.at[s, j], dr.at[s, j], xm if s else xp)
    onward = lambda j: go(orel.at[j], og.at[2, j], fs.at[j], fr.at[j], xp if j < 2 else xm)
    r, d, f = {}, {}, {}
    r[0] = to_relay(0)
    r[2] = to_relay(2)
    r[1] = to_relay(1)
    r[3] = to_relay(3)
    d[0, 0] = direct(0, 0)
    d[0, 1] = direct(0, 1)
    d[1, 1] = direct(1, 1)
    r[0].wait_recv()
    f[0] = onward(0)
    d[1, 0] = direct(1, 0)
    r[2].wait_recv()
    f[2] = onward(2)
    d[2, 1] = direct(2, 1)
    r[1].wait_recv()
    f[1] = onward(1)
    d[2, 0] = direct(2, 0)
    d[3, 0] = direct(3, 0)
    r[3].wait_recv()
    f[3] = onward(3)
    d[3, 1] = direct(3, 1)
    for c in stc:
        c.wait_recv()
    gate = gate_ref[0]
    width = out_ref.shape[1]
    pairs, z1, z2 = {}, {}, {}

    def mix_and_project(j):
        for c in (d[j, 0], d[j, 1], f[j]):
            c.wait_recv()
        for h in range(2):
            m = [st_ref[x * nb + j, h, 0:1, :]] + [stg[s, j, h, 0:1, :] for s in range(3)]
            l = [st_ref[x * nb + j, h, 1:2, :]] + [stg[s, j, h, 1:2, :] for s in range(3)]
            best = jnp.maximum(jnp.maximum(m[0], m[1]), jnp.maximum(m[2], m[3]))
            scale = [jnp.exp2((m[s] - best) * C) for s in range(4)]
            total = jnp.maximum((l[0] * scale[0] + l[1] * scale[1]) + (l[2] * scale[2] + l[3] * scale[3]), 1.0)
            mixed = o_ref[x * nb + j, h].astype(jnp.float32) * (scale[0] / total)
            for s in range(3):
                mixed = mixed + og[s, j, h].astype(jnp.float32) * (scale[s + 1] / total)
            mixed = mixed.T.astype(jnp.bfloat16)
            for g in range(GROUP):
                col = (h * GROUP + g) * HD
                attn[:, col:col + HD] = mixed[g * TBLK:(g + 1) * TBLK, :]
        def proj(zo, co):
            cols = pl.ds(pl.multiple_of((zo * 2 + co) * width, width), width)
            return jnp.dot(attn[...], wo[:, cols], preferred_element_type=jnp.float32)
        for zo in range(2):
            pair_out[j, zo] = proj(zo, 1 - core).astype(jnp.bfloat16)
        pairs[j] = go(pair_out.at[j], pair_in.at[j], cs.at[j], cr.at[j], other)
        keep[j, 1] = proj(1 - zh, core)
        keep[j, 0] = proj(zh, core)

    hh = TBLK // 2

    def sum_pair(j):
        pairs[j].wait_recv()
        zs[j] = (keep[j, 1] + pair_in[j, 1 - zh].astype(jnp.float32)).astype(jnp.bfloat16)
        for v, dev in ((0, inner), (1, outer)):
            part = pl.ds(v * hh, hh)
            z1[j, v] = go(zs.at[j, part], zrel.at[j, v], as_.at[j, v], ar.at[j, v], dev)
        keep[j, 0] = keep[j, 0] + pair_in[j, zh].astype(jnp.float32)

    def relay_z(j):
        for v, dev in ((0, outer), (1, inner)):
            z1[j, v].wait_recv()
            z2[j, v] = go(zrel.at[j, v], zin.at[j, pl.ds(v * hh, hh)], bs.at[j, v], br.at[j, v], dev)

    def finish(j):
        for v in range(2):
            z2[j, v].wait_recv()
        out_ref[j * TBLK:(j + 1) * TBLK, :] = (gate * (keep[j, 0] + zin[j].astype(jnp.float32))).astype(jnp.bfloat16)

    for j in range(nb + 3):
        if j < nb:
            mix_and_project(j)
            sum_pair(j)
        if 1 <= j <= nb:
            relay_z(j - 1)
        if 2 <= j <= nb + 1:
            finish(j - 2)
    for c in started:
        c.wait_send()


def combine_all(gate, o, st, wo, rows):
    bf = jnp.bfloat16
    nb = rows // TBLK
    width = wo.shape[1] // 4
    vm = pl.BlockSpec(memory_space=pltpu.VMEM)
    dma = pltpu.SemaphoreType.DMA
    tile = o.shape[1:]
    return pl.pallas_call(
        combine_kernel,
        out_shape=jax.ShapeDtypeStruct((rows, width), bf),
        in_specs=[pl.BlockSpec(memory_space=pltpu.SMEM), vm, vm, vm],
        out_specs=vm,
        scratch_shapes=[
            pltpu.VMEM((3, nb, *tile), bf),
            pltpu.VMEM((nb, *tile), bf),
            pltpu.VMEM((3, nb, *st.shape[1:]), jnp.float32),
            pltpu.VMEM((TBLK, wo.shape[0]), bf),
            pltpu.VMEM((nb, 2, TBLK, width), bf),
            pltpu.VMEM((nb, 2, TBLK, width), bf),
            pltpu.VMEM((nb, 2, TBLK, width), jnp.float32),
            pltpu.VMEM((nb, TBLK, width), bf),
            pltpu.VMEM((nb, 2, TBLK // 2, width), bf),
            pltpu.VMEM((nb, TBLK, width), bf),
            dma((3,)), dma((3,)), dma((4,)), dma((4,)), dma((2, 4)), dma((2, 4)), dma((4,)), dma((4,)), dma((4,)), dma((4,)),
            dma((4, 2)), dma((4, 2)), dma((4, 2)), dma((4, 2)),
        ],
        compiler_params=pltpu.CompilerParams(collective_id=1, has_side_effects=True, vmem_limit_bytes=24 * 1024 * 1024),
        cost_estimate=pl.CostEstimate(flops=2 * rows * wo.shape[0] * wo.shape[1], bytes_accessed=20 * 2**20, transcendentals=0),
        name="combine",
    )(gate, o, st, wo)


def shards(text, wq, keys, values, wo, gate, lengths, limits):
    here = [pltpu.with_memory_space_constraint(a, pltpu.HBM) for a in (text, keys, values, lengths, limits)]
    nv, q, k, vt, kx = gather_all(*here[:3], wq, *here[3:])
    o, st = attention(nv, q.reshape(-1, *q.shape[2:]), k, vt, kx)
    return combine_all(jnp.tanh(gate), o, st, wo, text.shape[0])


def solution(mesh):
    mesh = Mesh(mesh.devices.reshape(2, 4, 4, 2, 2), ("zl", "y", "x", "zh", "core"))
    seq, head = ("zl", "y", "x"), ("zh", "core")
    in_specs = (P(seq, head), P(None, head), P(seq, head), P(seq, head), P(head, None), P(), P(), P())
    return jax.shard_map(shards, mesh=mesh, in_specs=in_specs, out_specs=P(seq, head), check_vma=False)
```

```python
import math

import jax
import jax.numpy as jnp
from jax import lax
from jax.experimental import pallas as pl
from jax.experimental.pallas import tpu as pltpu
from jax.sharding import Mesh, PartitionSpec as P

HD = 128
TBLK = 64
GROUP = 4
NEG = -1e30
C = math.log2(math.e) / math.sqrt(HD)
TK = 512
CH = 64
UN = 4
PB = 2


def attn_kernel(nv_ref, q_ref, k_ref, vt_ref, kx_ref, o_ref, st_ref, *scr):
    S = [scr[2 * u:2 * u + 2] for u in range(UN)]
    PP = [scr[2 * UN + 2 * u:2 * UN + 2 * u + 2] for u in range(UN)]
    mx_st, al_st, m_c, l_c, a_c, qx, tiles, after, blk, tile, first, flag = scr[4 * UN:]
    blocks = o_ref.shape[0]

    total = jnp.int32(0)
    for b in range(blocks):
        tiles[b] = lax.shift_right_logical(nv_ref[b] + (TK - 1), TK.bit_length() - 1)
        total = total + tiles[b]
    nxt = jnp.int32(0)
    for b in reversed(range(blocks)):
        after[b] = nxt
        nxt = jnp.where(tiles[b] > 0, b, nxt)
    n = lax.shift_right_logical(total + (PB - 1), PB.bit_length() - 1)

    def describe(i, b, t, real):
        blk[i] = b
        tile[i] = t
        first[i] = jnp.where(real & (t == 0), 1, 0)
        flag[i] = jnp.where(real, jnp.where(t + 1 == tiles[b], b, blocks), blocks + 1)

    def advance(i):
        b, t = blk[i - 1], tile[i - 1]
        ends = t + 1 >= tiles[b]
        real = i < total + PB
        nb = jnp.where(real & ends, after[b], b)
        nt = jnp.where(real, jnp.where(ends, 0, t + 1), t)
        describe(i, nb, nt, real)

    for i in range(PB):
        describe(i, nxt, 0, total < 0)
    describe(PB, nxt, 0, total > 0)
    @pl.loop(PB + 1, total + 3 * PB)
    def _(i):
        advance(i)

    o_ref[...] = jnp.zeros_like(o_ref)
    for b in range(blocks):
        for h in range(2):
            st_ref[b, h, 0:1, :] = jnp.full((1, 4 * TBLK), NEG, jnp.float32)
            st_ref[b, h, 1:2, :] = jnp.zeros((1, 4 * TBLK), jnp.float32)
    al_st[...] = jnp.zeros_like(al_st)
    m_c[...] = jnp.full_like(m_c, NEG)
    l_c[...] = jnp.zeros_like(l_c)
    a_c[...] = jnp.zeros_like(a_c)
    for h in range(2):
        for u in range(UN):
            PP[u][h][...] = jnp.zeros_like(PP[u][h])
    qx[...] = jnp.where(lax.broadcasted_iota(jnp.int32, qx.shape, 0) == 0, NEG, 0.0).astype(jnp.bfloat16)

    def qk(par, i, h):
        b, t = blk[i], tile[i]
        lhs = jnp.concatenate([k_ref[t, :, h * HD:(h + 1) * HD], kx_ref[flag[i]]], axis=1)
        rhs = jnp.concatenate([q_ref[b, h], qx[...]], axis=0)
        s = jnp.dot(lhs, rhs, preferred_element_type=jnp.float32)
        S[par][h][...] = s
        mx_st[par, h] = jnp.max(s.reshape(TK // 8, 8, 4 * TBLK), axis=0)

    def pv(par, i, h, late):
        r = jnp.dot(vt_ref[tile[i], h * HD:(h + 1) * HD, :], PP[par][h][...], preferred_element_type=jnp.float32)
        new = a_c[h] * al_st[par, h] + r
        a_c[h] = new
        late.append((i, h, new))

    def softmax(par, i, h, late):
        s_ref, p_ref = S[par][h], PP[par][h]
        m_prev = jnp.where(first[i] == 1, jnp.full((1, 4 * TBLK), NEG, jnp.float32), m_c[h])
        m_new = jnp.maximum(m_prev, jnp.max(mx_st[par, h], axis=0, keepdims=True))
        m_c[h] = m_new
        alpha = jnp.exp2((m_prev - m_new) * C)
        al_st[par, h] = alpha
        ls = None
        for c in range(TK // CH):
            p = jnp.exp2((s_ref[c * CH:(c + 1) * CH, :] - m_new) * C)
            v = jnp.sum(p.reshape(CH // 8, 8, 4 * TBLK), axis=0)
            ls = v if ls is None else ls + v
            p_ref[c * CH:(c + 1) * CH, :] = p.astype(jnp.bfloat16)
        l_new = l_c[h] * alpha + ls
        l_c[h] = l_new
        late.append((i, h, m_new, jnp.sum(l_new, axis=0, keepdims=True)))

    def flush(late):
        for i, h, *v in late:
            if len(v) == 1:
                o_ref[blk[i], h] = v[0].astype(jnp.bfloat16)
            else:
                st_ref[blk[i], h, 0:1, :] = v[0]
                st_ref[blk[i], h, 1:2, :] = v[1]

    for u in range(PB):
        for h in range(2):
            qk(u, PB + u, h)

    us = [(u, h) for u in range(PB) for h in range(2)]

    def block(base, i):
        late = []
        for u, h in us:
            qk((base + u + PB) % UN, i + u + PB, h)
        for u, h in us:
            pv((base + u - PB) % UN, i + u - PB, h, late)
        for u, h in us:
            softmax((base + u) % UN, i + u, h, late)
        flush(late)

    def tail(base, i):
        late = []
        for u, h in us:
            pv((base + u) % UN, i + u, h, late)
        flush(late)

    R = UN // PB

    @pl.loop(0, lax.div(n + R, R))
    def _(j):
        for r in range(R):
            step = j * R + r

            @pl.when(step < n)
            def _():
                block(r * PB, (step + 1) * PB)

            @pl.when((step == n) & (n > 0))
            def _():
                tail(((r - 1) * PB) % UN, step * PB)


def attention(nv, q, k, vt, kx):
    blocks = nv.shape[0]
    sm = pl.BlockSpec(memory_space=pltpu.SMEM)
    vm = pl.BlockSpec(memory_space=pltpu.VMEM)
    f32, bf = jnp.float32, jnp.bfloat16
    w = 4 * TBLK
    table = pltpu.SMEM((blocks * k.shape[0] + 4 * PB,), jnp.int32)
    return pl.pallas_call(
        attn_kernel,
        out_shape=(jax.ShapeDtypeStruct((blocks, 2, HD, w), bf), jax.ShapeDtypeStruct((blocks, 2, 2, w), f32)),
        in_specs=[sm] + [vm] * 4,
        out_specs=(vm, vm),
        scratch_shapes=[pltpu.VMEM((TK, w), f32)] * (2 * UN) + [pltpu.VMEM((TK, w), bf)] * (2 * UN) + [
            pltpu.VMEM((UN, 2, 8, w), f32), pltpu.VMEM((UN, 2, 1, w), f32), pltpu.VMEM((2, 1, w), f32),
            pltpu.VMEM((2, 8, w), f32), pltpu.VMEM((2, HD, w), f32), pltpu.VMEM((HD, w), bf),
            pltpu.SMEM((blocks,), jnp.int32), pltpu.SMEM((blocks,), jnp.int32), table, table, table, table],
        compiler_params=pltpu.CompilerParams(vmem_limit_bytes=24 * 1024 * 1024),
        cost_estimate=pl.CostEstimate(flops=10**10, bytes_accessed=10**7, transcendentals=10**7),
        name="attend",
    )(nv, q, k, vt, kx)


MESH_ID = pl.DeviceIdType.MESH


def gather_kernel(text_hbm, k_hbm, v_hbm, wq_hbm, len_ref, lim_ref, nv_ref, q_all, k_all, vt_all, kx_all,
                  text_ref, v_ref, tx, relay, wq, part, ends, in_sem, t1s, t1r, t2s, t2r, t3s, t3r, t4s, t4r, ks, kr, qs_, qr):
    zl, y, x = lax.axis_index("zl"), lax.axis_index("y"), lax.axis_index("x")
    zh, core = lax.axis_index("zh"), lax.axis_index("core")
    inner = {"zl": 1 - zl}
    outer = {"zh": 1 - zh, "zl": 1 - zl}
    other = {"core": 1 - core}
    yp, ym = {"y": lax.rem(y + 1, 4)}, {"y": lax.rem(y + 3, 4)}
    xp, xm = {"x": lax.rem(x + 1, 4)}, {"x": lax.rem(x + 3, 4)}

    c_me = zl * 4 + y
    loads = [pltpu.make_async_copy(src, dst, in_sem.at[i]) for i, (src, dst) in enumerate(
        ((v_hbm, v_ref), (text_hbm, text_ref), (k_hbm, k_all.at[c_me]), (wq_hbm, wq)))]
    for c in loads:
        c.start()
    barrier = pltpu.get_barrier_semaphore()
    for peer in (inner, outer, other, yp, ym, xp, xm):
        pl.semaphore_signal(barrier, inc=1, device_id=peer, device_id_type=MESH_ID)
    loads[0].wait()
    vt_all[c_me] = v_ref[...].astype(jnp.float32).T.astype(jnp.bfloat16)
    loads[1].wait()
    loads[2].wait()
    pl.semaphore_wait(barrier, 7)

    def copy(src, dst, ssem, rsem, dev):
        return pltpu.make_async_remote_copy(src_ref=src, dst_ref=dst, send_sem=ssem, recv_sem=rsem,
                                            device_id=dev, device_id_type=MESH_ID)

    rows = text_ref.shape[0]
    step = rows // 4
    piece = [pl.ds(p * step, step) for p in range(4)]
    started = []

    def go(c):
        c.start()
        started.append(c)
        return c

    t1 = [go(copy(text_ref.at[piece[p]], relay.at[p], t1s.at[p], t1r.at[p], outer if p % 2 else inner)) for p in (1, 0, 3, 2)]
    t1 = {p: c for p, c in zip((1, 0, 3, 2), t1)}
    t3 = go(copy(text_ref, tx.at[0], t3s, t3r, other))
    c_in = (1 - zl) * 4 + y
    c_m, c_p = zl * 4 + lax.rem(y + 3, 4), zl * 4 + lax.rem(y + 1, 4)
    cz_m, cz_p = (1 - zl) * 4 + lax.rem(y + 3, 4), (1 - zl) * 4 + lax.rem(y + 1, 4)
    K = lambda c: k_all.at[c]
    V = lambda c: vt_all.at[c]
    sem = iter(range(14))

    def kv(src, dst, dev):
        i = next(sem)
        return go(copy(src, dst, ks.at[i], kr.at[i], dev))

    a_kp = kv(K(c_me), K(c_me), yp)
    a_vm = kv(V(c_me), V(c_me), ym)
    a_vp = kv(V(c_me), V(c_me), yp)
    a_km = kv(K(c_me), K(c_me), ym)
    t2 = {}
    for p in (1, 0, 3, 2):
        t1[p].wait_recv()
        t2[p] = go(copy(relay.at[p], tx.at[1, piece[p]], t2s.at[p], t2r.at[p], inner if p % 2 else outer))
    z_k = kv(K(c_me), K(c_me), inner)
    z_v = kv(V(c_me), V(c_me), inner)
    a_kp.wait_recv()
    f_k = kv(K(c_m), K(c_m), yp)
    a_vm.wait_recv()
    f_v = kv(V(c_p), V(c_p), ym)

    NT = GROUP * HD
    half = rows // 2

    def project(src, slot, h, first, last):
        r = pl.ds(h * half, half)

        @pl.loop(0, wq.shape[2] // NT)
        def _(n):
            cols = pl.ds(pl.multiple_of(n * NT, NT), NT)
            d = jnp.dot(src[0][r, :], wq[slot[0], :, cols], preferred_element_type=jnp.float32)
            d = d + jnp.dot(src[1][r, :], wq[slot[1], :, cols], preferred_element_type=jnp.float32)
            if not first:
                d = d + part[r, cols]
            if last:
                for b in range(half // TBLK):
                    heads = [d[b * TBLK:(b + 1) * TBLK, g * HD:(g + 1) * HD] for g in range(GROUP)]
                    q_all[x, h * (half // TBLK) + b, n] = jnp.concatenate(heads, axis=0).T.astype(jnp.bfloat16)
            else:
                part[r, cols] = d

    ends[0] = jnp.int32(0)
    for f in range(len_ref.shape[0]):
        ends[f + 1] = ends[f] + len_ref[f]
    blocks = nv_ref.shape[0]
    chunk = k_all.shape[1]
    spot = lax.broadcasted_iota(jnp.int32, kx_all.shape[1:], 0)
    for b in range(blocks):
        seen = ends[lim_ref[c_me * blocks + b]]
        tail = jnp.clip((seen & (4 * chunk - 1)) - x * chunk, 0, chunk)
        mine = lax.shift_right_logical(seen, (4 * chunk).bit_length() - 1) * chunk + tail
        nv_ref[b] = mine
        edge = mine & (TK - 1)
        kx_all[b] = jnp.where(spot < jnp.where(edge == 0, TK, edge), 0.0, 1.0).astype(jnp.bfloat16)
    kx_all[blocks] = jnp.zeros(kx_all.shape[1:], jnp.bfloat16)
    kx_all[blocks + 1] = jnp.ones(kx_all.shape[1:], jnp.bfloat16)
    loads[3].wait()
    t3.wait_recv()
    mine = zh * 2 + core
    beside = zh * 2 + 1 - core
    far = (1 - zh) * 2 + core
    far_beside = (1 - zh) * 2 + 1 - core
    for h in range(2):
        project((text_ref, tx.at[0]), (mine, beside), h, True, False)
    t4 = {}
    for p in (1, 0, 3, 2):
        t2[p].wait_recv()
        t4[p] = go(copy(tx.at[1, piece[p]], tx.at[2, piece[p]], t4s.at[p], t4r.at[p], other))
    halves = [pl.ds(h * (half // TBLK), half // TBLK) for h in range(2)]
    q = {}

    def qcopy(i, src_x, h, dev):
        ref = q_all.at[src_x, halves[h]]
        return go(copy(ref, ref, qs_.at[i], qr.at[i], dev))

    for h in range(2):
        for p in (2 * h, 2 * h + 1):
            t4[p].wait_recv()
        project((tx.at[1], tx.at[2]), (far, far_beside), h, False, True)
        q[h, 1] = qcopy(2 * h, x, h, xp)
        q[h, -1] = qcopy(2 * h + 1, x, h, xm)
    z_k.wait_recv()
    b_kp = kv(K(c_in), K(c_in), yp)
    b_km = kv(K(c_in), K(c_in), ym)
    q[0, 1].wait_recv()
    q_f = qcopy(4, lax.rem(x + 3, 4), 0, xp)
    z_v.wait_recv()
    b_vm = kv(V(c_in), V(c_in), ym)
    b_vp = kv(V(c_in), V(c_in), yp)
    q[1, -1].wait_recv()
    q_b = qcopy(5, lax.rem(x + 1, 4), 1, xm)
    b_kp.wait_recv()
    g_k = kv(K(cz_m), K(cz_m), yp)
    b_vm.wait_recv()
    g_v = kv(V(cz_p), V(cz_p), ym)
    for c in (a_vp, a_km, f_k, f_v, q[0, -1], q[1, 1], q_f, q_b, b_km, b_vp, g_k, g_v):
        c.wait_recv()
    for c in started:
        c.wait_send()


def gather_all(text, keys, values, wq, lengths, limits):
    rows, width = text.shape
    bf = jnp.bfloat16
    blocks = 4 * rows // TBLK
    vm = pl.BlockSpec(memory_space=pltpu.VMEM)
    sm = pl.BlockSpec(memory_space=pltpu.SMEM)
    hbm = pl.BlockSpec(memory_space=pltpu.HBM)
    dma = pltpu.SemaphoreType.DMA
    return pl.pallas_call(
        gather_kernel,
        out_shape=(
            jax.ShapeDtypeStruct((blocks,), jnp.int32),
            jax.ShapeDtypeStruct((4, rows // TBLK, 2, HD, GROUP * TBLK), bf),
            jax.ShapeDtypeStruct((8, *keys.shape), bf),
            jax.ShapeDtypeStruct((8, *values.shape[::-1]), bf),
            jax.ShapeDtypeStruct((blocks + 2, TK, HD), bf),
        ),
        in_specs=[hbm] * 4 + [sm] * 2,
        out_specs=(sm, vm, vm, vm, vm),
        scratch_shapes=[
            pltpu.VMEM((rows, width), bf),
            pltpu.VMEM(values.shape, bf),
            pltpu.VMEM((3, rows, width), bf),
            pltpu.VMEM((4, rows // 4, width), bf),
            pltpu.VMEM((4, width, wq.shape[1]), bf),
            pltpu.VMEM((rows, wq.shape[1]), jnp.float32),
            pltpu.SMEM((lengths.shape[0] + 1,), jnp.int32),
            dma((4,)), dma((4,)), dma((4,)), dma((4,)), dma((4,)), dma, dma, dma((4,)), dma((4,)), dma((14,)), dma((14,)), dma((6,)), dma((6,)),
        ],
        compiler_params=pltpu.CompilerParams(collective_id=0, has_side_effects=True, vmem_limit_bytes=40 * 1024 * 1024),
        cost_estimate=pl.CostEstimate(flops=2 * rows * 4 * width * wq.shape[1], bytes_accessed=20 * 2**20, transcendentals=0),
        name="gather",
    )(text, keys, values, wq.reshape(4, width, wq.shape[1]), lengths, limits)


def combine_kernel(gate_ref, o_ref, st_ref, wo, out_ref, og, orel, stg, attn, pair_out, pair_in, keep, zs, zrel, zin,
                   sts, str_, rs, rr, ds_, dr, fs, fr, cs, cr, as_, ar, bs, br):
    zl, y, x = lax.axis_index("zl"), lax.axis_index("y"), lax.axis_index("x")
    zh, core = lax.axis_index("zh"), lax.axis_index("core")
    inner = {"zl": 1 - zl}
    outer = {"zh": 1 - zh, "zl": 1 - zl}
    other = {"core": 1 - core}
    ip, im, i2 = lax.rem(x + 1, 4), lax.rem(x + 3, 4), lax.rem(x + 2, 4)
    xp, xm, x2 = {"x": ip}, {"x": im}, {"x": i2}

    barrier = pltpu.get_barrier_semaphore()
    for peer in (inner, outer, other, xp, xm, x2):
        pl.semaphore_signal(barrier, inc=1, device_id=peer, device_id_type=MESH_ID)
    pl.semaphore_wait(barrier, 6)
    started = []

    def go(src, dst, ssem, rsem, dev):
        c = pltpu.make_async_remote_copy(src_ref=src, dst_ref=dst, send_sem=ssem, recv_sem=rsem,
                                         device_id=dev, device_id_type=MESH_ID)
        c.start()
        started.append(c)
        return c

    nb = out_ref.shape[0] // TBLK
    stc = [go(st_ref.at[pl.ds(i * nb, nb)], stg.at[s], sts.at[s], str_.at[s], dev)
           for s, i, dev in ((0, ip, xp), (1, im, xm), (2, i2, x2))]
    to_relay = lambda j: go(o_ref.at[i2 * nb + j], orel.at[j], rs.at[j], rr.at[j], xp if j < 2 else xm)
    direct = lambda j, s: go(o_ref.at[(im if s else ip) * nb + j], og.at[s, j], ds_.at[s, j], dr.at[s, j], xm if s else xp)
    onward = lambda j: go(orel.at[j], og.at[2, j], fs.at[j], fr.at[j], xp if j < 2 else xm)
    r, d, f = {}, {}, {}
    r[0] = to_relay(0)
    r[2] = to_relay(2)
    r[1] = to_relay(1)
    r[3] = to_relay(3)
    d[0, 0] = direct(0, 0)
    d[0, 1] = direct(0, 1)
    d[1, 1] = direct(1, 1)
    r[0].wait_recv()
    f[0] = onward(0)
    d[1, 0] = direct(1, 0)
    r[2].wait_recv()
    f[2] = onward(2)
    d[2, 1] = direct(2, 1)
    r[1].wait_recv()
    f[1] = onward(1)
    d[2, 0] = direct(2, 0)
    d[3, 0] = direct(3, 0)
    r[3].wait_recv()
    f[3] = onward(3)
    d[3, 1] = direct(3, 1)
    for c in stc:
        c.wait_recv()
    gate = gate_ref[0]
    width = out_ref.shape[1]
    pairs, z1, z2 = {}, {}, {}

    def mix_and_project(j):
        for c in (d[j, 0], d[j, 1], f[j]):
            c.wait_recv()
        for h in range(2):
            m = [st_ref[x * nb + j, h, 0:1, :]] + [stg[s, j, h, 0:1, :] for s in range(3)]
            l = [st_ref[x * nb + j, h, 1:2, :]] + [stg[s, j, h, 1:2, :] for s in range(3)]
            best = jnp.maximum(jnp.maximum(m[0], m[1]), jnp.maximum(m[2], m[3]))
            scale = [jnp.exp2((m[s] - best) * C) for s in range(4)]
            total = jnp.maximum((l[0] * scale[0] + l[1] * scale[1]) + (l[2] * scale[2] + l[3] * scale[3]), 1.0)
            mixed = o_ref[x * nb + j, h].astype(jnp.float32) * (scale[0] / total)
            for s in range(3):
                mixed = mixed + og[s, j, h].astype(jnp.float32) * (scale[s + 1] / total)
            mixed = mixed.T.astype(jnp.bfloat16)
            for g in range(GROUP):
                col = (h * GROUP + g) * HD
                attn[:, col:col + HD] = mixed[g * TBLK:(g + 1) * TBLK, :]
        def proj(zo, co):
            cols = pl.ds(pl.multiple_of((zo * 2 + co) * width, width), width)
            return jnp.dot(attn[...], wo[:, cols], preferred_element_type=jnp.float32)
        for zo in range(2):
            pair_out[j, zo] = proj(zo, 1 - core).astype(jnp.bfloat16)
        pairs[j] = go(pair_out.at[j], pair_in.at[j], cs.at[j], cr.at[j], other)
        keep[j, 1] = proj(1 - zh, core)
        keep[j, 0] = proj(zh, core)

    hh = TBLK // 2

    def sum_pair(j):
        pairs[j].wait_recv()
        zs[j] = (keep[j, 1] + pair_in[j, 1 - zh].astype(jnp.float32)).astype(jnp.bfloat16)
        for v, dev in ((0, inner), (1, outer)):
            part = pl.ds(v * hh, hh)
            z1[j, v] = go(zs.at[j, part], zrel.at[j, v], as_.at[j, v], ar.at[j, v], dev)
        keep[j, 0] = keep[j, 0] + pair_in[j, zh].astype(jnp.float32)

    def relay_z(j):
        for v, dev in ((0, outer), (1, inner)):
            z1[j, v].wait_recv()
            z2[j, v] = go(zrel.at[j, v], zin.at[j, pl.ds(v * hh, hh)], bs.at[j, v], br.at[j, v], dev)

    def finish(j):
        for v in range(2):
            z2[j, v].wait_recv()
        out_ref[j * TBLK:(j + 1) * TBLK, :] = (gate * (keep[j, 0] + zin[j].astype(jnp.float32))).astype(jnp.bfloat16)

    for j in range(nb + 3):
        if j < nb:
            mix_and_project(j)
            sum_pair(j)
        if 1 <= j <= nb:
            relay_z(j - 1)
        if 2 <= j <= nb + 1:
            finish(j - 2)
    for c in started:
        c.wait_send()


def combine_all(gate, o, st, wo, rows):
    bf = jnp.bfloat16
    nb = rows // TBLK
    width = wo.shape[1] // 4
    vm = pl.BlockSpec(memory_space=pltpu.VMEM)
    dma = pltpu.SemaphoreType.DMA
    tile = o.shape[1:]
    return pl.pallas_call(
        combine_kernel,
        out_shape=jax.ShapeDtypeStruct((rows, width), bf),
        in_specs=[pl.BlockSpec(memory_space=pltpu.SMEM), vm, vm, vm],
        out_specs=vm,
        scratch_shapes=[
            pltpu.VMEM((3, nb, *tile), bf),
            pltpu.VMEM((nb, *tile), bf),
            pltpu.VMEM((3, nb, *st.shape[1:]), jnp.float32),
            pltpu.VMEM((TBLK, wo.shape[0]), bf),
            pltpu.VMEM((nb, 2, TBLK, width), bf),
            pltpu.VMEM((nb, 2, TBLK, width), bf),
            pltpu.VMEM((nb, 2, TBLK, width), jnp.float32),
            pltpu.VMEM((nb, TBLK, width), bf),
            pltpu.VMEM((nb, 2, TBLK // 2, width), bf),
            pltpu.VMEM((nb, TBLK, width), bf),
            dma((3,)), dma((3,)), dma((4,)), dma((4,)), dma((2, 4)), dma((2, 4)), dma((4,)), dma((4,)), dma((4,)), dma((4,)),
            dma((4, 2)), dma((4, 2)), dma((4, 2)), dma((4, 2)),
        ],
        compiler_params=pltpu.CompilerParams(collective_id=1, has_side_effects=True, vmem_limit_bytes=24 * 1024 * 1024),
        cost_estimate=pl.CostEstimate(flops=2 * rows * wo.shape[0] * wo.shape[1], bytes_accessed=20 * 2**20, transcendentals=0),
        name="combine",
    )(gate, o, st, wo)


def shards(text, wq, keys, values, wo, gate, lengths, limits):
    here = [pltpu.with_memory_space_constraint(a, pltpu.HBM) for a in (text, keys, values, lengths, limits)]
    nv, q, k, vt, kx = gather_all(*here[:3], wq, *here[3:])
    o, st = attention(nv, q.reshape(-1, *q.shape[2:]), k, vt, kx)
    return combine_all(jnp.tanh(gate), o, st, wo, text.shape[0])


def solution(mesh):
    mesh = Mesh(mesh.devices.reshape(2, 4, 4, 2, 2), ("zl", "y", "x", "zh", "core"))
    seq, head = ("zl", "y", "x"), ("zh", "core")
    in_specs = (P(seq, head), P(None, head), P(seq, head), P(seq, head), P(head, None), P(), P(), P())
    return jax.shard_map(shards, mesh=mesh, in_specs=in_specs, out_specs=P(seq, head), check_vma=False)
```

```python
import math

import jax
import jax.numpy as jnp
from jax import lax
from jax.experimental import pallas as pl
from jax.experimental.pallas import tpu as pltpu
from jax.sharding import Mesh, PartitionSpec as P

HD = 128
TBLK = 64
GROUP = 4
NEG = -1e30
C = math.log2(math.e) / math.sqrt(HD)
TK = 512
CH = 64
UN = 4
PB = 2


def attn_kernel(nv_ref, q_ref, k_ref, vt_ref, kx_ref, o_ref, st_ref, *scr):
    S = [scr[2 * u:2 * u + 2] for u in range(UN)]
    PP = [scr[2 * UN + 2 * u:2 * UN + 2 * u + 2] for u in range(UN)]
    mx_st, al_st, m_c, l_c, a_c, qx, tiles, after, blk, tile, first, flag = scr[4 * UN:]
    blocks = o_ref.shape[0]

    total = jnp.int32(0)
    for b in range(blocks):
        tiles[b] = lax.shift_right_logical(nv_ref[b] + (TK - 1), TK.bit_length() - 1)
        total = total + tiles[b]
    nxt = jnp.int32(0)
    for b in reversed(range(blocks)):
        after[b] = nxt
        nxt = jnp.where(tiles[b] > 0, b, nxt)
    n = lax.shift_right_logical(total + (PB - 1), PB.bit_length() - 1)

    def describe(i, b, t, real):
        blk[i] = b
        tile[i] = t
        first[i] = jnp.where(real & (t == 0), 1, 0)
        flag[i] = jnp.where(real, jnp.where(t + 1 == tiles[b], b, blocks), blocks + 1)

    def advance(i):
        b, t = blk[i - 1], tile[i - 1]
        ends = t + 1 >= tiles[b]
        real = i < total + PB
        nb = jnp.where(real & ends, after[b], b)
        nt = jnp.where(real, jnp.where(ends, 0, t + 1), t)
        describe(i, nb, nt, real)

    for i in range(PB):
        describe(i, nxt, 0, total < 0)
    describe(PB, nxt, 0, total > 0)
    @pl.loop(PB + 1, total + 3 * PB)
    def _(i):
        advance(i)

    o_ref[...] = jnp.zeros_like(o_ref)
    for b in range(blocks):
        for h in range(2):
            st_ref[b, h, 0:1, :] = jnp.full((1, 4 * TBLK), NEG, jnp.float32)
            st_ref[b, h, 1:2, :] = jnp.zeros((1, 4 * TBLK), jnp.float32)
    al_st[...] = jnp.zeros_like(al_st)
    m_c[...] = jnp.full_like(m_c, NEG)
    l_c[...] = jnp.zeros_like(l_c)
    a_c[...] = jnp.zeros_like(a_c)
    for h in range(2):
        for u in range(UN):
            PP[u][h][...] = jnp.zeros_like(PP[u][h])
    qx[...] = jnp.where(lax.broadcasted_iota(jnp.int32, qx.shape, 0) == 0, NEG, 0.0).astype(jnp.bfloat16)

    def qk(par, i, h):
        b, t = blk[i], tile[i]
        lhs = jnp.concatenate([k_ref[t, :, h * HD:(h + 1) * HD], kx_ref[flag[i]]], axis=1)
        rhs = jnp.concatenate([q_ref[b, h], qx[...]], axis=0)
        s = jnp.dot(lhs, rhs, preferred_element_type=jnp.float32)
        S[par][h][...] = s
        mx_st[par, h] = jnp.max(s.reshape(TK // 8, 8, 4 * TBLK), axis=0)

    def pv(par, i, h, late):
        r = jnp.dot(vt_ref[tile[i], h * HD:(h + 1) * HD, :], PP[par][h][...], preferred_element_type=jnp.float32)
        new = a_c[h] * al_st[par, h] + r
        a_c[h] = new
        late.append((i, h, new))

    def softmax(par, i, h, late):
        s_ref, p_ref = S[par][h], PP[par][h]
        m_prev = jnp.where(first[i] == 1, jnp.full((1, 4 * TBLK), NEG, jnp.float32), m_c[h])
        m_new = jnp.maximum(m_prev, jnp.max(mx_st[par, h], axis=0, keepdims=True))
        m_c[h] = m_new
        alpha = jnp.exp2((m_prev - m_new) * C)
        al_st[par, h] = alpha
        ls = None
        for c in range(TK // CH):
            p = jnp.exp2((s_ref[c * CH:(c + 1) * CH, :] - m_new) * C)
            v = jnp.sum(p.reshape(CH // 8, 8, 4 * TBLK), axis=0)
            ls = v if ls is None else ls + v
            p_ref[c * CH:(c + 1) * CH, :] = p.astype(jnp.bfloat16)
        l_new = l_c[h] * alpha + ls
        l_c[h] = l_new
        late.append((i, h, m_new, jnp.sum(l_new, axis=0, keepdims=True)))

    def flush(late):
        for i, h, *v in late:
            if len(v) == 1:
                o_ref[blk[i], h] = v[0].astype(jnp.bfloat16)
            else:
                st_ref[blk[i], h, 0:1, :] = v[0]
                st_ref[blk[i], h, 1:2, :] = v[1]

    for u in range(PB):
        for h in range(2):
            qk(u, PB + u, h)

    us = [(u, h) for u in range(PB) for h in range(2)]

    def block(base, i):
        late = []
        for u, h in us:
            qk((base + u + PB) % UN, i + u + PB, h)
        for u, h in us:
            pv((base + u - PB) % UN, i + u - PB, h, late)
        for u, h in us:
            softmax((base + u) % UN, i + u, h, late)
        flush(late)

    def tail(base, i):
        late = []
        for u, h in us:
            pv((base + u) % UN, i + u, h, late)
        flush(late)

    R = UN // PB

    @pl.loop(0, lax.div(n + R, R))
    def _(j):
        for r in range(R):
            step = j * R + r

            @pl.when(step < n)
            def _():
                block(r * PB, (step + 1) * PB)

            @pl.when((step == n) & (n > 0))
            def _():
                tail(((r - 1) * PB) % UN, step * PB)


def attention(nv, q, k, vt, kx):
    blocks = nv.shape[0]
    sm = pl.BlockSpec(memory_space=pltpu.SMEM)
    vm = pl.BlockSpec(memory_space=pltpu.VMEM)
    f32, bf = jnp.float32, jnp.bfloat16
    w = 4 * TBLK
    table = pltpu.SMEM((blocks * k.shape[0] + 4 * PB,), jnp.int32)
    return pl.pallas_call(
        attn_kernel,
        out_shape=(jax.ShapeDtypeStruct((blocks, 2, HD, w), bf), jax.ShapeDtypeStruct((blocks, 2, 2, w), f32)),
        in_specs=[sm] + [vm] * 4,
        out_specs=(vm, vm),
        scratch_shapes=[pltpu.VMEM((TK, w), f32)] * (2 * UN) + [pltpu.VMEM((TK, w), bf)] * (2 * UN) + [
            pltpu.VMEM((UN, 2, 8, w), f32), pltpu.VMEM((UN, 2, 1, w), f32), pltpu.VMEM((2, 1, w), f32),
            pltpu.VMEM((2, 8, w), f32), pltpu.VMEM((2, HD, w), f32), pltpu.VMEM((HD, w), bf),
            pltpu.SMEM((blocks,), jnp.int32), pltpu.SMEM((blocks,), jnp.int32), table, table, table, table],
        compiler_params=pltpu.CompilerParams(vmem_limit_bytes=24 * 1024 * 1024),
        cost_estimate=pl.CostEstimate(flops=10**10, bytes_accessed=10**7, transcendentals=10**7),
        name="attend",
    )(nv, q, k, vt, kx)


MESH_ID = pl.DeviceIdType.MESH


def gather_kernel(text_hbm, k_hbm, v_hbm, wq_hbm, len_ref, lim_ref, nv_ref, q_all, k_all, vt_all, kx_all,
                  text_ref, v_ref, tx, relay, wq, part, ends, in_sem, t1s, t1r, t2s, t2r, t3s, t3r, t4s, t4r, ks, kr, qs_, qr):
    zl, y, x = lax.axis_index("zl"), lax.axis_index("y"), lax.axis_index("x")
    zh, core = lax.axis_index("zh"), lax.axis_index("core")
    inner = {"zl": 1 - zl}
    outer = {"zh": 1 - zh, "zl": 1 - zl}
    other = {"core": 1 - core}
    yp, ym = {"y": lax.rem(y + 1, 4)}, {"y": lax.rem(y + 3, 4)}
    xp, xm = {"x": lax.rem(x + 1, 4)}, {"x": lax.rem(x + 3, 4)}

    c_me = zl * 4 + y
    loads = [pltpu.make_async_copy(src, dst, in_sem.at[i]) for i, (src, dst) in enumerate(
        ((v_hbm, v_ref), (text_hbm, text_ref), (k_hbm, k_all.at[c_me]), (wq_hbm, wq)))]
    for c in loads:
        c.start()
    barrier = pltpu.get_barrier_semaphore()
    for peer in (inner, outer, other, yp, ym, xp, xm):
        pl.semaphore_signal(barrier, inc=1, device_id=peer, device_id_type=MESH_ID)
    loads[0].wait()
    vt_all[c_me] = v_ref[...].astype(jnp.float32).T.astype(jnp.bfloat16)
    loads[1].wait()
    loads[2].wait()
    pl.semaphore_wait(barrier, 7)

    def copy(src, dst, ssem, rsem, dev):
        return pltpu.make_async_remote_copy(src_ref=src, dst_ref=dst, send_sem=ssem, recv_sem=rsem,
                                            device_id=dev, device_id_type=MESH_ID)

    rows = text_ref.shape[0]
    step = rows // 4
    piece = [pl.ds(p * step, step) for p in range(4)]
    started = []

    def go(c):
        c.start()
        started.append(c)
        return c

    t1 = [go(copy(text_ref.at[piece[p]], relay.at[p], t1s.at[p], t1r.at[p], outer if p % 2 else inner)) for p in (1, 0, 3, 2)]
    t1 = {p: c for p, c in zip((1, 0, 3, 2), t1)}
    t3 = go(copy(text_ref, tx.at[0], t3s, t3r, other))
    c_in = (1 - zl) * 4 + y
    c_m, c_p = zl * 4 + lax.rem(y + 3, 4), zl * 4 + lax.rem(y + 1, 4)
    cz_m, cz_p = (1 - zl) * 4 + lax.rem(y + 3, 4), (1 - zl) * 4 + lax.rem(y + 1, 4)
    K = lambda c: k_all.at[c]
    V = lambda c: vt_all.at[c]
    sem = iter(range(15))
    c_2 = zl * 4 + lax.rem(y + 2, 4)
    vh = vt_all.shape[1] // 2
    VH = lambda c, i: vt_all.at[c, pl.ds(i * vh, vh)]

    def kv(src, dst, dev):
        i = next(sem)
        return go(copy(src, dst, ks.at[i], kr.at[i], dev))

    a_kp = kv(K(c_me), K(c_me), yp)
    a_vm = kv(V(c_me), V(c_me), ym)
    a_vp = kv(V(c_me), V(c_me), yp)
    a_km = kv(K(c_me), K(c_me), ym)
    t2 = {}
    for p in (1, 0, 3, 2):
        t1[p].wait_recv()
        t2[p] = go(copy(relay.at[p], tx.at[1, piece[p]], t2s.at[p], t2r.at[p], inner if p % 2 else outer))
    z_k = kv(K(c_me), K(c_me), inner)
    z_v = kv(V(c_me), V(c_me), inner)
    a_kp.wait_recv()
    f_k = kv(K(c_m), K(c_m), yp)
    a_vm.wait_recv()
    f_v = kv(V(c_p), V(c_p), ym)

    NT = GROUP * HD
    half = rows // 2

    def project(src, slot, h, first, last):
        r = pl.ds(h * half, half)

        @pl.loop(0, wq.shape[2] // NT)
        def _(n):
            cols = pl.ds(pl.multiple_of(n * NT, NT), NT)
            d = jnp.dot(src[0][r, :], wq[slot[0], :, cols], preferred_element_type=jnp.float32)
            d = d + jnp.dot(src[1][r, :], wq[slot[1], :, cols], preferred_element_type=jnp.float32)
            if not first:
                d = d + part[r, cols]
            if last:
                for b in range(half // TBLK):
                    heads = [d[b * TBLK:(b + 1) * TBLK, g * HD:(g + 1) * HD] for g in range(GROUP)]
                    q_all[x, h * (half // TBLK) + b, n] = jnp.concatenate(heads, axis=0).T.astype(jnp.bfloat16)
            else:
                part[r, cols] = d

    ends[0] = jnp.int32(0)
    for f in range(len_ref.shape[0]):
        ends[f + 1] = ends[f] + len_ref[f]
    blocks = nv_ref.shape[0]
    chunk = k_all.shape[1]
    spot = lax.broadcasted_iota(jnp.int32, kx_all.shape[1:], 0)
    for b in range(blocks):
        seen = ends[lim_ref[c_me * blocks + b]]
        tail = jnp.clip((seen & (4 * chunk - 1)) - x * chunk, 0, chunk)
        mine = lax.shift_right_logical(seen, (4 * chunk).bit_length() - 1) * chunk + tail
        nv_ref[b] = mine
        edge = mine & (TK - 1)
        kx_all[b] = jnp.where(spot < jnp.where(edge == 0, TK, edge), 0.0, 1.0).astype(jnp.bfloat16)
    kx_all[blocks] = jnp.zeros(kx_all.shape[1:], jnp.bfloat16)
    kx_all[blocks + 1] = jnp.ones(kx_all.shape[1:], jnp.bfloat16)
    loads[3].wait()
    t3.wait_recv()
    mine = zh * 2 + core
    beside = zh * 2 + 1 - core
    far = (1 - zh) * 2 + core
    far_beside = (1 - zh) * 2 + 1 - core
    for h in range(2):
        project((text_ref, tx.at[0]), (mine, beside), h, True, False)
    t4 = {}
    for p in (1, 0, 3, 2):
        t2[p].wait_recv()
        t4[p] = go(copy(tx.at[1, piece[p]], tx.at[2, piece[p]], t4s.at[p], t4r.at[p], other))
    halves = [pl.ds(h * (half // TBLK), half // TBLK) for h in range(2)]
    q = {}

    def qcopy(i, src_x, h, dev):
        ref = q_all.at[src_x, halves[h]]
        return go(copy(ref, ref, qs_.at[i], qr.at[i], dev))

    for h in range(2):
        for p in (2 * h, 2 * h + 1):
            t4[p].wait_recv()
        project((tx.at[1], tx.at[2]), (far, far_beside), h, False, True)
        q[h, 1] = qcopy(2 * h, x, h, xp)
        q[h, -1] = qcopy(2 * h + 1, x, h, xm)
    z_k.wait_recv()
    b_kp = kv(K(c_in), K(c_in), yp)
    b_km = kv(K(c_in), K(c_in), ym)
    q[0, 1].wait_recv()
    q_f = qcopy(4, lax.rem(x + 3, 4), 0, xp)
    f_k.wait_recv()
    g_k = kv(K(c_2), K(c_2), inner)
    z_v.wait_recv()
    b_vm = kv(V(c_in), V(c_in), ym)
    b_vp = kv(V(c_in), V(c_in), yp)
    q[1, -1].wait_recv()
    q_b = qcopy(5, lax.rem(x + 1, 4), 1, xm)
    b_vm.wait_recv()
    g_v = kv(VH(cz_p, 1), VH(cz_p, 1), ym)
    b_vp.wait_recv()
    g_w = kv(VH(cz_m, 0), VH(cz_m, 0), yp)
    for c in (a_vp, a_km, f_v, q[0, -1], q[1, 1], q_f, q_b, b_km, b_kp, g_k, g_v, g_w):
        c.wait_recv()
    for c in started:
        c.wait_send()


def gather_all(text, keys, values, wq, lengths, limits):
    rows, width = text.shape
    bf = jnp.bfloat16
    blocks = 4 * rows // TBLK
    vm = pl.BlockSpec(memory_space=pltpu.VMEM)
    sm = pl.BlockSpec(memory_space=pltpu.SMEM)
    hbm = pl.BlockSpec(memory_space=pltpu.HBM)
    dma = pltpu.SemaphoreType.DMA
    return pl.pallas_call(
        gather_kernel,
        out_shape=(
            jax.ShapeDtypeStruct((blocks,), jnp.int32),
            jax.ShapeDtypeStruct((4, rows // TBLK, 2, HD, GROUP * TBLK), bf),
            jax.ShapeDtypeStruct((8, *keys.shape), bf),
            jax.ShapeDtypeStruct((8, *values.shape[::-1]), bf),
            jax.ShapeDtypeStruct((blocks + 2, TK, HD), bf),
        ),
        in_specs=[hbm] * 4 + [sm] * 2,
        out_specs=(sm, vm, vm, vm, vm),
        scratch_shapes=[
            pltpu.VMEM((rows, width), bf),
            pltpu.VMEM(values.shape, bf),
            pltpu.VMEM((3, rows, width), bf),
            pltpu.VMEM((4, rows // 4, width), bf),
            pltpu.VMEM((4, width, wq.shape[1]), bf),
            pltpu.VMEM((rows, wq.shape[1]), jnp.float32),
            pltpu.SMEM((lengths.shape[0] + 1,), jnp.int32),
            dma((4,)), dma((4,)), dma((4,)), dma((4,)), dma((4,)), dma, dma, dma((4,)), dma((4,)), dma((15,)), dma((15,)), dma((6,)), dma((6,)),
        ],
        compiler_params=pltpu.CompilerParams(collective_id=0, has_side_effects=True, vmem_limit_bytes=40 * 1024 * 1024),
        cost_estimate=pl.CostEstimate(flops=2 * rows * 4 * width * wq.shape[1], bytes_accessed=20 * 2**20, transcendentals=0),
        name="gather",
    )(text, keys, values, wq.reshape(4, width, wq.shape[1]), lengths, limits)


def combine_kernel(gate_ref, o_ref, st_ref, wo, out_ref, og, orel, merged, stg, st_far, attn, pair_out, pair_in, keep, zs, zrel, zin,
                   sts, str_, rs, rr, ds_, dr, cs, cr, as_, ar, bs, br):
    zl, y, x = lax.axis_index("zl"), lax.axis_index("y"), lax.axis_index("x")
    zh, core = lax.axis_index("zh"), lax.axis_index("core")
    inner = {"zl": 1 - zl}
    outer = {"zh": 1 - zh, "zl": 1 - zl}
    other = {"core": 1 - core}
    ip, im, i2 = lax.rem(x + 1, 4), lax.rem(x + 3, 4), lax.rem(x + 2, 4)
    xp, xm, x2 = {"x": ip}, {"x": im}, {"x": i2}

    barrier = pltpu.get_barrier_semaphore()
    for peer in (inner, outer, other, xp, xm, x2):
        pl.semaphore_signal(barrier, inc=1, device_id=peer, device_id_type=MESH_ID)
    pl.semaphore_wait(barrier, 6)
    started = []

    def go(src, dst, ssem, rsem, dev):
        c = pltpu.make_async_remote_copy(src_ref=src, dst_ref=dst, send_sem=ssem, recv_sem=rsem,
                                         device_id=dev, device_id_type=MESH_ID)
        c.start()
        started.append(c)
        return c

    nb = out_ref.shape[0] // TBLK
    stc = [go(st_ref.at[pl.ds(i * nb, nb)], stg.at[s], sts.at[s], str_.at[s], dev)
           for s, i, dev in ((0, ip, xp), (1, im, xm), (2, i2, x2))]
    half = nb // 2
    far = [go(st_ref.at[pl.ds(i2 * nb + v * half, half)], st_far.at[v], sts.at[3 + v], str_.at[3 + v], xm if v else xp)
           for v in range(2)]
    to_relay = lambda j: go(o_ref.at[i2 * nb + j], orel.at[j], rs.at[j], rr.at[j], xp if j < half else xm)
    direct = lambda j, s: go(o_ref.at[(im if s else ip) * nb + j], og.at[s, j], ds_.at[s, j], dr.at[s, j], xm if s else xp)
    r, d = {}, {}

    def merge(j):
        v = j // half
        dest = (im if v else ip) * nb + j
        r[j].wait_recv()
        for h in range(2):
            m1 = st_ref[dest, h, 0:1, :]
            m2 = st_far[v, j - v * half, h, 0:1, :]
            best = jnp.maximum(m1, m2)
            both = o_ref[dest, h].astype(jnp.float32) * jnp.exp2((m1 - best) * C)
            both = both + orel[j, h].astype(jnp.float32) * jnp.exp2((m2 - best) * C)
            merged[j, h] = both.astype(jnp.bfloat16)
        d[j, v] = go(merged.at[j], og.at[v, j], ds_.at[v, j], dr.at[v, j], xm if v else xp)

    r[0] = to_relay(0)
    r[2] = to_relay(2)
    r[1] = to_relay(1)
    r[3] = to_relay(3)
    d[0, 1] = direct(0, 1)
    d[1, 1] = direct(1, 1)
    for c in far:
        c.wait_recv()
    merge(0)
    merge(1)
    d[2, 0] = direct(2, 0)
    d[3, 0] = direct(3, 0)
    merge(2)
    merge(3)
    for c in stc:
        c.wait_recv()
    gate = gate_ref[0]
    width = out_ref.shape[1]
    pairs, z1, z2 = {}, {}, {}

    def mix_and_project(j):
        near = j // half
        for c in (d[j, 0], d[j, 1]):
            c.wait_recv()
        for h in range(2):
            m = [st_ref[x * nb + j, h, 0:1, :]] + [stg[s, j, h, 0:1, :] for s in range(3)]
            l = [st_ref[x * nb + j, h, 1:2, :]] + [stg[s, j, h, 1:2, :] for s in range(3)]
            best = jnp.maximum(jnp.maximum(m[0], m[1]), jnp.maximum(m[2], m[3]))
            scale = [jnp.exp2((m[s] - best) * C) for s in range(4)]
            total = jnp.maximum((l[0] * scale[0] + l[1] * scale[1]) + (l[2] * scale[2] + l[3] * scale[3]), 1.0)
            joint = jnp.exp2((jnp.maximum(m[near + 1], m[3]) - best) * C)
            mixed = o_ref[x * nb + j, h].astype(jnp.float32) * (scale[0] / total)
            mixed = mixed + og[near, j, h].astype(jnp.float32) * (joint / total)
            mixed = mixed + og[1 - near, j, h].astype(jnp.float32) * (scale[2 - near] / total)
            mixed = mixed.T.astype(jnp.bfloat16)
            for g in range(GROUP):
                col = (h * GROUP + g) * HD
                attn[:, col:col + HD] = mixed[g * TBLK:(g + 1) * TBLK, :]
        def proj(zo, co):
            cols = pl.ds(pl.multiple_of((zo * 2 + co) * width, width), width)
            return jnp.dot(attn[...], wo[:, cols], preferred_element_type=jnp.float32)
        for zo in range(2):
            pair_out[j, zo] = proj(zo, 1 - core).astype(jnp.bfloat16)
        pairs[j] = go(pair_out.at[j], pair_in.at[j], cs.at[j], cr.at[j], other)
        keep[j, 1] = proj(1 - zh, core)
        keep[j, 0] = proj(zh, core)

    hh = TBLK // 2

    def sum_pair(j):
        pairs[j].wait_recv()
        zs[j] = (keep[j, 1] + pair_in[j, 1 - zh].astype(jnp.float32)).astype(jnp.bfloat16)
        for v, dev in ((0, inner), (1, outer)):
            part = pl.ds(v * hh, hh)
            z1[j, v] = go(zs.at[j, part], zrel.at[j, v], as_.at[j, v], ar.at[j, v], dev)
        keep[j, 0] = keep[j, 0] + pair_in[j, zh].astype(jnp.float32)

    def relay_z(j):
        for v, dev in ((0, outer), (1, inner)):
            z1[j, v].wait_recv()
            z2[j, v] = go(zrel.at[j, v], zin.at[j, pl.ds(v * hh, hh)], bs.at[j, v], br.at[j, v], dev)

    def finish(j):
        for v in range(2):
            z2[j, v].wait_recv()
        out_ref[j * TBLK:(j + 1) * TBLK, :] = (gate * (keep[j, 0] + zin[j].astype(jnp.float32))).astype(jnp.bfloat16)

    for j in range(nb + 3):
        if j < nb:
            mix_and_project(j)
            sum_pair(j)
        if 1 <= j <= nb:
            relay_z(j - 1)
        if 2 <= j <= nb + 1:
            finish(j - 2)
    for c in started:
        c.wait_send()


def combine_all(gate, o, st, wo, rows):
    bf = jnp.bfloat16
    nb = rows // TBLK
    width = wo.shape[1] // 4
    vm = pl.BlockSpec(memory_space=pltpu.VMEM)
    dma = pltpu.SemaphoreType.DMA
    tile = o.shape[1:]
    return pl.pallas_call(
        combine_kernel,
        out_shape=jax.ShapeDtypeStruct((rows, width), bf),
        in_specs=[pl.BlockSpec(memory_space=pltpu.SMEM), vm, vm, vm],
        out_specs=vm,
        scratch_shapes=[
            pltpu.VMEM((2, nb, *tile), bf),
            pltpu.VMEM((nb, *tile), bf),
            pltpu.VMEM((nb, *tile), bf),
            pltpu.VMEM((3, nb, *st.shape[1:]), jnp.float32),
            pltpu.VMEM((2, nb // 2, *st.shape[1:]), jnp.float32),
            pltpu.VMEM((TBLK, wo.shape[0]), bf),
            pltpu.VMEM((nb, 2, TBLK, width), bf),
            pltpu.VMEM((nb, 2, TBLK, width), bf),
            pltpu.VMEM((nb, 2, TBLK, width), jnp.float32),
            pltpu.VMEM((nb, TBLK, width), bf),
            pltpu.VMEM((nb, 2, TBLK // 2, width), bf),
            pltpu.VMEM((nb, TBLK, width), bf),
            dma((5,)), dma((5,)), dma((4,)), dma((4,)), dma((2, 4)), dma((2, 4)), dma((4,)), dma((4,)),
            dma((4, 2)), dma((4, 2)), dma((4, 2)), dma((4, 2)),
        ],
        compiler_params=pltpu.CompilerParams(collective_id=1, has_side_effects=True, vmem_limit_bytes=24 * 1024 * 1024),
        cost_estimate=pl.CostEstimate(flops=2 * rows * wo.shape[0] * wo.shape[1], bytes_accessed=20 * 2**20, transcendentals=0),
        name="combine",
    )(gate, o, st, wo)


def shards(text, wq, keys, values, wo, gate, lengths, limits):
    here = [pltpu.with_memory_space_constraint(a, pltpu.HBM) for a in (text, keys, values, lengths, limits)]
    nv, q, k, vt, kx = gather_all(*here[:3], wq, *here[3:])
    o, st = attention(nv, q.reshape(-1, *q.shape[2:]), k, vt, kx)
    return combine_all(jnp.tanh(gate), o, st, wo, text.shape[0])


def solution(mesh):
    mesh = Mesh(mesh.devices.reshape(2, 4, 4, 2, 2), ("zl", "y", "x", "zh", "core"))
    seq, head = ("zl", "y", "x"), ("zh", "core")
    in_specs = (P(seq, head), P(None, head), P(seq, head), P(seq, head), P(head, None), P(), P(), P())
    return jax.shard_map(shards, mesh=mesh, in_specs=in_specs, out_specs=P(seq, head), check_vma=False)
```

```python
import math

import jax
import jax.numpy as jnp
from jax import lax
from jax.experimental import pallas as pl
from jax.experimental.pallas import tpu as pltpu
from jax.sharding import Mesh, PartitionSpec as P

HD = 128
TBLK = 64
GROUP = 4
NEG = -1e30
C = math.log2(math.e) / math.sqrt(HD)
TK = 512
CH = 64
UN = 4
PB = 2


def attn_kernel(nv_ref, q_ref, k_ref, vt_ref, kx_ref, o_ref, st_ref, *scr):
    S = [scr[2 * u:2 * u + 2] for u in range(UN)]
    PP = [scr[2 * UN + 2 * u:2 * UN + 2 * u + 2] for u in range(UN)]
    mx_st, al_st, m_c, l_c, a_c, qx, blk, tile, flag = scr[4 * UN:]
    blocks = o_ref.shape[0]

    for i in range(PB):
        blk[i] = 0
        tile[i] = 1
        flag[i] = blocks + 1
    end = jnp.int32(PB)
    last = jnp.int32(0)
    for b in range(blocks):
        count = lax.shift_right_logical(nv_ref[b] + (TK - 1), TK.bit_length() - 1)

        @pl.loop(0, count)
        def _(t):
            blk[end + t] = b
            tile[end + t] = t
            flag[end + t] = blocks

        end = end + count
        last = jnp.where(count > 0, b, last)
        flag[end - 1] = jnp.where(count > 0, b, flag[end - 1])
    for i in range(2 * PB):
        blk[end + i] = last
        tile[end + i] = 1
        flag[end + i] = blocks + 1
    n = lax.shift_right_logical(end - PB + (PB - 1), PB.bit_length() - 1)

    o_ref[...] = jnp.zeros_like(o_ref)
    for b in range(blocks):
        for h in range(2):
            st_ref[b, h, 0:1, :] = jnp.full((1, 4 * TBLK), NEG, jnp.float32)
            st_ref[b, h, 1:2, :] = jnp.zeros((1, 4 * TBLK), jnp.float32)
    al_st[...] = jnp.zeros_like(al_st)
    m_c[...] = jnp.full_like(m_c, NEG)
    l_c[...] = jnp.zeros_like(l_c)
    a_c[...] = jnp.zeros_like(a_c)
    for h in range(2):
        for u in range(UN):
            PP[u][h][...] = jnp.zeros_like(PP[u][h])
    qx[...] = jnp.where(lax.broadcasted_iota(jnp.int32, qx.shape, 0) == 0, NEG, 0.0).astype(jnp.bfloat16)

    def qk(par, i, h):
        b, t = blk[i], tile[i]
        lhs = jnp.concatenate([k_ref[t, :, h * HD:(h + 1) * HD], kx_ref[flag[i]]], axis=1)
        rhs = jnp.concatenate([q_ref[b, h], qx[...]], axis=0)
        s = jnp.dot(lhs, rhs, preferred_element_type=jnp.float32)
        S[par][h][...] = s
        mx_st[par, h] = jnp.max(s.reshape(TK // 8, 8, 4 * TBLK), axis=0)

    def pv(par, i, h, late):
        r = jnp.dot(vt_ref[tile[i], h * HD:(h + 1) * HD, :], PP[par][h][...], preferred_element_type=jnp.float32)
        new = a_c[h] * al_st[par, h] + r
        a_c[h] = new
        late.append((i, h, new))

    def softmax(par, i, h, late):
        s_ref, p_ref = S[par][h], PP[par][h]
        m_prev = jnp.where(tile[i] == 0, jnp.full((1, 4 * TBLK), NEG, jnp.float32), m_c[h])
        m_new = jnp.maximum(m_prev, jnp.max(mx_st[par, h], axis=0, keepdims=True))
        m_c[h] = m_new
        alpha = jnp.exp2((m_prev - m_new) * C)
        al_st[par, h] = alpha
        ls = None
        for c in range(TK // CH):
            p = jnp.exp2((s_ref[c * CH:(c + 1) * CH, :] - m_new) * C)
            v = jnp.sum(p.reshape(CH // 8, 8, 4 * TBLK), axis=0)
            ls = v if ls is None else ls + v
            p_ref[c * CH:(c + 1) * CH, :] = p.astype(jnp.bfloat16)
        l_new = l_c[h] * alpha + ls
        l_c[h] = l_new
        late.append((i, h, m_new, jnp.sum(l_new, axis=0, keepdims=True)))

    def flush(late):
        for i, h, *v in late:
            if len(v) == 1:
                o_ref[blk[i], h] = v[0].astype(jnp.bfloat16)
            else:
                st_ref[blk[i], h, 0:1, :] = v[0]
                st_ref[blk[i], h, 1:2, :] = v[1]

    for u in range(PB):
        for h in range(2):
            qk(u, PB + u, h)

    us = [(u, h) for u in range(PB) for h in range(2)]

    def block(base, i):
        late = []
        for u, h in us:
            qk((base + u + PB) % UN, i + u + PB, h)
        for u, h in us:
            pv((base + u - PB) % UN, i + u - PB, h, late)
        for u, h in us:
            softmax((base + u) % UN, i + u, h, late)
        flush(late)

    def tail(base, i):
        late = []
        for u, h in us:
            pv((base + u) % UN, i + u, h, late)
        flush(late)

    R = UN // PB

    @pl.loop(0, lax.div(n + R, R))
    def _(j):
        for r in range(R):
            step = j * R + r

            @pl.when(step < n)
            def _():
                block(r * PB, (step + 1) * PB)

            @pl.when((step == n) & (n > 0))
            def _():
                tail(((r - 1) * PB) % UN, step * PB)


def attention(nv, q, k, vt, kx):
    blocks = nv.shape[0]
    sm = pl.BlockSpec(memory_space=pltpu.SMEM)
    vm = pl.BlockSpec(memory_space=pltpu.VMEM)
    f32, bf = jnp.float32, jnp.bfloat16
    w = 4 * TBLK
    table = pltpu.SMEM((blocks * k.shape[0] + 4 * PB,), jnp.int32)
    return pl.pallas_call(
        attn_kernel,
        out_shape=(jax.ShapeDtypeStruct((blocks, 2, HD, w), bf), jax.ShapeDtypeStruct((blocks, 2, 2, w), f32)),
        in_specs=[sm] + [vm] * 4,
        out_specs=(vm, vm),
        scratch_shapes=[pltpu.VMEM((TK, w), f32)] * (2 * UN) + [pltpu.VMEM((TK, w), bf)] * (2 * UN) + [
            pltpu.VMEM((UN, 2, 8, w), f32), pltpu.VMEM((UN, 2, 1, w), f32), pltpu.VMEM((2, 1, w), f32),
            pltpu.VMEM((2, 8, w), f32), pltpu.VMEM((2, HD, w), f32), pltpu.VMEM((HD, w), bf),
            table, table, table],
        compiler_params=pltpu.CompilerParams(vmem_limit_bytes=24 * 1024 * 1024),
        cost_estimate=pl.CostEstimate(flops=10**10, bytes_accessed=10**7, transcendentals=10**7),
        name="attend",
    )(nv, q, k, vt, kx)


MESH_ID = pl.DeviceIdType.MESH


def gather_kernel(text_hbm, k_hbm, v_hbm, wq_hbm, len_ref, lim_ref, nv_ref, q_all, k_all, vt_all, kx_all,
                  text_ref, v_ref, tx, relay, wq, part, ends, in_sem, t1s, t1r, t2s, t2r, t3s, t3r, t4s, t4r, ks, kr, qs_, qr):
    zl, y, x = lax.axis_index("zl"), lax.axis_index("y"), lax.axis_index("x")
    zh, core = lax.axis_index("zh"), lax.axis_index("core")
    inner = {"zl": 1 - zl}
    outer = {"zh": 1 - zh, "zl": 1 - zl}
    other = {"core": 1 - core}
    yp, ym = {"y": lax.rem(y + 1, 4)}, {"y": lax.rem(y + 3, 4)}
    xp, xm = {"x": lax.rem(x + 1, 4)}, {"x": lax.rem(x + 3, 4)}

    c_me = zl * 4 + y
    loads = [pltpu.make_async_copy(src, dst, in_sem.at[i]) for i, (src, dst) in enumerate(
        ((v_hbm, v_ref), (text_hbm, text_ref), (k_hbm, k_all.at[c_me]), (wq_hbm, wq)))]
    for c in loads:
        c.start()
    barrier = pltpu.get_barrier_semaphore()
    for peer in (inner, outer, other, yp, ym, xp, xm):
        pl.semaphore_signal(barrier, inc=1, device_id=peer, device_id_type=MESH_ID)
    loads[0].wait()
    vt_all[c_me] = v_ref[...].astype(jnp.float32).T.astype(jnp.bfloat16)
    loads[1].wait()
    loads[2].wait()
    pl.semaphore_wait(barrier, 7)

    def copy(src, dst, ssem, rsem, dev):
        return pltpu.make_async_remote_copy(src_ref=src, dst_ref=dst, send_sem=ssem, recv_sem=rsem,
                                            device_id=dev, device_id_type=MESH_ID)

    rows = text_ref.shape[0]
    step = rows // 4
    piece = [pl.ds(p * step, step) for p in range(4)]
    started = []

    def go(c):
        c.start()
        started.append(c)
        return c

    t1 = [go(copy(text_ref.at[piece[p]], relay.at[p], t1s.at[p], t1r.at[p], outer if p % 2 else inner)) for p in (1, 0, 3, 2)]
    t1 = {p: c for p, c in zip((1, 0, 3, 2), t1)}
    t3 = go(copy(text_ref, tx.at[0], t3s, t3r, other))
    c_in = (1 - zl) * 4 + y
    c_m, c_p = zl * 4 + lax.rem(y + 3, 4), zl * 4 + lax.rem(y + 1, 4)
    cz_m, cz_p = (1 - zl) * 4 + lax.rem(y + 3, 4), (1 - zl) * 4 + lax.rem(y + 1, 4)
    K = lambda c: k_all.at[c]
    V = lambda c: vt_all.at[c]
    sem = iter(range(15))
    c_2 = zl * 4 + lax.rem(y + 2, 4)
    vh = vt_all.shape[1] // 2
    VH = lambda c, i: vt_all.at[c, pl.ds(i * vh, vh)]

    def kv(src, dst, dev):
        i = next(sem)
        return go(copy(src, dst, ks.at[i], kr.at[i], dev))

    a_kp = kv(K(c_me), K(c_me), yp)
    a_vm = kv(V(c_me), V(c_me), ym)
    a_vp = kv(V(c_me), V(c_me), yp)
    a_km = kv(K(c_me), K(c_me), ym)
    t2 = {}
    for p in (1, 0, 3, 2):
        t1[p].wait_recv()
        t2[p] = go(copy(relay.at[p], tx.at[1, piece[p]], t2s.at[p], t2r.at[p], inner if p % 2 else outer))
    z_k = kv(K(c_me), K(c_me), inner)
    z_v = kv(V(c_me), V(c_me), inner)
    a_kp.wait_recv()
    f_k = kv(K(c_m), K(c_m), yp)
    a_vm.wait_recv()
    f_v = kv(V(c_p), V(c_p), ym)

    NT = GROUP * HD
    half = rows // 2

    def project(src, slot, h, first, last):
        r = pl.ds(h * half, half)

        @pl.loop(0, wq.shape[2] // NT)
        def _(n):
            cols = pl.ds(pl.multiple_of(n * NT, NT), NT)
            d = jnp.dot(src[0][r, :], wq[slot[0], :, cols], preferred_element_type=jnp.float32)
            d = d + jnp.dot(src[1][r, :], wq[slot[1], :, cols], preferred_element_type=jnp.float32)
            if not first:
                d = d + part[r, cols]
            if last:
                for b in range(half // TBLK):
                    heads = [d[b * TBLK:(b + 1) * TBLK, g * HD:(g + 1) * HD] for g in range(GROUP)]
                    q_all[x, h * (half // TBLK) + b, n] = jnp.concatenate(heads, axis=0).T.astype(jnp.bfloat16)
            else:
                part[r, cols] = d

    ends[0] = jnp.int32(0)
    for f in range(len_ref.shape[0]):
        ends[f + 1] = ends[f] + len_ref[f]
    blocks = nv_ref.shape[0]
    chunk = k_all.shape[1]
    spot = lax.broadcasted_iota(jnp.int32, kx_all.shape[1:], 0)
    for b in range(blocks):
        seen = ends[lim_ref[c_me * blocks + b]]
        tail = jnp.clip((seen & (4 * chunk - 1)) - x * chunk, 0, chunk)
        mine = lax.shift_right_logical(seen, (4 * chunk).bit_length() - 1) * chunk + tail
        nv_ref[b] = mine
        edge = mine & (TK - 1)
        kx_all[b] = jnp.where(spot < jnp.where(edge == 0, TK, edge), 0.0, 1.0).astype(jnp.bfloat16)
    kx_all[blocks] = jnp.zeros(kx_all.shape[1:], jnp.bfloat16)
    kx_all[blocks + 1] = jnp.ones(kx_all.shape[1:], jnp.bfloat16)
    loads[3].wait()
    t3.wait_recv()
    mine = zh * 2 + core
    beside = zh * 2 + 1 - core
    far = (1 - zh) * 2 + core
    far_beside = (1 - zh) * 2 + 1 - core
    for h in range(2):
        project((text_ref, tx.at[0]), (mine, beside), h, True, False)
    t4 = {}
    for p in (1, 0, 3, 2):
        t2[p].wait_recv()
        t4[p] = go(copy(tx.at[1, piece[p]], tx.at[2, piece[p]], t4s.at[p], t4r.at[p], other))
    halves = [pl.ds(h * (half // TBLK), half // TBLK) for h in range(2)]
    q = {}

    def qcopy(i, src_x, h, dev):
        ref = q_all.at[src_x, halves[h]]
        return go(copy(ref, ref, qs_.at[i], qr.at[i], dev))

    for h in range(2):
        for p in (2 * h, 2 * h + 1):
            t4[p].wait_recv()
        project((tx.at[1], tx.at[2]), (far, far_beside), h, False, True)
        q[h, 1] = qcopy(2 * h, x, h, xp)
        q[h, -1] = qcopy(2 * h + 1, x, h, xm)
    z_k.wait_recv()
    b_kp = kv(K(c_in), K(c_in), yp)
    b_km = kv(K(c_in), K(c_in), ym)
    q[0, 1].wait_recv()
    q_f = qcopy(4, lax.rem(x + 3, 4), 0, xp)
    f_k.wait_recv()
    g_k = kv(K(c_2), K(c_2), inner)
    z_v.wait_recv()
    b_vm = kv(V(c_in), V(c_in), ym)
    b_vp = kv(V(c_in), V(c_in), yp)
    q[1, -1].wait_recv()
    q_b = qcopy(5, lax.rem(x + 1, 4), 1, xm)
    b_vm.wait_recv()
    g_v = kv(VH(cz_p, 1), VH(cz_p, 1), ym)
    b_vp.wait_recv()
    g_w = kv(VH(cz_m, 0), VH(cz_m, 0), yp)
    for c in (a_vp, a_km, f_v, q[0, -1], q[1, 1], q_f, q_b, b_km, b_kp, g_k, g_v, g_w):
        c.wait_recv()
    for c in started:
        c.wait_send()


def gather_all(text, keys, values, wq, lengths, limits):
    rows, width = text.shape
    bf = jnp.bfloat16
    blocks = 4 * rows // TBLK
    vm = pl.BlockSpec(memory_space=pltpu.VMEM)
    sm = pl.BlockSpec(memory_space=pltpu.SMEM)
    hbm = pl.BlockSpec(memory_space=pltpu.HBM)
    dma = pltpu.SemaphoreType.DMA
    return pl.pallas_call(
        gather_kernel,
        out_shape=(
            jax.ShapeDtypeStruct((blocks,), jnp.int32),
            jax.ShapeDtypeStruct((4, rows // TBLK, 2, HD, GROUP * TBLK), bf),
            jax.ShapeDtypeStruct((8, *keys.shape), bf),
            jax.ShapeDtypeStruct((8, *values.shape[::-1]), bf),
            jax.ShapeDtypeStruct((blocks + 2, TK, HD), bf),
        ),
        in_specs=[hbm] * 4 + [sm] * 2,
        out_specs=(sm, vm, vm, vm, vm),
        scratch_shapes=[
            pltpu.VMEM((rows, width), bf),
            pltpu.VMEM(values.shape, bf),
            pltpu.VMEM((3, rows, width), bf),
            pltpu.VMEM((4, rows // 4, width), bf),
            pltpu.VMEM((4, width, wq.shape[1]), bf),
            pltpu.VMEM((rows, wq.shape[1]), jnp.float32),
            pltpu.SMEM((lengths.shape[0] + 1,), jnp.int32),
            dma((4,)), dma((4,)), dma((4,)), dma((4,)), dma((4,)), dma, dma, dma((4,)), dma((4,)), dma((15,)), dma((15,)), dma((6,)), dma((6,)),
        ],
        compiler_params=pltpu.CompilerParams(collective_id=0, has_side_effects=True, vmem_limit_bytes=40 * 1024 * 1024),
        cost_estimate=pl.CostEstimate(flops=2 * rows * 4 * width * wq.shape[1], bytes_accessed=20 * 2**20, transcendentals=0),
        name="gather",
    )(text, keys, values, wq.reshape(4, width, wq.shape[1]), lengths, limits)


def combine_kernel(gate_ref, o_ref, st_ref, wo, out_ref, og, orel, merged, stg, st_far, attn, pair_out, pair_in, keep, zs, zrel, zin,
                   sts, str_, rs, rr, ds_, dr, cs, cr, as_, ar, bs, br):
    zl, y, x = lax.axis_index("zl"), lax.axis_index("y"), lax.axis_index("x")
    zh, core = lax.axis_index("zh"), lax.axis_index("core")
    inner = {"zl": 1 - zl}
    outer = {"zh": 1 - zh, "zl": 1 - zl}
    other = {"core": 1 - core}
    ip, im, i2 = lax.rem(x + 1, 4), lax.rem(x + 3, 4), lax.rem(x + 2, 4)
    xp, xm, x2 = {"x": ip}, {"x": im}, {"x": i2}

    barrier = pltpu.get_barrier_semaphore()
    for peer in (inner, outer, other, xp, xm, x2):
        pl.semaphore_signal(barrier, inc=1, device_id=peer, device_id_type=MESH_ID)
    pl.semaphore_wait(barrier, 6)
    started = []

    def go(src, dst, ssem, rsem, dev):
        c = pltpu.make_async_remote_copy(src_ref=src, dst_ref=dst, send_sem=ssem, recv_sem=rsem,
                                         device_id=dev, device_id_type=MESH_ID)
        c.start()
        started.append(c)
        return c

    nb = out_ref.shape[0] // TBLK
    stc = [go(st_ref.at[pl.ds(i * nb, nb)], stg.at[s], sts.at[s], str_.at[s], dev)
           for s, i, dev in ((0, ip, xp), (1, im, xm), (2, i2, x2))]
    half = nb // 2
    far = [go(st_ref.at[pl.ds(i2 * nb + v * half, half)], st_far.at[v], sts.at[3 + v], str_.at[3 + v], xm if v else xp)
           for v in range(2)]
    to_relay = lambda j: go(o_ref.at[i2 * nb + j], orel.at[j], rs.at[j], rr.at[j], xp if j < half else xm)
    direct = lambda j, s: go(o_ref.at[(im if s else ip) * nb + j], og.at[s, j], ds_.at[s, j], dr.at[s, j], xm if s else xp)
    r, d = {}, {}

    def merge(j):
        v = j // half
        dest = (im if v else ip) * nb + j
        r[j].wait_recv()
        for h in range(2):
            m1 = st_ref[dest, h, 0:1, :]
            m2 = st_far[v, j - v * half, h, 0:1, :]
            best = jnp.maximum(m1, m2)
            both = o_ref[dest, h].astype(jnp.float32) * jnp.exp2((m1 - best) * C)
            both = both + orel[j, h].astype(jnp.float32) * jnp.exp2((m2 - best) * C)
            merged[j, h] = both.astype(jnp.bfloat16)
        d[j, v] = go(merged.at[j], og.at[v, j], ds_.at[v, j], dr.at[v, j], xm if v else xp)

    r[0] = to_relay(0)
    r[2] = to_relay(2)
    r[1] = to_relay(1)
    r[3] = to_relay(3)
    d[0, 1] = direct(0, 1)
    d[1, 1] = direct(1, 1)
    for c in far:
        c.wait_recv()
    merge(0)
    merge(1)
    d[2, 0] = direct(2, 0)
    d[3, 0] = direct(3, 0)
    merge(2)
    merge(3)
    for c in stc:
        c.wait_recv()
    gate = jnp.tanh(jnp.full((1, out_ref.shape[1]), gate_ref[0], jnp.float32))
    width = out_ref.shape[1]
    pairs, z1, z2 = {}, {}, {}

    def mix_and_project(j):
        near = j // half
        for c in (d[j, 0], d[j, 1]):
            c.wait_recv()
        for h in range(2):
            m = [st_ref[x * nb + j, h, 0:1, :]] + [stg[s, j, h, 0:1, :] for s in range(3)]
            l = [st_ref[x * nb + j, h, 1:2, :]] + [stg[s, j, h, 1:2, :] for s in range(3)]
            best = jnp.maximum(jnp.maximum(m[0], m[1]), jnp.maximum(m[2], m[3]))
            scale = [jnp.exp2((m[s] - best) * C) for s in range(4)]
            total = jnp.maximum((l[0] * scale[0] + l[1] * scale[1]) + (l[2] * scale[2] + l[3] * scale[3]), 1.0)
            joint = jnp.exp2((jnp.maximum(m[near + 1], m[3]) - best) * C)
            mixed = o_ref[x * nb + j, h].astype(jnp.float32) * (scale[0] / total)
            mixed = mixed + og[near, j, h].astype(jnp.float32) * (joint / total)
            mixed = mixed + og[1 - near, j, h].astype(jnp.float32) * (scale[2 - near] / total)
            mixed = mixed.T.astype(jnp.bfloat16)
            for g in range(GROUP):
                col = (h * GROUP + g) * HD
                attn[:, col:col + HD] = mixed[g * TBLK:(g + 1) * TBLK, :]
        def proj(zo, co):
            cols = pl.ds(pl.multiple_of((zo * 2 + co) * width, width), width)
            return jnp.dot(attn[...], wo[:, cols], preferred_element_type=jnp.float32)
        def pair(i, zo):
            pair_out[j, i] = proj(zo, 1 - core).astype(jnp.bfloat16)
            pairs[j, i] = go(pair_out.at[j, i], pair_in.at[j, i], cs.at[j, i], cr.at[j, i], other)
            keep[j, i] = proj(zo, core)

        pair(0, 1 - zh)
        pairs[j, 0].wait_recv()
        zs[j] = (keep[j, 0] + pair_in[j, 0].astype(jnp.float32)).astype(jnp.bfloat16)
        for v, dev in ((0, inner), (1, outer)):
            part = pl.ds(v * hh, hh)
            z1[j, v] = go(zs.at[j, part], zrel.at[j, v], as_.at[j, v], ar.at[j, v], dev)
        pair(1, zh)

    hh = TBLK // 2

    def relay_z(j):
        for v, dev in ((0, outer), (1, inner)):
            z1[j, v].wait_recv()
            z2[j, v] = go(zrel.at[j, v], zin.at[j, pl.ds(v * hh, hh)], bs.at[j, v], br.at[j, v], dev)

    def finish(j):
        for v in range(2):
            z2[j, v].wait_recv()
        pairs[j, 1].wait_recv()
        mine = keep[j, 1] + pair_in[j, 1].astype(jnp.float32)
        out_ref[j * TBLK:(j + 1) * TBLK, :] = (gate * (mine + zin[j].astype(jnp.float32))).astype(jnp.bfloat16)

    for j in range(nb + 3):
        if j < nb:
            mix_and_project(j)
        if 1 <= j <= nb:
            relay_z(j - 1)
        if 2 <= j <= nb + 1:
            finish(j - 2)
    for c in started:
        c.wait_send()


def combine_all(gate, o, st, wo, rows):
    bf = jnp.bfloat16
    nb = rows // TBLK
    width = wo.shape[1] // 4
    vm = pl.BlockSpec(memory_space=pltpu.VMEM)
    dma = pltpu.SemaphoreType.DMA
    tile = o.shape[1:]
    return pl.pallas_call(
        combine_kernel,
        out_shape=jax.ShapeDtypeStruct((rows, width), bf),
        in_specs=[pl.BlockSpec(memory_space=pltpu.SMEM), vm, vm, vm],
        out_specs=vm,
        scratch_shapes=[
            pltpu.VMEM((2, nb, *tile), bf),
            pltpu.VMEM((nb, *tile), bf),
            pltpu.VMEM((nb, *tile), bf),
            pltpu.VMEM((3, nb, *st.shape[1:]), jnp.float32),
            pltpu.VMEM((2, nb // 2, *st.shape[1:]), jnp.float32),
            pltpu.VMEM((TBLK, wo.shape[0]), bf),
            pltpu.VMEM((nb, 2, TBLK, width), bf),
            pltpu.VMEM((nb, 2, TBLK, width), bf),
            pltpu.VMEM((nb, 2, TBLK, width), jnp.float32),
            pltpu.VMEM((nb, TBLK, width), bf),
            pltpu.VMEM((nb, 2, TBLK // 2, width), bf),
            pltpu.VMEM((nb, TBLK, width), bf),
            dma((5,)), dma((5,)), dma((4,)), dma((4,)), dma((2, 4)), dma((2, 4)), dma((4, 2)), dma((4, 2)),
            dma((4, 2)), dma((4, 2)), dma((4, 2)), dma((4, 2)),
        ],
        compiler_params=pltpu.CompilerParams(collective_id=1, has_side_effects=True, vmem_limit_bytes=24 * 1024 * 1024),
        cost_estimate=pl.CostEstimate(flops=2 * rows * wo.shape[0] * wo.shape[1], bytes_accessed=20 * 2**20, transcendentals=0),
        name="combine",
    )(gate, o, st, wo)


def shards(text, wq, keys, values, wo, gate, lengths, limits):
    here = [pltpu.with_memory_space_constraint(a, pltpu.HBM) for a in (text, keys, values, lengths, limits)]
    nv, q, k, vt, kx = gather_all(*here[:3], wq, *here[3:])
    o, st = attention(nv, q.reshape(-1, *q.shape[2:]), k, vt, kx)
    return combine_all(gate, o, st, wo, text.shape[0])


def solution(mesh):
    mesh = Mesh(mesh.devices.reshape(2, 4, 4, 2, 2), ("zl", "y", "x", "zh", "core"))
    seq, head = ("zl", "y", "x"), ("zh", "core")
    in_specs = (P(seq, head), P(None, head), P(seq, head), P(seq, head), P(head, None), P(), P(), P())
    return jax.shard_map(shards, mesh=mesh, in_specs=in_specs, out_specs=P(seq, head), check_vma=False)
```

```python
import math

import jax
import jax.numpy as jnp
from jax import lax
from jax.experimental import pallas as pl
from jax.experimental.pallas import tpu as pltpu
from jax.sharding import Mesh, PartitionSpec as P

HD = 128
TBLK = 64
GROUP = 4
NEG = -1e30
C = math.log2(math.e) / math.sqrt(HD)
TK = 512
CH = 64
UN = 4
PB = 2


def attn_kernel(nv_ref, q_ref, k_ref, vt_ref, kx_ref, o_ref, st_ref, *scr):
    S = [scr[2 * u:2 * u + 2] for u in range(UN)]
    PP = [scr[2 * UN + 2 * u:2 * UN + 2 * u + 2] for u in range(UN)]
    mx_st, al_st, m_c, l_c, a_c, qx, blk, tile, flag = scr[4 * UN:]
    blocks = o_ref.shape[0]

    for i in range(PB):
        blk[i] = 0
        tile[i] = 1
        flag[i] = blocks + 1
    end = jnp.int32(PB)
    last = jnp.int32(0)
    for b in range(blocks):
        count = lax.shift_right_logical(nv_ref[b] + (TK - 1), TK.bit_length() - 1)

        @pl.loop(0, count)
        def _(t):
            blk[end + t] = b
            tile[end + t] = t
            flag[end + t] = blocks

        end = end + count
        last = jnp.where(count > 0, b, last)
        flag[end - 1] = jnp.where(count > 0, b, flag[end - 1])
    for i in range(2 * PB):
        blk[end + i] = last
        tile[end + i] = 1
        flag[end + i] = blocks + 1
    n = lax.shift_right_logical(end - PB + (PB - 1), PB.bit_length() - 1)

    for b in range(blocks):
        @pl.when(nv_ref[b] == 0)
        def _():
            o_ref[b] = jnp.zeros(o_ref.shape[1:], o_ref.dtype)

        for h in range(2):
            st_ref[b, h, 0:1, :] = jnp.full((1, 4 * TBLK), NEG, jnp.float32)
            st_ref[b, h, 1:2, :] = jnp.zeros((1, 4 * TBLK), jnp.float32)
    al_st[...] = jnp.zeros_like(al_st)
    m_c[...] = jnp.full_like(m_c, NEG)
    l_c[...] = jnp.zeros_like(l_c)
    a_c[...] = jnp.zeros_like(a_c)
    for h in range(2):
        for u in range(UN - PB, UN):
            PP[u][h][...] = jnp.zeros_like(PP[u][h])
    qx[...] = jnp.where(lax.broadcasted_iota(jnp.int32, qx.shape, 0) == 0, NEG, 0.0).astype(jnp.bfloat16)

    def qk(par, i, h):
        b, t = blk[i], tile[i]
        lhs = jnp.concatenate([k_ref[t, :, h * HD:(h + 1) * HD], kx_ref[flag[i]]], axis=1)
        rhs = jnp.concatenate([q_ref[b, h], qx[...]], axis=0)
        s = jnp.dot(lhs, rhs, preferred_element_type=jnp.float32)
        S[par][h][...] = s
        mx_st[par, h] = jnp.max(s.reshape(TK // 8, 8, 4 * TBLK), axis=0)

    def pv(par, i, h, late):
        r = jnp.dot(vt_ref[tile[i], h * HD:(h + 1) * HD, :], PP[par][h][...], preferred_element_type=jnp.float32)
        new = a_c[h] * al_st[par, h] + r
        a_c[h] = new
        late.append((i, h, new))

    def softmax(par, i, h, late):
        s_ref, p_ref = S[par][h], PP[par][h]
        m_prev = jnp.where(tile[i] == 0, jnp.full((1, 4 * TBLK), NEG, jnp.float32), m_c[h])
        m_new = jnp.maximum(m_prev, jnp.max(mx_st[par, h], axis=0, keepdims=True))
        m_c[h] = m_new
        alpha = jnp.exp2((m_prev - m_new) * C)
        al_st[par, h] = alpha
        ls = None
        for c in range(TK // CH):
            p = jnp.exp2((s_ref[c * CH:(c + 1) * CH, :] - m_new) * C)
            v = jnp.sum(p.reshape(CH // 8, 8, 4 * TBLK), axis=0)
            ls = v if ls is None else ls + v
            p_ref[c * CH:(c + 1) * CH, :] = p.astype(jnp.bfloat16)
        l_new = l_c[h] * alpha + ls
        l_c[h] = l_new
        late.append((i, h, m_new, jnp.sum(l_new, axis=0, keepdims=True)))

    def flush(late):
        for i, h, *v in late:
            if len(v) == 1:
                o_ref[blk[i], h] = v[0].astype(jnp.bfloat16)
            else:
                st_ref[blk[i], h, 0:1, :] = v[0]
                st_ref[blk[i], h, 1:2, :] = v[1]

    for u in range(PB):
        for h in range(2):
            qk(u, PB + u, h)

    us = [(u, h) for u in range(PB) for h in range(2)]

    def block(base, i):
        late = []
        for u, h in us:
            qk((base + u + PB) % UN, i + u + PB, h)
        for u, h in us:
            pv((base + u - PB) % UN, i + u - PB, h, late)
        for u, h in us:
            softmax((base + u) % UN, i + u, h, late)
        flush(late)

    def tail(base, i):
        late = []
        for u, h in us:
            pv((base + u) % UN, i + u, h, late)
        flush(late)

    R = UN // PB

    @pl.loop(0, lax.div(n + R, R))
    def _(j):
        for r in range(R):
            step = j * R + r

            @pl.when(step < n)
            def _():
                block(r * PB, (step + 1) * PB)

            @pl.when((step == n) & (n > 0))
            def _():
                tail(((r - 1) * PB) % UN, step * PB)


def attention(nv, q, k, vt, kx):
    blocks = nv.shape[0]
    sm = pl.BlockSpec(memory_space=pltpu.SMEM)
    vm = pl.BlockSpec(memory_space=pltpu.VMEM)
    f32, bf = jnp.float32, jnp.bfloat16
    w = 4 * TBLK
    table = pltpu.SMEM((blocks * k.shape[0] + 4 * PB,), jnp.int32)
    return pl.pallas_call(
        attn_kernel,
        out_shape=(jax.ShapeDtypeStruct((blocks, 2, HD, w), bf), jax.ShapeDtypeStruct((blocks, 2, 2, w), f32)),
        in_specs=[sm] + [vm] * 4,
        out_specs=(vm, vm),
        scratch_shapes=[pltpu.VMEM((TK, w), f32)] * (2 * UN) + [pltpu.VMEM((TK, w), bf)] * (2 * UN) + [
            pltpu.VMEM((UN, 2, 8, w), f32), pltpu.VMEM((UN, 2, 1, w), f32), pltpu.VMEM((2, 1, w), f32),
            pltpu.VMEM((2, 8, w), f32), pltpu.VMEM((2, HD, w), f32), pltpu.VMEM((HD, w), bf),
            table, table, table],
        compiler_params=pltpu.CompilerParams(vmem_limit_bytes=24 * 1024 * 1024),
        cost_estimate=pl.CostEstimate(flops=10**10, bytes_accessed=10**7, transcendentals=10**7),
        name="attend",
    )(nv, q, k, vt, kx)


MESH_ID = pl.DeviceIdType.MESH


def gather_kernel(text_hbm, k_hbm, v_hbm, wq_hbm, len_ref, lim_ref, nv_ref, q_all, k_all, vt_all, kx_all,
                  text_ref, v_ref, tx, relay, wq, part, ends, in_sem, t1s, t1r, t2s, t2r, t3s, t3r, t4s, t4r, ks, kr, qs_, qr):
    zl, y, x = lax.axis_index("zl"), lax.axis_index("y"), lax.axis_index("x")
    zh, core = lax.axis_index("zh"), lax.axis_index("core")
    inner = {"zl": 1 - zl}
    outer = {"zh": 1 - zh, "zl": 1 - zl}
    other = {"core": 1 - core}
    yp, ym = {"y": lax.rem(y + 1, 4)}, {"y": lax.rem(y + 3, 4)}
    xp, xm = {"x": lax.rem(x + 1, 4)}, {"x": lax.rem(x + 3, 4)}

    c_me = zl * 4 + y
    loads = [pltpu.make_async_copy(src, dst, in_sem.at[i]) for i, (src, dst) in enumerate(
        ((v_hbm, v_ref), (text_hbm, text_ref), (k_hbm, k_all.at[c_me]), (wq_hbm, wq)))]
    for c in loads:
        c.start()
    barrier = pltpu.get_barrier_semaphore()
    for peer in (inner, outer, other, yp, ym, xp, xm):
        pl.semaphore_signal(barrier, inc=1, device_id=peer, device_id_type=MESH_ID)
    loads[0].wait()
    vt_all[c_me] = v_ref[...].astype(jnp.float32).T.astype(jnp.bfloat16)
    loads[1].wait()
    loads[2].wait()
    pl.semaphore_wait(barrier, 7)

    def copy(src, dst, ssem, rsem, dev):
        return pltpu.make_async_remote_copy(src_ref=src, dst_ref=dst, send_sem=ssem, recv_sem=rsem,
                                            device_id=dev, device_id_type=MESH_ID)

    rows = text_ref.shape[0]
    step = rows // 4
    piece = [pl.ds(p * step, step) for p in range(4)]
    started = []

    def go(c):
        c.start()
        started.append(c)
        return c

    t1 = [go(copy(text_ref.at[piece[p]], relay.at[p], t1s.at[p], t1r.at[p], outer if p % 2 else inner)) for p in (1, 0, 3, 2)]
    t1 = {p: c for p, c in zip((1, 0, 3, 2), t1)}
    t3 = go(copy(text_ref, tx.at[0], t3s, t3r, other))
    c_in = (1 - zl) * 4 + y
    c_m, c_p = zl * 4 + lax.rem(y + 3, 4), zl * 4 + lax.rem(y + 1, 4)
    cz_m, cz_p = (1 - zl) * 4 + lax.rem(y + 3, 4), (1 - zl) * 4 + lax.rem(y + 1, 4)
    K = lambda c: k_all.at[c]
    V = lambda c: vt_all.at[c]
    sem = iter(range(15))
    c_2 = zl * 4 + lax.rem(y + 2, 4)
    vh = vt_all.shape[1] // 2
    VH = lambda c, i: vt_all.at[c, pl.ds(i * vh, vh)]

    def kv(src, dst, dev):
        i = next(sem)
        return go(copy(src, dst, ks.at[i], kr.at[i], dev))

    a_kp = kv(K(c_me), K(c_me), yp)
    a_vm = kv(V(c_me), V(c_me), ym)
    a_vp = kv(V(c_me), V(c_me), yp)
    a_km = kv(K(c_me), K(c_me), ym)
    t2 = {}
    for p in (1, 0, 3, 2):
        t1[p].wait_recv()
        t2[p] = go(copy(relay.at[p], tx.at[1, piece[p]], t2s.at[p], t2r.at[p], inner if p % 2 else outer))
    z_k = kv(K(c_me), K(c_me), inner)
    z_v = kv(V(c_me), V(c_me), inner)
    a_kp.wait_recv()
    f_k = kv(K(c_m), K(c_m), yp)
    a_vm.wait_recv()
    f_v = kv(V(c_p), V(c_p), ym)

    NT = GROUP * HD
    half = rows // 2

    def project(src, slot, h, first, last):
        r = pl.ds(h * half, half)

        @pl.loop(0, wq.shape[2] // NT)
        def _(n):
            cols = pl.ds(pl.multiple_of(n * NT, NT), NT)
            d = jnp.dot(src[0][r, :], wq[slot[0], :, cols], preferred_element_type=jnp.float32)
            d = d + jnp.dot(src[1][r, :], wq[slot[1], :, cols], preferred_element_type=jnp.float32)
            if not first:
                d = d + part[r, cols]
            if last:
                for b in range(half // TBLK):
                    heads = [d[b * TBLK:(b + 1) * TBLK, g * HD:(g + 1) * HD] for g in range(GROUP)]
                    q_all[x, h * (half // TBLK) + b, n] = jnp.concatenate(heads, axis=0).T.astype(jnp.bfloat16)
            else:
                part[r, cols] = d

    loads[3].wait()
    t3.wait_recv()
    mine = zh * 2 + core
    beside = zh * 2 + 1 - core
    far = (1 - zh) * 2 + core
    far_beside = (1 - zh) * 2 + 1 - core
    for h in range(2):
        project((text_ref, tx.at[0]), (mine, beside), h, True, False)
    t4 = {}
    for p in (1, 0, 3, 2):
        t2[p].wait_recv()
        t4[p] = go(copy(tx.at[1, piece[p]], tx.at[2, piece[p]], t4s.at[p], t4r.at[p], other))
    halves = [pl.ds(h * (half // TBLK), half // TBLK) for h in range(2)]
    q = {}

    def qcopy(i, src_x, h, dev):
        ref = q_all.at[src_x, halves[h]]
        return go(copy(ref, ref, qs_.at[i], qr.at[i], dev))

    for h in range(2):
        for p in (2 * h, 2 * h + 1):
            t4[p].wait_recv()
        project((tx.at[1], tx.at[2]), (far, far_beside), h, False, True)
        q[h, 1] = qcopy(2 * h, x, h, xp)
        q[h, -1] = qcopy(2 * h + 1, x, h, xm)
    z_k.wait_recv()
    b_kp = kv(K(c_in), K(c_in), yp)
    b_km = kv(K(c_in), K(c_in), ym)
    q[0, 1].wait_recv()
    q_f = qcopy(4, lax.rem(x + 3, 4), 0, xp)
    f_k.wait_recv()
    g_k = kv(K(c_2), K(c_2), inner)
    z_v.wait_recv()
    b_vm = kv(V(c_in), V(c_in), ym)
    b_vp = kv(V(c_in), V(c_in), yp)
    q[1, -1].wait_recv()
    q_b = qcopy(5, lax.rem(x + 1, 4), 1, xm)
    ends[0] = jnp.int32(0)
    for f in range(len_ref.shape[0]):
        ends[f + 1] = ends[f] + len_ref[f]
    blocks = nv_ref.shape[0]
    chunk = k_all.shape[1]
    spot = lax.broadcasted_iota(jnp.int32, kx_all.shape[1:], 0)
    for b in range(blocks):
        seen = ends[lim_ref[c_me * blocks + b]]
        tail = jnp.clip((seen & (4 * chunk - 1)) - x * chunk, 0, chunk)
        seen_here = lax.shift_right_logical(seen, (4 * chunk).bit_length() - 1) * chunk + tail
        nv_ref[b] = seen_here
        edge = seen_here & (TK - 1)
        kx_all[b] = jnp.where(spot < jnp.where(edge == 0, TK, edge), 0.0, 1.0).astype(jnp.bfloat16)
    kx_all[blocks] = jnp.zeros(kx_all.shape[1:], jnp.bfloat16)
    kx_all[blocks + 1] = jnp.ones(kx_all.shape[1:], jnp.bfloat16)
    b_vm.wait_recv()
    g_v = kv(VH(cz_p, 1), VH(cz_p, 1), ym)
    b_vp.wait_recv()
    g_w = kv(VH(cz_m, 0), VH(cz_m, 0), yp)
    for c in (a_vp, a_km, f_v, q[0, -1], q[1, 1], q_f, q_b, b_km, b_kp, g_k, g_v, g_w):
        c.wait_recv()
    for c in started:
        c.wait_send()


def gather_all(text, keys, values, wq, lengths, limits):
    rows, width = text.shape
    bf = jnp.bfloat16
    blocks = 4 * rows // TBLK
    vm = pl.BlockSpec(memory_space=pltpu.VMEM)
    sm = pl.BlockSpec(memory_space=pltpu.SMEM)
    hbm = pl.BlockSpec(memory_space=pltpu.HBM)
    dma = pltpu.SemaphoreType.DMA
    return pl.pallas_call(
        gather_kernel,
        out_shape=(
            jax.ShapeDtypeStruct((blocks,), jnp.int32),
            jax.ShapeDtypeStruct((4, rows // TBLK, 2, HD, GROUP * TBLK), bf),
            jax.ShapeDtypeStruct((8, *keys.shape), bf),
            jax.ShapeDtypeStruct((8, *values.shape[::-1]), bf),
            jax.ShapeDtypeStruct((blocks + 2, TK, HD), bf),
        ),
        in_specs=[hbm] * 4 + [sm] * 2,
        out_specs=(sm, vm, vm, vm, vm),
        scratch_shapes=[
            pltpu.VMEM((rows, width), bf),
            pltpu.VMEM(values.shape, bf),
            pltpu.VMEM((3, rows, width), bf),
            pltpu.VMEM((4, rows // 4, width), bf),
            pltpu.VMEM((4, width, wq.shape[1]), bf),
            pltpu.VMEM((rows, wq.shape[1]), jnp.float32),
            pltpu.SMEM((lengths.shape[0] + 1,), jnp.int32),
            dma((4,)), dma((4,)), dma((4,)), dma((4,)), dma((4,)), dma, dma, dma((4,)), dma((4,)), dma((15,)), dma((15,)), dma((6,)), dma((6,)),
        ],
        compiler_params=pltpu.CompilerParams(collective_id=0, has_side_effects=True, vmem_limit_bytes=40 * 1024 * 1024),
        cost_estimate=pl.CostEstimate(flops=2 * rows * 4 * width * wq.shape[1], bytes_accessed=20 * 2**20, transcendentals=0),
        name="gather",
    )(text, keys, values, wq.reshape(4, width, wq.shape[1]), lengths, limits)


def combine_kernel(gate_ref, o_ref, st_ref, wo, out_ref, og, orel, merged, stg, st_far, attn, pair_out, pair_in, keep, zs, zrel, zin,
                   sts, str_, rs, rr, ds_, dr, cs, cr, as_, ar, bs, br):
    zl, y, x = lax.axis_index("zl"), lax.axis_index("y"), lax.axis_index("x")
    zh, core = lax.axis_index("zh"), lax.axis_index("core")
    inner = {"zl": 1 - zl}
    outer = {"zh": 1 - zh, "zl": 1 - zl}
    other = {"core": 1 - core}
    ip, im, i2 = lax.rem(x + 1, 4), lax.rem(x + 3, 4), lax.rem(x + 2, 4)
    xp, xm, x2 = {"x": ip}, {"x": im}, {"x": i2}

    barrier = pltpu.get_barrier_semaphore()
    for peer in (inner, outer, other, xp, xm, x2):
        pl.semaphore_signal(barrier, inc=1, device_id=peer, device_id_type=MESH_ID)
    pl.semaphore_wait(barrier, 6)
    started = []

    def go(src, dst, ssem, rsem, dev):
        c = pltpu.make_async_remote_copy(src_ref=src, dst_ref=dst, send_sem=ssem, recv_sem=rsem,
                                         device_id=dev, device_id_type=MESH_ID)
        c.start()
        started.append(c)
        return c

    nb = out_ref.shape[0] // TBLK
    stc = [go(st_ref.at[pl.ds(i * nb, nb)], stg.at[s], sts.at[s], str_.at[s], dev)
           for s, i, dev in ((0, ip, xp), (1, im, xm), (2, i2, x2))]
    half = nb // 2
    far = [go(st_ref.at[pl.ds(i2 * nb + v * half, half)], st_far.at[v], sts.at[3 + v], str_.at[3 + v], xm if v else xp)
           for v in range(2)]
    to_relay = lambda j: go(o_ref.at[i2 * nb + j], orel.at[j], rs.at[j], rr.at[j], xp if j < half else xm)
    direct = lambda j, s: go(o_ref.at[(im if s else ip) * nb + j], og.at[s, j], ds_.at[s, j], dr.at[s, j], xm if s else xp)
    r, d = {}, {}

    def merge(j):
        v = j // half
        dest = (im if v else ip) * nb + j
        r[j].wait_recv()
        for h in range(2):
            m1 = st_ref[dest, h, 0:1, :]
            m2 = st_far[v, j - v * half, h, 0:1, :]
            best = jnp.maximum(m1, m2)
            both = o_ref[dest, h].astype(jnp.float32) * jnp.exp2((m1 - best) * C)
            both = both + orel[j, h].astype(jnp.float32) * jnp.exp2((m2 - best) * C)
            merged[j, h] = both.astype(jnp.bfloat16)
        d[j, v] = go(merged.at[j], og.at[v, j], ds_.at[v, j], dr.at[v, j], xm if v else xp)

    r[0] = to_relay(0)
    r[2] = to_relay(2)
    r[1] = to_relay(1)
    r[3] = to_relay(3)
    d[0, 1] = direct(0, 1)
    d[1, 1] = direct(1, 1)
    for c in far:
        c.wait_recv()
    merge(0)
    merge(1)
    d[2, 0] = direct(2, 0)
    d[3, 0] = direct(3, 0)
    merge(2)
    merge(3)
    for c in stc:
        c.wait_recv()
    gate = jnp.tanh(jnp.full((1, out_ref.shape[1]), gate_ref[0], jnp.float32))
    width = out_ref.shape[1]
    pairs, z1, z2 = {}, {}, {}

    def mix_and_project(j):
        near = j // half
        for c in (d[j, 0], d[j, 1]):
            c.wait_recv()
        for h in range(2):
            m = [st_ref[x * nb + j, h, 0:1, :]] + [stg[s, j, h, 0:1, :] for s in range(3)]
            l = [st_ref[x * nb + j, h, 1:2, :]] + [stg[s, j, h, 1:2, :] for s in range(3)]
            best = jnp.maximum(jnp.maximum(m[0], m[1]), jnp.maximum(m[2], m[3]))
            scale = [jnp.exp2((m[s] - best) * C) for s in range(4)]
            total = jnp.maximum((l[0] * scale[0] + l[1] * scale[1]) + (l[2] * scale[2] + l[3] * scale[3]), 1.0)
            joint = jnp.exp2((jnp.maximum(m[near + 1], m[3]) - best) * C)
            mixed = o_ref[x * nb + j, h].astype(jnp.float32) * (scale[0] / total)
            mixed = mixed + og[near, j, h].astype(jnp.float32) * (joint / total)
            mixed = mixed + og[1 - near, j, h].astype(jnp.float32) * (scale[2 - near] / total)
            mixed = mixed.T.astype(jnp.bfloat16)
            for g in range(GROUP):
                col = (h * GROUP + g) * HD
                attn[:, col:col + HD] = mixed[g * TBLK:(g + 1) * TBLK, :]
        def proj(zo, co):
            cols = pl.ds(pl.multiple_of((zo * 2 + co) * width, width), width)
            return jnp.dot(attn[...], wo[:, cols], preferred_element_type=jnp.float32)
        def pair(i, zo):
            pair_out[j, i] = proj(zo, 1 - core).astype(jnp.bfloat16)
            pairs[j, i] = go(pair_out.at[j, i], pair_in.at[j, i], cs.at[j, i], cr.at[j, i], other)
            keep[j, i] = proj(zo, core)

        pair(0, 1 - zh)
        pairs[j, 0].wait_recv()
        zs[j] = (keep[j, 0] + pair_in[j, 0].astype(jnp.float32)).astype(jnp.bfloat16)
        for v, dev in ((0, inner), (1, outer)):
            part = pl.ds(v * hh, hh)
            z1[j, v] = go(zs.at[j, part], zrel.at[j, v], as_.at[j, v], ar.at[j, v], dev)
        pair(1, zh)

    hh = TBLK // 2

    def relay_z(j):
        for v, dev in ((0, outer), (1, inner)):
            z1[j, v].wait_recv()
            z2[j, v] = go(zrel.at[j, v], zin.at[j, pl.ds(v * hh, hh)], bs.at[j, v], br.at[j, v], dev)

    def finish(j):
        for v in range(2):
            z2[j, v].wait_recv()
        pairs[j, 1].wait_recv()
        mine = keep[j, 1] + pair_in[j, 1].astype(jnp.float32)
        out_ref[j * TBLK:(j + 1) * TBLK, :] = (gate * (mine + zin[j].astype(jnp.float32))).astype(jnp.bfloat16)

    for j in range(nb + 3):
        if j < nb:
            mix_and_project(j)
        if 1 <= j <= nb:
            relay_z(j - 1)
        if 2 <= j <= nb + 1:
            finish(j - 2)
    for c in started:
        c.wait_send()


def combine_all(gate, o, st, wo, rows):
    bf = jnp.bfloat16
    nb = rows // TBLK
    width = wo.shape[1] // 4
    vm = pl.BlockSpec(memory_space=pltpu.VMEM)
    dma = pltpu.SemaphoreType.DMA
    tile = o.shape[1:]
    return pl.pallas_call(
        combine_kernel,
        out_shape=jax.ShapeDtypeStruct((rows, width), bf),
        in_specs=[pl.BlockSpec(memory_space=pltpu.SMEM), vm, vm, vm],
        out_specs=vm,
        scratch_shapes=[
            pltpu.VMEM((2, nb, *tile), bf),
            pltpu.VMEM((nb, *tile), bf),
            pltpu.VMEM((nb, *tile), bf),
            pltpu.VMEM((3, nb, *st.shape[1:]), jnp.float32),
            pltpu.VMEM((2, nb // 2, *st.shape[1:]), jnp.float32),
            pltpu.VMEM((TBLK, wo.shape[0]), bf),
            pltpu.VMEM((nb, 2, TBLK, width), bf),
            pltpu.VMEM((nb, 2, TBLK, width), bf),
            pltpu.VMEM((nb, 2, TBLK, width), jnp.float32),
            pltpu.VMEM((nb, TBLK, width), bf),
            pltpu.VMEM((nb, 2, TBLK // 2, width), bf),
            pltpu.VMEM((nb, TBLK, width), bf),
            dma((5,)), dma((5,)), dma((4,)), dma((4,)), dma((2, 4)), dma((2, 4)), dma((4, 2)), dma((4, 2)),
            dma((4, 2)), dma((4, 2)), dma((4, 2)), dma((4, 2)),
        ],
        compiler_params=pltpu.CompilerParams(collective_id=1, has_side_effects=True, vmem_limit_bytes=24 * 1024 * 1024),
        cost_estimate=pl.CostEstimate(flops=2 * rows * wo.shape[0] * wo.shape[1], bytes_accessed=20 * 2**20, transcendentals=0),
        name="combine",
    )(gate, o, st, wo)


def shards(text, wq, keys, values, wo, gate, lengths, limits):
    here = [pltpu.with_memory_space_constraint(a, pltpu.HBM) for a in (text, keys, values, lengths, limits)]
    nv, q, k, vt, kx = gather_all(*here[:3], wq, *here[3:])
    o, st = attention(nv, q.reshape(-1, *q.shape[2:]), k, vt, kx)
    return combine_all(gate, o, st, wo, text.shape[0])


def solution(mesh):
    mesh = Mesh(mesh.devices.reshape(2, 4, 4, 2, 2), ("zl", "y", "x", "zh", "core"))
    seq, head = ("zl", "y", "x"), ("zh", "core")
    in_specs = (P(seq, head), P(None, head), P(seq, head), P(seq, head), P(head, None), P(), P(), P())
    return jax.shard_map(shards, mesh=mesh, in_specs=in_specs, out_specs=P(seq, head), check_vma=False)
```

```python
import math

import jax
import jax.numpy as jnp
from jax import lax
from jax.experimental import pallas as pl
from jax.experimental.pallas import tpu as pltpu
from jax.sharding import Mesh, PartitionSpec as P

HD = 128
TBLK = 64
GROUP = 4
NEG = -1e30
C = math.log2(math.e) / math.sqrt(HD)
TK = 512
CH = 64
UN = 4
PB = 2


def attn_kernel(nv_ref, q_ref, k_ref, vt_ref, kx_ref, o_ref, st_ref, *scr):
    S = [scr[2 * u:2 * u + 2] for u in range(UN)]
    PP = [scr[2 * UN + 2 * u:2 * UN + 2 * u + 2] for u in range(UN)]
    mx_st, al_st, m_c, l_c, a_c, qx, blk, tile, flag = scr[4 * UN:]
    blocks = o_ref.shape[0]

    for i in range(PB):
        blk[i] = 0
        tile[i] = 1
        flag[i] = blocks + 1
    end = jnp.int32(PB)
    last = jnp.int32(0)
    for b in range(blocks):
        count = lax.shift_right_logical(nv_ref[b] + (TK - 1), TK.bit_length() - 1)

        @pl.loop(0, count)
        def _(t):
            blk[end + t] = b
            tile[end + t] = t
            flag[end + t] = blocks

        end = end + count
        last = jnp.where(count > 0, b, last)
        flag[end - 1] = jnp.where(count > 0, b, flag[end - 1])
    for i in range(2 * PB):
        blk[end + i] = last
        tile[end + i] = 1
        flag[end + i] = blocks + 1
    n = lax.shift_right_logical(end - PB + (PB - 1), PB.bit_length() - 1)

    for b in range(blocks):
        @pl.when(nv_ref[b] == 0)
        def _():
            o_ref[b] = jnp.zeros(o_ref.shape[1:], o_ref.dtype)

        for h in range(2):
            st_ref[b, h, 0:1, :] = jnp.full((1, 4 * TBLK), NEG, jnp.float32)
            st_ref[b, h, 1:2, :] = jnp.zeros((1, 4 * TBLK), jnp.float32)
    al_st[...] = jnp.zeros_like(al_st)
    m_c[...] = jnp.full_like(m_c, NEG)
    l_c[...] = jnp.zeros_like(l_c)
    a_c[...] = jnp.zeros_like(a_c)
    for h in range(2):
        for u in range(UN - PB, UN):
            PP[u][h][...] = jnp.zeros_like(PP[u][h])
    qx[...] = jnp.where(lax.broadcasted_iota(jnp.int32, qx.shape, 0) == 0, NEG, 0.0).astype(jnp.bfloat16)

    def qk(par, i, h):
        b, t = blk[i], tile[i]
        lhs = jnp.concatenate([k_ref[t, :, h * HD:(h + 1) * HD], kx_ref[flag[i]]], axis=1)
        rhs = jnp.concatenate([q_ref[b, h], qx[...]], axis=0)
        s = jnp.dot(lhs, rhs, preferred_element_type=jnp.float32)
        S[par][h][...] = s
        mx_st[par, h] = jnp.max(s.reshape(TK // 8, 8, 4 * TBLK), axis=0)

    def pv(par, i, h, late):
        r = jnp.dot(vt_ref[tile[i], h * HD:(h + 1) * HD, :], PP[par][h][...], preferred_element_type=jnp.float32)
        new = a_c[h] * al_st[par, h] + r
        a_c[h] = new
        late.append((i, h, new))

    def softmax(par, i, h, late):
        s_ref, p_ref = S[par][h], PP[par][h]
        m_prev = jnp.where(tile[i] == 0, jnp.full((1, 4 * TBLK), NEG, jnp.float32), m_c[h])
        m_new = jnp.maximum(m_prev, jnp.max(mx_st[par, h], axis=0, keepdims=True))
        m_c[h] = m_new
        alpha = jnp.exp2((m_prev - m_new) * C)
        al_st[par, h] = alpha
        ls = None
        for c in range(TK // CH):
            p = jnp.exp2((s_ref[c * CH:(c + 1) * CH, :] - m_new) * C)
            v = jnp.sum(p.reshape(CH // 8, 8, 4 * TBLK), axis=0)
            ls = v if ls is None else ls + v
            p_ref[c * CH:(c + 1) * CH, :] = p.astype(jnp.bfloat16)
        l_new = l_c[h] * alpha + ls
        l_c[h] = l_new
        late.append((i, h, m_new, jnp.sum(l_new, axis=0, keepdims=True)))

    def flush(late):
        for i, h, *v in late:
            if len(v) == 1:
                o_ref[blk[i], h] = v[0].astype(jnp.bfloat16)
            else:
                st_ref[blk[i], h, 0:1, :] = v[0]
                st_ref[blk[i], h, 1:2, :] = v[1]

    for u in range(PB):
        for h in range(2):
            qk(u, PB + u, h)

    us = [(u, h) for u in range(PB) for h in range(2)]

    def block(base, i):
        late = []
        for u, h in us:
            qk((base + u + PB) % UN, i + u + PB, h)
        for u, h in us:
            pv((base + u - PB) % UN, i + u - PB, h, late)
        for u, h in us:
            softmax((base + u) % UN, i + u, h, late)
        flush(late)

    def tail(base, i):
        late = []
        for u, h in us:
            pv((base + u) % UN, i + u, h, late)
        flush(late)

    R = UN // PB

    @pl.loop(0, lax.div(n + R, R))
    def _(j):
        for r in range(R):
            step = j * R + r

            @pl.when(step < n)
            def _():
                block(r * PB, (step + 1) * PB)

            @pl.when((step == n) & (n > 0))
            def _():
                tail(((r - 1) * PB) % UN, step * PB)


def attention(nv, q, k, vt, kx):
    blocks = nv.shape[0]
    sm = pl.BlockSpec(memory_space=pltpu.SMEM)
    vm = pl.BlockSpec(memory_space=pltpu.VMEM)
    f32, bf = jnp.float32, jnp.bfloat16
    w = 4 * TBLK
    table = pltpu.SMEM((blocks * k.shape[0] + 4 * PB,), jnp.int32)
    return pl.pallas_call(
        attn_kernel,
        out_shape=(jax.ShapeDtypeStruct((blocks, 2, HD, w), bf), jax.ShapeDtypeStruct((blocks, 2, 2, w), f32)),
        in_specs=[sm] + [vm] * 4,
        out_specs=(vm, vm),
        scratch_shapes=[pltpu.VMEM((TK, w), f32)] * (2 * UN) + [pltpu.VMEM((TK, w), bf)] * (2 * UN) + [
            pltpu.VMEM((UN, 2, 8, w), f32), pltpu.VMEM((UN, 2, 1, w), f32), pltpu.VMEM((2, 1, w), f32),
            pltpu.VMEM((2, 8, w), f32), pltpu.VMEM((2, HD, w), f32), pltpu.VMEM((HD, w), bf),
            table, table, table],
        compiler_params=pltpu.CompilerParams(vmem_limit_bytes=24 * 1024 * 1024),
        cost_estimate=pl.CostEstimate(flops=10**10, bytes_accessed=10**7, transcendentals=10**7),
        name="attend",
    )(nv, q, k, vt, kx)


MESH_ID = pl.DeviceIdType.MESH


def gather_kernel(text_hbm, k_hbm, v_hbm, wq_hbm, len_ref, lim_ref, nv_ref, q_all, k_all, vt_all, kx_all,
                  text_ref, v_ref, tx, relay, wq, part, ends, in_sem, t1s, t1r, t2s, t2r, t3s, t3r, t4s, t4r, ks, kr, qs_, qr):
    zl, y, x = lax.axis_index("zl"), lax.axis_index("y"), lax.axis_index("x")
    zh, core = lax.axis_index("zh"), lax.axis_index("core")
    inner = {"zl": 1 - zl}
    outer = {"zh": 1 - zh, "zl": 1 - zl}
    other = {"core": 1 - core}
    yp, ym = {"y": lax.rem(y + 1, 4)}, {"y": lax.rem(y + 3, 4)}
    xp, xm = {"x": lax.rem(x + 1, 4)}, {"x": lax.rem(x + 3, 4)}

    c_me = zl * 4 + y
    loads = [pltpu.make_async_copy(src, dst, in_sem.at[i]) for i, (src, dst) in enumerate(
        ((v_hbm, v_ref), (text_hbm, text_ref), (k_hbm, k_all.at[c_me]), (wq_hbm, wq)))]
    for c in loads:
        c.start()
    barrier = pltpu.get_barrier_semaphore()
    for peer in (inner, outer, other, yp, ym, xp, xm):
        pl.semaphore_signal(barrier, inc=1, device_id=peer, device_id_type=MESH_ID)
    loads[0].wait()
    vt_all[c_me] = v_ref[...].astype(jnp.float32).T.astype(jnp.bfloat16)
    loads[1].wait()
    loads[2].wait()
    pl.semaphore_wait(barrier, 7)

    def copy(src, dst, ssem, rsem, dev):
        return pltpu.make_async_remote_copy(src_ref=src, dst_ref=dst, send_sem=ssem, recv_sem=rsem,
                                            device_id=dev, device_id_type=MESH_ID)

    rows = text_ref.shape[0]
    step = rows // 4
    piece = [pl.ds(p * step, step) for p in range(4)]
    started = []

    def go(c):
        c.start()
        started.append(c)
        return c

    t1 = [go(copy(text_ref.at[piece[p]], relay.at[p], t1s.at[p], t1r.at[p], outer if p % 2 else inner)) for p in (1, 0, 3, 2)]
    t1 = {p: c for p, c in zip((1, 0, 3, 2), t1)}
    t3 = go(copy(text_ref, tx.at[0], t3s, t3r, other))
    c_in = (1 - zl) * 4 + y
    c_m, c_p = zl * 4 + lax.rem(y + 3, 4), zl * 4 + lax.rem(y + 1, 4)
    cz_m, cz_p = (1 - zl) * 4 + lax.rem(y + 3, 4), (1 - zl) * 4 + lax.rem(y + 1, 4)
    K = lambda c: k_all.at[c]
    V = lambda c: vt_all.at[c]
    sem = iter(range(15))
    c_2 = zl * 4 + lax.rem(y + 2, 4)
    kh = k_all.shape[1] // 2
    KH = lambda c, i: k_all.at[c, pl.ds(i * kh, kh)]

    def kv(src, dst, dev):
        i = next(sem)
        return go(copy(src, dst, ks.at[i], kr.at[i], dev))

    a_kp = kv(K(c_me), K(c_me), yp)
    a_vm = kv(V(c_me), V(c_me), ym)
    a_vp = kv(V(c_me), V(c_me), yp)
    a_km = kv(K(c_me), K(c_me), ym)
    t2 = {}
    for p in (1, 0, 3, 2):
        t1[p].wait_recv()
        t2[p] = go(copy(relay.at[p], tx.at[1, piece[p]], t2s.at[p], t2r.at[p], inner if p % 2 else outer))
    z_k = kv(K(c_me), K(c_me), inner)
    z_v = kv(V(c_me), V(c_me), inner)
    a_kp.wait_recv()
    f_k = kv(K(c_m), K(c_m), yp)
    a_vm.wait_recv()
    f_v = kv(V(c_p), V(c_p), ym)

    NT = GROUP * HD
    half = rows // 2

    def project(src, slot, h, first, last):
        r = pl.ds(h * half, half)

        @pl.loop(0, wq.shape[2] // NT)
        def _(n):
            cols = pl.ds(pl.multiple_of(n * NT, NT), NT)
            d = jnp.dot(src[0][r, :], wq[slot[0], :, cols], preferred_element_type=jnp.float32)
            d = d + jnp.dot(src[1][r, :], wq[slot[1], :, cols], preferred_element_type=jnp.float32)
            if not first:
                d = d + part[r, cols]
            if last:
                for b in range(half // TBLK):
                    heads = [d[b * TBLK:(b + 1) * TBLK, g * HD:(g + 1) * HD] for g in range(GROUP)]
                    q_all[x, h * (half // TBLK) + b, n] = jnp.concatenate(heads, axis=0).T.astype(jnp.bfloat16)
            else:
                part[r, cols] = d

    ends[0] = jnp.int32(0)
    for f in range(len_ref.shape[0]):
        ends[f + 1] = ends[f] + len_ref[f]
    blocks = nv_ref.shape[0]
    chunk = k_all.shape[1]
    spot = lax.broadcasted_iota(jnp.int32, kx_all.shape[1:], 0)
    for b in range(blocks):
        seen = ends[lim_ref[c_me * blocks + b]]
        tail = jnp.clip((seen & (4 * chunk - 1)) - x * chunk, 0, chunk)
        mine = lax.shift_right_logical(seen, (4 * chunk).bit_length() - 1) * chunk + tail
        nv_ref[b] = mine
        edge = mine & (TK - 1)
        kx_all[b] = jnp.where(spot < jnp.where(edge == 0, TK, edge), 0.0, 1.0).astype(jnp.bfloat16)
    kx_all[blocks] = jnp.zeros(kx_all.shape[1:], jnp.bfloat16)
    kx_all[blocks + 1] = jnp.ones(kx_all.shape[1:], jnp.bfloat16)
    loads[3].wait()
    t3.wait_recv()
    mine = zh * 2 + core
    beside = zh * 2 + 1 - core
    far = (1 - zh) * 2 + core
    far_beside = (1 - zh) * 2 + 1 - core
    for h in range(2):
        project((text_ref, tx.at[0]), (mine, beside), h, True, False)
    t4 = {}
    for p in (1, 0, 3, 2):
        t2[p].wait_recv()
        t4[p] = go(copy(tx.at[1, piece[p]], tx.at[2, piece[p]], t4s.at[p], t4r.at[p], other))
    halves = [pl.ds(h * (half // TBLK), half // TBLK) for h in range(2)]
    q = {}

    def qcopy(i, src_x, h, dev):
        ref = q_all.at[src_x, halves[h]]
        return go(copy(ref, ref, qs_.at[i], qr.at[i], dev))

    for h in range(2):
        for p in (2 * h, 2 * h + 1):
            t4[p].wait_recv()
        project((tx.at[1], tx.at[2]), (far, far_beside), h, False, True)
        q[h, 1] = qcopy(2 * h, x, h, xp)
        q[h, -1] = qcopy(2 * h + 1, x, h, xm)
    z_k.wait_recv()
    b_kp = kv(K(c_in), K(c_in), yp)
    b_km = kv(K(c_in), K(c_in), ym)
    q[0, 1].wait_recv()
    q_f = qcopy(4, lax.rem(x + 3, 4), 0, xp)
    f_v.wait_recv()
    g_v = kv(V(c_2), V(c_2), inner)
    z_v.wait_recv()
    b_vm = kv(V(c_in), V(c_in), ym)
    b_vp = kv(V(c_in), V(c_in), yp)
    q[1, -1].wait_recv()
    q_b = qcopy(5, lax.rem(x + 1, 4), 1, xm)
    b_kp.wait_recv()
    g_k = kv(KH(cz_m, 0), KH(cz_m, 0), yp)
    b_km.wait_recv()
    g_w = kv(KH(cz_p, 1), KH(cz_p, 1), ym)
    for c in (a_vp, a_km, f_k, q[0, -1], q[1, 1], q_f, q_b, b_vm, b_vp, g_k, g_v, g_w):
        c.wait_recv()
    for c in started:
        c.wait_send()


def gather_all(text, keys, values, wq, lengths, limits):
    rows, width = text.shape
    bf = jnp.bfloat16
    blocks = 4 * rows // TBLK
    vm = pl.BlockSpec(memory_space=pltpu.VMEM)
    sm = pl.BlockSpec(memory_space=pltpu.SMEM)
    hbm = pl.BlockSpec(memory_space=pltpu.HBM)
    dma = pltpu.SemaphoreType.DMA
    return pl.pallas_call(
        gather_kernel,
        out_shape=(
            jax.ShapeDtypeStruct((blocks,), jnp.int32),
            jax.ShapeDtypeStruct((4, rows // TBLK, 2, HD, GROUP * TBLK), bf),
            jax.ShapeDtypeStruct((8, *keys.shape), bf),
            jax.ShapeDtypeStruct((8, *values.shape[::-1]), bf),
            jax.ShapeDtypeStruct((blocks + 2, TK, HD), bf),
        ),
        in_specs=[hbm] * 4 + [sm] * 2,
        out_specs=(sm, vm, vm, vm, vm),
        scratch_shapes=[
            pltpu.VMEM((rows, width), bf),
            pltpu.VMEM(values.shape, bf),
            pltpu.VMEM((3, rows, width), bf),
            pltpu.VMEM((4, rows // 4, width), bf),
            pltpu.VMEM((4, width, wq.shape[1]), bf),
            pltpu.VMEM((rows, wq.shape[1]), jnp.float32),
            pltpu.SMEM((lengths.shape[0] + 1,), jnp.int32),
            dma((4,)), dma((4,)), dma((4,)), dma((4,)), dma((4,)), dma, dma, dma((4,)), dma((4,)), dma((15,)), dma((15,)), dma((6,)), dma((6,)),
        ],
        compiler_params=pltpu.CompilerParams(collective_id=0, has_side_effects=True, vmem_limit_bytes=40 * 1024 * 1024),
        cost_estimate=pl.CostEstimate(flops=2 * rows * 4 * width * wq.shape[1], bytes_accessed=20 * 2**20, transcendentals=0),
        name="gather",
    )(text, keys, values, wq.reshape(4, width, wq.shape[1]), lengths, limits)


def combine_kernel(gate_ref, o_ref, st_ref, wo, out_ref, og, orel, merged, stg, st_far, attn, pair_out, pair_in, keep, zs, zrel, zin,
                   sts, str_, rs, rr, ds_, dr, cs, cr, as_, ar, bs, br):
    zl, y, x = lax.axis_index("zl"), lax.axis_index("y"), lax.axis_index("x")
    zh, core = lax.axis_index("zh"), lax.axis_index("core")
    inner = {"zl": 1 - zl}
    outer = {"zh": 1 - zh, "zl": 1 - zl}
    other = {"core": 1 - core}
    ip, im, i2 = lax.rem(x + 1, 4), lax.rem(x + 3, 4), lax.rem(x + 2, 4)
    xp, xm, x2 = {"x": ip}, {"x": im}, {"x": i2}

    barrier = pltpu.get_barrier_semaphore()
    for peer in (inner, outer, other, xp, xm, x2):
        pl.semaphore_signal(barrier, inc=1, device_id=peer, device_id_type=MESH_ID)
    pl.semaphore_wait(barrier, 6)
    started = []

    def go(src, dst, ssem, rsem, dev):
        c = pltpu.make_async_remote_copy(src_ref=src, dst_ref=dst, send_sem=ssem, recv_sem=rsem,
                                         device_id=dev, device_id_type=MESH_ID)
        c.start()
        started.append(c)
        return c

    nb = out_ref.shape[0] // TBLK
    stc = [go(st_ref.at[pl.ds(i * nb, nb)], stg.at[s], sts.at[s], str_.at[s], dev)
           for s, i, dev in ((0, ip, xp), (1, im, xm), (2, i2, x2))]
    half = nb // 2
    far = [go(st_ref.at[pl.ds(i2 * nb + v * half, half)], st_far.at[v], sts.at[3 + v], str_.at[3 + v], xm if v else xp)
           for v in range(2)]
    to_relay = lambda j: go(o_ref.at[i2 * nb + j], orel.at[j], rs.at[j], rr.at[j], xp if j < half else xm)
    direct = lambda j, s: go(o_ref.at[(im if s else ip) * nb + j], og.at[s, j], ds_.at[s, j], dr.at[s, j], xm if s else xp)
    r, d = {}, {}

    def merge(j):
        v = j // half
        dest = (im if v else ip) * nb + j
        r[j].wait_recv()
        for h in range(2):
            m1 = st_ref[dest, h, 0:1, :]
            m2 = st_far[v, j - v * half, h, 0:1, :]
            best = jnp.maximum(m1, m2)
            both = o_ref[dest, h].astype(jnp.float32) * jnp.exp2((m1 - best) * C)
            both = both + orel[j, h].astype(jnp.float32) * jnp.exp2((m2 - best) * C)
            merged[j, h] = both.astype(jnp.bfloat16)
        d[j, v] = go(merged.at[j], og.at[v, j], ds_.at[v, j], dr.at[v, j], xm if v else xp)

    r[0] = to_relay(0)
    r[2] = to_relay(2)
    r[1] = to_relay(1)
    r[3] = to_relay(3)
    d[0, 1] = direct(0, 1)
    d[1, 1] = direct(1, 1)
    for c in far:
        c.wait_recv()
    merge(0)
    merge(1)
    d[2, 0] = direct(2, 0)
    d[3, 0] = direct(3, 0)
    merge(2)
    merge(3)
    for c in stc:
        c.wait_recv()
    gate = jnp.tanh(jnp.full((1, out_ref.shape[1]), gate_ref[0], jnp.float32))
    width = out_ref.shape[1]
    pairs, z1, z2 = {}, {}, {}

    def mix_and_project(j):
        near = j // half
        for c in (d[j, 0], d[j, 1]):
            c.wait_recv()
        for h in range(2):
            m = [st_ref[x * nb + j, h, 0:1, :]] + [stg[s, j, h, 0:1, :] for s in range(3)]
            l = [st_ref[x * nb + j, h, 1:2, :]] + [stg[s, j, h, 1:2, :] for s in range(3)]
            best = jnp.maximum(jnp.maximum(m[0], m[1]), jnp.maximum(m[2], m[3]))
            scale = [jnp.exp2((m[s] - best) * C) for s in range(4)]
            total = jnp.maximum((l[0] * scale[0] + l[1] * scale[1]) + (l[2] * scale[2] + l[3] * scale[3]), 1.0)
            joint = jnp.exp2((jnp.maximum(m[near + 1], m[3]) - best) * C)
            mixed = o_ref[x * nb + j, h].astype(jnp.float32) * (scale[0] / total)
            mixed = mixed + og[near, j, h].astype(jnp.float32) * (joint / total)
            mixed = mixed + og[1 - near, j, h].astype(jnp.float32) * (scale[2 - near] / total)
            mixed = mixed.T.astype(jnp.bfloat16)
            for g in range(GROUP):
                col = (h * GROUP + g) * HD
                attn[:, col:col + HD] = mixed[g * TBLK:(g + 1) * TBLK, :]
        def proj(zo, co):
            cols = pl.ds(pl.multiple_of((zo * 2 + co) * width, width), width)
            return jnp.dot(attn[...], wo[:, cols], preferred_element_type=jnp.float32)
        def pair(i, zo):
            pair_out[j, i] = proj(zo, 1 - core).astype(jnp.bfloat16)
            pairs[j, i] = go(pair_out.at[j, i], pair_in.at[j, i], cs.at[j, i], cr.at[j, i], other)
            keep[j, i] = proj(zo, core)

        pair(0, 1 - zh)
        pairs[j, 0].wait_recv()
        zs[j] = (keep[j, 0] + pair_in[j, 0].astype(jnp.float32)).astype(jnp.bfloat16)
        for v, dev in ((0, inner), (1, outer)):
            part = pl.ds(v * hh, hh)
            z1[j, v] = go(zs.at[j, part], zrel.at[j, v], as_.at[j, v], ar.at[j, v], dev)
        pair(1, zh)

    hh = TBLK // 2

    def relay_z(j):
        for v, dev in ((0, outer), (1, inner)):
            z1[j, v].wait_recv()
            z2[j, v] = go(zrel.at[j, v], zin.at[j, pl.ds(v * hh, hh)], bs.at[j, v], br.at[j, v], dev)

    def finish(j):
        for v in range(2):
            z2[j, v].wait_recv()
        pairs[j, 1].wait_recv()
        mine = keep[j, 1] + pair_in[j, 1].astype(jnp.float32)
        out_ref[j * TBLK:(j + 1) * TBLK, :] = (gate * (mine + zin[j].astype(jnp.float32))).astype(jnp.bfloat16)

    for j in range(nb + 3):
        if j < nb:
            mix_and_project(j)
        if 1 <= j <= nb:
            relay_z(j - 1)
        if 2 <= j <= nb + 1:
            finish(j - 2)
    for c in started:
        c.wait_send()


def combine_all(gate, o, st, wo, rows):
    bf = jnp.bfloat16
    nb = rows // TBLK
    width = wo.shape[1] // 4
    vm = pl.BlockSpec(memory_space=pltpu.VMEM)
    dma = pltpu.SemaphoreType.DMA
    tile = o.shape[1:]
    return pl.pallas_call(
        combine_kernel,
        out_shape=jax.ShapeDtypeStruct((rows, width), bf),
        in_specs=[pl.BlockSpec(memory_space=pltpu.SMEM), vm, vm, vm],
        out_specs=vm,
        scratch_shapes=[
            pltpu.VMEM((2, nb, *tile), bf),
            pltpu.VMEM((nb, *tile), bf),
            pltpu.VMEM((nb, *tile), bf),
            pltpu.VMEM((3, nb, *st.shape[1:]), jnp.float32),
            pltpu.VMEM((2, nb // 2, *st.shape[1:]), jnp.float32),
            pltpu.VMEM((TBLK, wo.shape[0]), bf),
            pltpu.VMEM((nb, 2, TBLK, width), bf),
            pltpu.VMEM((nb, 2, TBLK, width), bf),
            pltpu.VMEM((nb, 2, TBLK, width), jnp.float32),
            pltpu.VMEM((nb, TBLK, width), bf),
            pltpu.VMEM((nb, 2, TBLK // 2, width), bf),
            pltpu.VMEM((nb, TBLK, width), bf),
            dma((5,)), dma((5,)), dma((4,)), dma((4,)), dma((2, 4)), dma((2, 4)), dma((4, 2)), dma((4, 2)),
            dma((4, 2)), dma((4, 2)), dma((4, 2)), dma((4, 2)),
        ],
        compiler_params=pltpu.CompilerParams(collective_id=1, has_side_effects=True, vmem_limit_bytes=24 * 1024 * 1024),
        cost_estimate=pl.CostEstimate(flops=2 * rows * wo.shape[0] * wo.shape[1], bytes_accessed=20 * 2**20, transcendentals=0),
        name="combine",
    )(gate, o, st, wo)


def shards(text, wq, keys, values, wo, gate, lengths, limits):
    here = [pltpu.with_memory_space_constraint(a, pltpu.HBM) for a in (text, keys, values, lengths, limits)]
    nv, q, k, vt, kx = gather_all(*here[:3], wq, *here[3:])
    o, st = attention(nv, q.reshape(-1, *q.shape[2:]), k, vt, kx)
    return combine_all(gate, o, st, wo, text.shape[0])


def solution(mesh):
    mesh = Mesh(mesh.devices.reshape(2, 4, 4, 2, 2), ("zl", "y", "x", "zh", "core"))
    seq, head = ("zl", "y", "x"), ("zh", "core")
    in_specs = (P(seq, head), P(None, head), P(seq, head), P(seq, head), P(head, None), P(), P(), P())
    return jax.shard_map(shards, mesh=mesh, in_specs=in_specs, out_specs=P(seq, head), check_vma=False)
```
